32 devices in a mesh: px: 8 (over z, x), py: 4 (over y, core).
Axes of the slice: x: 2, y: 2, z: 4, core: 2. Of those that a mesh axis runs over, the one named last changes fastest.
Arguments:
- potential: float32 [256, 256, 256], P(('px', 'py')), may hold values from 0 to 1
- recovery: float32 [256, 256, 256], P(('px', 'py')), may hold values from 0 to 2
- stimulus: float32 [256, 256, 256], P(('px', 'py')), may hold values from -8 to 8
- conductivity: float32 [256, 256, 256], P('px', 'py'), may hold values from 0.2 to 5
Outputs:
- potential_next: float32 [256, 256, 256], P(('px', 'py'))
- recovery_next: float32 [256, 256, 256], P(('px', 'py'))
The draws below stay inside these ranges and needn't reach their ends.
All inputs are finite; a program needn't handle non-finite values.
Results may differ from the reference program's by a relative error of at most 0.0003.
Values sent between devices are 32-bit elements; how exact they have to be, the bound alone decides.
A program may use at most 128 MiB of HBM per device.

```python
import math
import jax
import jax.numpy as jnp

GX = 256
GY = 256
GZ = 256
ITERS = 4


def draw_stimulus(key, part):
    noise = jnp.clip(jax.random.normal(key, (GX, GY, GZ), jnp.float32), -4.0, 4.0) * 2.0
    return noise


def block_scale(rng, shape, split, low, high):
    level, own = 1.0, jax.random.fold_in(rng, 6)
    for axis_at, parts in split:
        heights = jnp.exp(jax.random.uniform(jax.random.fold_in(own, axis_at), (parts,), jnp.float32, low / len(split), high / len(split)))
        level = level * jnp.repeat(heights, shape[axis_at] // parts).reshape([-1 if axis == axis_at else 1 for axis in range(len(shape))])
    return level


def setup_inputs(seed: int = 0) -> dict:
    key_list = jax.random.split(jax.random.key(seed), 5)
    potential = jnp.clip(1.0 * jax.random.uniform(key_list[0], (GX, GY, GZ), jnp.float32) ** block_scale(key_list[0], (GX, GY, GZ), ((0, 32),), -0.2, 0.2), 0.0, 1.0)
    recovery = jnp.clip(2.0 * jax.random.uniform(key_list[1], (GX, GY, GZ), jnp.float32) ** block_scale(key_list[1], (GX, GY, GZ), ((0, 32),), -0.2, 0.2), 0.0, 2.0)
    stimulus = draw_stimulus(jax.random.fold_in(key_list[4], 71), 0)
    conductivity = jnp.clip(jnp.exp(math.log(5.0) - 3.218876 * jax.random.uniform(key_list[3], (GX, GY, GZ), jnp.float32) ** block_scale(key_list[3], (GX, GY, GZ), ((0, 8), (1, 4)), -0.2, 0.2)), 0.2, 5.0)
    return dict(potential=potential, recovery=recovery, stimulus=stimulus, conductivity=conductivity)


mass_rate = 0.01
mean_conduct = 1.0
excite_gain = 8.0
threshold = 0.15
base_rate = 0.002
rate_slope = 0.2
rate_shift = 0.3
time_step = 0.1


def face_conductance(conductivity):
    result_list = []
    for dimension in range(3):
        for offset in (-1, 1):
            result_list.append(0.5 * (conductivity + jnp.roll(conductivity, offset, dimension)))
    return result_list


def operate(field, conductance):
    result_sum = mass_rate * field
    position = 0
    for dimension in range(3):
        for offset in (-1, 1):
            result_sum = result_sum + conductance[position] * (field - jnp.roll(field, offset, dimension))
            position = position + 1
    return result_sum


def wave_term(length):
    modes = jnp.arange(length, dtype=jnp.int32).astype(jnp.float32)
    return 2.0 - 2.0 * jnp.cos((2.0 * math.pi / length) * modes)


def precondition(residual, symbol):
    spectrum = jnp.fft.fftn(residual)
    return jnp.real(jnp.fft.ifftn(spectrum / symbol)).astype(residual.dtype)


def reference(potential, recovery, stimulus, conductivity):
    drive = excite_gain * potential * (potential - threshold) * (1.0 - potential) - potential * recovery
    v_star = potential + time_step * (drive + stimulus)
    rate = base_rate + rate_slope * recovery / (potential + rate_shift)
    recovery_next = recovery + time_step * rate * (-recovery - excite_gain * potential * (potential - threshold - 1.0))
    conductance = face_conductance(conductivity)
    symbol = mass_rate + mean_conduct * (wave_term(GX)[:, None, None] + wave_term(GY)[None, :, None] + wave_term(GZ)[None, None, :])
    solution = v_star
    residual = mass_rate * v_star - operate(solution, conductance)
    precond = precondition(residual, symbol)
    direction = precond
    product_now = jnp.sum(residual * precond)
    for step in range(ITERS):
        image = operate(direction, conductance)
        alpha = product_now / jnp.sum(direction * image)
        solution = solution + alpha * direction
        residual = residual - alpha * image
        if step < ITERS - 1:
            precond = precondition(residual, symbol)
            product_next = jnp.sum(residual * precond)
            direction = precond + (product_next / product_now) * direction
            product_now = product_next
    return solution, recovery_next
```

```python
import math

import jax
import jax.numpy as jnp
import numpy as np
from jax import lax
from jax.experimental import pallas as pl
from jax.experimental.pallas import tpu as pltpu
from jax.sharding import PartitionSpec as P

ITERS = 4

mass_rate = 0.01
excite_gain = 8.0
threshold = 0.15
base_rate = 0.002
rate_slope = 0.2
rate_shift = 0.3
time_step = 0.1
nodes = (2.6, 1.0, 4.0)
pivot_floor = 1e-6
AXES = ("px", "py")


def cas_table(length):
    steps = np.arange(length)
    angle = 2.0 * math.pi / length * (steps[:, None] * steps[None, :] % length)
    return np.cos(angle) + np.sin(angle)


def wave_term(length):
    return 2.0 - 2.0 * np.cos(2.0 * math.pi / length * np.arange(length))


def mode_tables(length_y, length_z):
    shift = mass_rate + wave_term(length_y)[:, None] + wave_term(length_z)[None, :]
    root = np.sqrt(shift * (4.0 + shift))
    rho = 2.0 / (2.0 + shift + root)
    scale = 1.0 / (root * length_y * length_z)
    return rho, scale


def local(potential, recovery, stimulus, conductivity):
    devices = lax.axis_size("px") * lax.axis_size("py")
    me = lax.axis_index(AXES)
    rows, length_y, length_z = potential.shape
    length_x = rows * devices
    forth = [(i, (i + 1) % devices) for i in range(devices)]
    back = [((i + 1) % devices, i) for i in range(devices)]
    drive = (
        excite_gain * potential * (potential - threshold) * (1.0 - potential) - potential * recovery
    )
    v_star = potential + time_step * (drive + stimulus)
    rate = base_rate + rate_slope * recovery / (potential + rate_shift)
    recovery_next = recovery + time_step * rate * (
        -recovery - excite_gain * potential * (potential - threshold - 1.0)
    )
    cond = lax.all_to_all(conductivity, "py", split_axis=0, concat_axis=1, tiled=True)

    def above(field):
        return lax.ppermute(field[:1], AXES, back)

    def below(field):
        return lax.ppermute(field[-1:], AXES, forth)

    cond_x = jnp.concatenate([below(cond), cond, above(cond)], 0)
    face_x = 0.5 * (cond_x[1:] + cond_x[:-1])
    face_y = 0.5 * (cond + jnp.roll(cond, -1, 1))
    face_z = 0.5 * (cond + jnp.roll(cond, -1, 2))

    def faces(field):
        padded = jnp.concatenate([below(field), field, above(field)], 0)
        flow_x = face_x * (padded[:-1] - padded[1:])
        flow_y = face_y * (field - jnp.roll(field, -1, 1))
        flow_z = face_z * (field - jnp.roll(field, -1, 2))
        return (
            (flow_x[1:] - flow_x[:-1])
            + (flow_y - jnp.roll(flow_y, 1, 1))
            + (flow_z - jnp.roll(flow_z, 1, 2))
        )

    rho64, scale64 = mode_tables(length_y, length_z)
    rho = jnp.asarray(rho64, jnp.float32)
    scale = jnp.asarray(scale64, jnp.float32)
    cas_y = jnp.asarray(cas_table(length_y), jnp.float32)
    cas_z = jnp.asarray(cas_table(length_z), jnp.float32)
    step_log = jnp.asarray(rows * np.log(rho64), jnp.float32)
    closing = jnp.asarray(1.0 / (1.0 - rho64**length_x), jnp.float32)
    part = length_y // devices
    step_log = lax.dynamic_slice_in_dim(step_log, me * part, part, 0)
    closing = lax.dynamic_slice_in_dim(closing, me * part, part, 0)
    order = np.arange(devices)
    gap = jnp.asarray((order[:, None] - 1 - order[None, :]) % devices, jnp.float32)

    def both(field):
        field = jnp.einsum("xyz,zk->xyk", field, cas_z, precision=lax.Precision.HIGH)
        return jnp.einsum("xyk,yq->xqk", field, cas_y, precision=lax.Precision.HIGH)

    def apply_inverse(residual):
        spectrum = both(residual)
        head = spectrum[rows - 1]
        tail = spectrum[0]
        for i in range(1, rows):
            head = head + rho**i * spectrum[rows - 1 - i]
            tail = tail + rho**i * spectrum[i]
        ends = jnp.stack([head, tail])[None]
        ends = lax.all_to_all(ends, AXES, split_axis=2, concat_axis=0, tiled=True)
        power = jnp.exp(gap[:, :, None, None] * step_log) * closing
        left = jnp.sum(power * ends[None, :, 0], 1)
        right = jnp.sum(jnp.swapaxes(power, 0, 1) * ends[None, :, 1], 1)
        carry = jnp.stack([left, right], 1)
        carry = lax.all_to_all(carry, AXES, split_axis=0, concat_axis=2, tiled=True)
        forward, backward = [None] * rows, [None] * rows
        value = carry[0, 0]
        for i in range(rows):
            value = spectrum[i] + rho * value
            forward[i] = value
        value = carry[0, 1]
        for i in reversed(range(rows)):
            backward[i] = rho * value
            value = spectrum[i] + backward[i]
        return both(jnp.stack([scale * (f + b) for f, b in zip(forward, backward)]))

    field = v_star
    residual = -faces(v_star)
    direction = image = gamma = alpha = None
    for step in range(ITERS):
        precond = apply_inverse(residual)
        applied = mass_rate * precond + faces(precond)
        sums = jnp.stack([jnp.sum(residual * precond), jnp.sum(applied * precond)])
        sums = jnp.sum(lax.all_gather(jnp.broadcast_to(sums[:, None], (2, 128)), AXES), 0)
        gamma_next, delta = sums[0, 0], sums[1, 0]
        if step == 0:
            alpha = gamma_next / delta
            direction, image = precond, applied
        else:
            beta = gamma_next / gamma
            alpha = gamma_next / (delta - beta * gamma_next / alpha)
            direction = precond + beta * direction
            image = applied + beta * image
        gamma = gamma_next
        field = field + alpha * direction
        residual = residual - alpha * image
    return (field, recovery_next)


def split(table):
    high = table.astype(jnp.bfloat16)
    low = (table - high.astype(np.float64)).astype(jnp.bfloat16)
    return jnp.asarray(high), jnp.asarray(low)


def parts_of(block):
    high = block.astype(jnp.bfloat16)
    return high, (block - high.astype(jnp.float32)).astype(jnp.bfloat16)


def product(left, right):
    def dot(a, b):
        return jnp.dot(a, b, preferred_element_type=jnp.float32)

    return dot(left[0], right[1]) + dot(left[1], right[0]) + dot(left[0], right[0])


def kernel(
    v_ref, cond_in, yh_ref, yl_ref, zh_ref, zl_ref, rho_ref, scale_ref, sigma_ref, pair_ref,
    close_ref,
    u_ref,
    cond, face_x, face_y, face_z, zs, res, first, imag, spec, mode_h, mode_l,
    out, both_ends, chip, recv, sol, car, back, carry, dots, mine, gath,
    c_send, c_recv, h_send, h_recv, p_send, p_recv, e_send, e_recv, s_send, s_recv,
    g_send, g_recv,
):
    count_y = lax.axis_size("py")
    devices = lax.axis_size("px") * count_y
    chips = devices // 2
    my_y = lax.axis_index("py")
    me = lax.axis_index("px") * count_y + my_y
    core = me % 2
    my_chip = me // 2
    rows, length_y, length_z = v_ref.shape
    half = length_y // 2
    part = half // chips
    wide_y = cond_in.shape[1]
    mesh_type = pl.DeviceIdType.MESH

    def device(index):
        return (index // count_y, index % count_y)

    def strip(index):
        return pl.ds(pl.multiple_of(index * part, part), part)

    def remote(source, target, send, recv_sem, index):
        return pltpu.make_async_remote_copy(
            source, target, send, recv_sem, device_id=device(index), device_id_type=mesh_type
        )

    def halo(buffer, base):
        left = (me + devices - 1) % devices
        right = (me + 1) % devices
        return (
            remote(buffer.at[1], buffer.at[rows + 1], h_send.at[base], h_recv.at[base], left),
            remote(
                buffer.at[rows], buffer.at[0], h_send.at[base + 1], h_recv.at[base + 1], right
            ),
        )

    def start_all(make, count):
        def begin(k, _):
            make(k).start()
            return 0

        lax.fori_loop(1, count, begin, 0)

    def wait_all(make, count):
        def finish(k, _):
            make(k).wait()
            return 0

        lax.fori_loop(1, count, finish, 0)

    def cond_copy(k):
        other = (my_y + k) % count_y
        return pltpu.make_async_remote_copy(
            cond_in.at[pl.ds(other * rows, rows)],
            cond.at[pl.ds(1, rows), pl.ds(pl.multiple_of(my_y * wide_y, 8), wide_y), :],
            c_send.at[k], c_recv.at[k],
            device_id=(lax.axis_index("px"), other), device_id_type=mesh_type,
        )

    def ends_copy(k):
        other = (my_chip + k) % chips
        return remote(
            chip.at[:, strip(other), :], recv.at[my_chip], e_send.at[k], e_recv.at[k],
            2 * other + core,
        )

    def carry_copy(k):
        other = (my_chip + k) % chips
        return remote(
            sol.at[other], car.at[:, strip(my_chip), :], s_send.at[k], s_recv.at[k],
            2 * other + core,
        )

    def gath_copy(k):
        return remote(mine, gath.at[me], g_send.at[k], g_recv.at[k], (me + k) % devices)

    partner = me + 1 - 2 * core
    pair_ends = remote(out, both_ends.at[core], p_send.at[0], p_recv.at[0], partner)
    pair_carry = remote(back, carry.at[core], p_send.at[1], p_recv.at[1], partner)

    def flux(field, i):
        here = field[i + 1]
        total = face_x[i + 1] * (here - field[i + 2]) - face_x[i] * (field[i] - here)
        flow = face_y[i] * (here - pltpu.roll(here, length_y - 1, 0))
        total = total + (flow - pltpu.roll(flow, 1, 0))
        flow = face_z[i] * (here - pltpu.roll(here, length_z - 1, 1))
        return here, total + (flow - pltpu.roll(flow, 1, 1))

    start_all(cond_copy, count_y)
    start = zs.at[0]
    for i in range(rows):
        start[i + 1] = v_ref[i]
    field_halo = halo(start, 0)
    for copy in field_halo:
        copy.start()
    cond[pl.ds(1, rows), pl.ds(pl.multiple_of(my_y * wide_y, 8), wide_y), :] = cond_in[
        pl.ds(my_y * rows, rows)
    ]

    def clear(i, _):
        for k in range(1, ITERS):
            zs[k, i + 1] = jnp.zeros((length_y, length_z), jnp.float32)
        return 0

    lax.fori_loop(0, rows, clear, 0)
    wait_all(cond_copy, count_y)
    cond_halo = halo(cond, 2)
    for copy in cond_halo:
        copy.start()

    def faces(i, _):
        here = cond[i + 1]
        face_y[i] = 0.5 * (here + pltpu.roll(here, length_y - 1, 0))
        face_z[i] = 0.5 * (here + pltpu.roll(here, length_z - 1, 1))
        return 0

    lax.fori_loop(0, rows, faces, 0)
    for copy in cond_halo + field_halo:
        copy.wait()

    def faces_along(i, _):
        face_x[i] = 0.5 * (cond[i] + cond[i + 1])
        return 0

    lax.fori_loop(0, rows + 1, faces_along, 0)

    def begin(i, _):
        _, total = flux(start, i)
        first[i] = -total
        res[i] = -total
        return 0

    lax.fori_loop(0, rows, begin, 0)

    def products(step):
        block = 8
        per = length_y // block

        def body(t, sums):
            i = t // per
            at = pl.ds(pl.multiple_of((t % per) * block, block), block)
            image = imag[i, at, :]
            fresh = [zs[j, i + 1, at, :] for j in range(ITERS)]
            sums = [total + z * image for total, z in zip(sums, fresh)] + [
                sums[ITERS] + zs[step, i + 1, at, :] * first[i, at, :]
            ]
            return tuple(sums)

        zero = jnp.zeros((block, length_z), jnp.float32)
        sums = lax.fori_loop(0, rows * per, body, (zero,) * (ITERS + 1), unroll=4)
        for m, total in enumerate(sums):
            dots[step, m] = sum(total[:, c : c + 128] for c in range(0, length_z, 128))

    def block_ends(where, side, target, block=8):
        def body(b, _):
            low = pl.multiple_of(b * block, block)
            at = pl.ds(pl.multiple_of(side * half + low, block), block)
            rho = rho_ref[at, :]
            planes = [spec[i, at, :] for i in range(rows)]
            head, tail = planes[0], planes[rows - 1]
            for i in range(1, rows):
                head = planes[i] + rho * head
                tail = planes[rows - 1 - i] + rho * tail
            target[0, pl.ds(low, block), :] = head
            target[1, pl.ds(low, block), :] = tail
            return 0

        lax.fori_loop(0, half // block, body, 0, unroll=2)

    def chip_ends(block=8):
        def body(b, _):
            low = pl.multiple_of(b * block, block)
            at = pl.ds(low, block)
            sigma = sigma_ref[pl.ds(pl.multiple_of(core * half + low, block), block), :]
            chip[0, at, :] = both_ends[1, 0, at, :] + sigma * both_ends[0, 0, at, :]
            chip[1, at, :] = both_ends[0, 1, at, :] + sigma * both_ends[1, 1, at, :]
            return 0

        lax.fori_loop(0, half // block, body, 0, unroll=4)

    def core_carries(block=8):
        def body(b, _):
            low = pl.multiple_of(b * block, block)
            at = pl.ds(low, block)
            sigma = sigma_ref[pl.ds(pl.multiple_of(core * half + low, block), block), :]
            left, right = car[0, at, :], car[1, at, :]
            after = both_ends[1, 1, at, :] + sigma * right
            before = both_ends[0, 0, at, :] + sigma * left
            carry[core, 0, at, :] = jnp.where(core == 0, left, before)
            carry[core, 1, at, :] = jnp.where(core == 0, after, right)
            back[0, at, :] = jnp.where(core == 0, before, left)
            back[1, at, :] = jnp.where(core == 0, right, after)
            return 0

        lax.fori_loop(0, half // block, body, 0, unroll=4)

    def recur(side, block=16, wide=128):
        def body(b, _):
            low = pl.multiple_of(b * block, block)
            at = pl.ds(pl.multiple_of(side * half + low, block), block)
            for c in range(0, length_z, wide):
                cut = slice(c, c + wide)
                rho = rho_ref[at, cut]
                scale = scale_ref[at, cut]
                left = carry[side, 0, pl.ds(low, block), cut]
                right = carry[side, 1, pl.ds(low, block), cut]
                planes = [spec[i, at, cut] for i in range(rows)]
                ahead = [None] * rows
                value = right
                for i in reversed(range(rows)):
                    ahead[i] = rho * value
                    value = planes[i] + ahead[i]
                modes = [left + rho * value]
                value = left
                for i in range(rows):
                    value = planes[i] + rho * value
                    modes.append(value + ahead[i])
                modes.append(right + rho * value)
                for i, mode in enumerate(modes):
                    mode_h[i, at, cut], mode_l[i, at, cut] = parts_of(scale * mode)
            return 0

        lax.fori_loop(0, half // block, body, 0)

    def solve():
        own = pl.ds(pl.multiple_of(core * half + my_chip * part, part), part)
        sigma = pair_ref[own, :]
        close = close_ref[own, :]
        zero = jnp.zeros_like(sigma)

        def sums(b, pair):
            return (
                recv[b, 0] + sigma * pair[0],
                recv[chips - 1 - b, 1] + sigma * pair[1],
            )

        pair = lax.fori_loop(0, chips, sums, (zero, zero), unroll=4)

        def place(b, pair):
            sol[b, 0] = pair[0]
            sol[chips - 1 - b, 1] = pair[1]
            return sums(b, pair)

        lax.fori_loop(0, chips, place, (pair[0] * close, pair[1] * close), unroll=4)

    def iteration(step, _):
        def ahead(i, _):
            block = product(parts_of(res[i]), (zh_ref[...], zl_ref[...]))
            spec[i] = product((yh_ref[...], yl_ref[...]), parts_of(block))
            return 0

        lax.fori_loop(0, rows, ahead, 0)
        block_ends(spec, 1 - core, out)
        pair_ends.start()
        block_ends(spec, core, both_ends.at[core])
        pair_ends.wait()
        chip_ends()
        start_all(ends_copy, chips)
        recv[my_chip] = chip[:, strip(my_chip), :]

        @pl.when(step > 0)
        def _():
            products(step - 1)

        wait_all(ends_copy, chips)
        solve()
        start_all(carry_copy, chips)
        car[:, strip(my_chip), :] = sol[my_chip]
        wait_all(carry_copy, chips)
        core_carries()
        pair_carry.start()
        recur(core)
        pair_carry.wait()
        recur(1 - core)

        def inverse(i, _):
            block = product((yh_ref[...], yl_ref[...]), (mode_h[i], mode_l[i]))
            zs[step, i] = product(parts_of(block), (zh_ref[...], zl_ref[...]))
            return 0

        lax.fori_loop(0, rows + 2, inverse, 0)
        node = jnp.where(
            step == 0, 1.0 / nodes[0], jnp.where(step == 1, 1.0 / nodes[1], 1.0 / nodes[2])
        )
        latest = zs.at[step]

        def apply(i, _):
            here, total = flux(latest, i)
            image = mass_rate * here + total
            imag[i] = image
            res[i] = res[i] - node * image
            return 0

        lax.fori_loop(0, rows, apply, 0)
        return 0

    lax.fori_loop(0, ITERS, iteration, 0)
    products(ITERS - 1)

    lane = lax.broadcasted_iota(jnp.int32, (1, 128), 1)
    packed = jnp.zeros((1, 128), jnp.float32)
    for k in range(ITERS):
        for m in range(ITERS + 1):
            total = jnp.sum(dots[k, m], keepdims=True)
            packed = jnp.where(lane == k * (ITERS + 1) + m, total, packed)
    mine[...] = packed
    start_all(gath_copy, devices)
    gath[me] = mine[...]
    wait_all(gath_copy, devices)
    total = jnp.sum(gath[...], 0)

    def entry(k, m):
        index = k * (ITERS + 1) + m
        return total[:, index : index + 1]

    lower = [[None] * ITERS for _ in range(ITERS)]
    inverse_pivot, partial, pivots = [], [], []
    for k in range(ITERS):
        pivot = entry(k, k)
        value = entry(k, ITERS)
        for j in range(k):
            pivot = pivot - lower[k][j] * lower[k][j] * pivots[j]
            value = value - lower[k][j] * partial[j]
        pivots.append(pivot)
        usable = pivot > pivot_floor * entry(k, k)
        inverse_pivot.append(jnp.where(usable, 1.0 / jnp.where(usable, pivot, 1.0), 0.0))
        partial.append(value)
        for i in range(k + 1, ITERS):
            value = entry(i, k)
            for j in range(k):
                value = value - lower[i][j] * lower[k][j] * pivots[j]
            lower[i][k] = value * inverse_pivot[k]
    coefs = [None] * ITERS
    for k in reversed(range(ITERS)):
        value = partial[k] * inverse_pivot[k]
        for i in range(k + 1, ITERS):
            value = value - lower[i][k] * coefs[i]
        coefs[k] = value

    def finish(i, _):
        value = v_ref[i]
        for k in range(ITERS):
            value = value + coefs[k] * zs[k, i + 1]
        u_ref[i] = value
        return 0

    lax.fori_loop(0, rows, finish, 0)


def fused(potential, recovery, stimulus, conductivity):
    count_y = lax.axis_size("py")
    devices = lax.axis_size("px") * count_y
    rows, length_y, length_z = potential.shape
    part = length_y // devices
    if count_y % 2 or part % 8 or length_z % 128 or conductivity.shape[1] % 8:
        return local(potential, recovery, stimulus, conductivity)
    drive = (
        excite_gain * potential * (potential - threshold) * (1.0 - potential) - potential * recovery
    )
    v_star = potential + time_step * (drive + stimulus)
    rate = base_rate + rate_slope * recovery / (potential + rate_shift)
    recovery_next = recovery + time_step * rate * (
        -recovery - excite_gain * potential * (potential - threshold - 1.0)
    )
    rho, scale = mode_tables(length_y, length_z)
    tables = split(cas_table(length_y)) + split(cas_table(length_z))
    tables += tuple(
        jnp.asarray(table, jnp.float32)
        for table in (
            rho, scale, rho**rows, rho ** (2 * rows), 1.0 / (1.0 - rho ** (rows * devices))
        )
    )
    plane = (length_y, length_z)
    whole = (rows,) + plane
    half = (2, length_y // 2, length_z)
    chips = devices // 2

    def vmem(shape, dtype=jnp.float32):
        return pltpu.VMEM(shape, dtype)

    dma = pltpu.SemaphoreType.DMA
    padded = (rows + 2,) + plane
    slots = (chips, 2, part, length_z)
    field = pl.pallas_call(
        kernel,
        out_shape=jax.ShapeDtypeStruct(whole, jnp.float32),
        in_specs=[pl.BlockSpec(memory_space=pltpu.VMEM)] * 11,
        out_specs=pl.BlockSpec(memory_space=pltpu.VMEM),
        scratch_shapes=[
            vmem(padded), vmem((rows + 1,) + plane), vmem(whole), vmem(whole),
            vmem((ITERS,) + padded), vmem(whole), vmem(whole), vmem(whole), vmem(whole),
            vmem(padded, jnp.bfloat16), vmem(padded, jnp.bfloat16),
            vmem(half), vmem((2,) + half), vmem(half), vmem(slots), vmem(slots), vmem(half),
            vmem(half), vmem((2,) + half),
            vmem((ITERS, ITERS + 1, 8, 128)), vmem((1, 128)), vmem((devices, 1, 128)),
            dma((count_y,)), dma((count_y,)), dma((4,)), dma((4,)), dma((2,)), dma((2,)),
            dma((chips,)), dma((chips,)), dma((chips,)), dma((chips,)),
            dma((devices,)), dma((devices,)),
        ],
        compiler_params=pltpu.CompilerParams(
            has_side_effects=True, vmem_limit_bytes=60 * 1024 * 1024
        ),
    )(v_star, conductivity, *tables)
    return (field, recovery_next)


def solution(mesh):
    in_specs = (
        P(AXES, None, None),
        P(AXES, None, None),
        P(AXES, None, None),
        P("px", "py", None),
    )
    out_specs = (P(AXES, None, None), P(AXES, None, None))
    return jax.shard_map(fused, mesh=mesh, in_specs=in_specs, out_specs=out_specs, check_vma=False)
```

```python
import math

import jax
import jax.numpy as jnp
import numpy as np
from jax import lax
from jax.experimental import pallas as pl
from jax.experimental.pallas import tpu as pltpu
from jax.sharding import PartitionSpec as P

ITERS = 4

mass_rate = 0.01
excite_gain = 8.0
threshold = 0.15
base_rate = 0.002
rate_slope = 0.2
rate_shift = 0.3
time_step = 0.1
nodes = (2.6, 1.0, 4.0)
pivot_floor = 1e-6
AXES = ("px", "py")


def cas_table(length):
    steps = np.arange(length)
    angle = 2.0 * math.pi / length * (steps[:, None] * steps[None, :] % length)
    return np.cos(angle) + np.sin(angle)


def wave_term(length):
    return 2.0 - 2.0 * np.cos(2.0 * math.pi / length * np.arange(length))


def mode_tables(length_y, length_z):
    shift = mass_rate + wave_term(length_y)[:, None] + wave_term(length_z)[None, :]
    root = np.sqrt(shift * (4.0 + shift))
    rho = 2.0 / (2.0 + shift + root)
    scale = 1.0 / (root * length_y * length_z)
    return rho, scale


def local(potential, recovery, stimulus, conductivity):
    devices = lax.axis_size("px") * lax.axis_size("py")
    me = lax.axis_index(AXES)
    rows, length_y, length_z = potential.shape
    length_x = rows * devices
    forth = [(i, (i + 1) % devices) for i in range(devices)]
    back = [((i + 1) % devices, i) for i in range(devices)]
    drive = (
        excite_gain * potential * (potential - threshold) * (1.0 - potential) - potential * recovery
    )
    v_star = potential + time_step * (drive + stimulus)
    rate = base_rate + rate_slope * recovery / (potential + rate_shift)
    recovery_next = recovery + time_step * rate * (
        -recovery - excite_gain * potential * (potential - threshold - 1.0)
    )
    cond = lax.all_to_all(conductivity, "py", split_axis=0, concat_axis=1, tiled=True)

    def above(field):
        return lax.ppermute(field[:1], AXES, back)

    def below(field):
        return lax.ppermute(field[-1:], AXES, forth)

    cond_x = jnp.concatenate([below(cond), cond, above(cond)], 0)
    face_x = 0.5 * (cond_x[1:] + cond_x[:-1])
    face_y = 0.5 * (cond + jnp.roll(cond, -1, 1))
    face_z = 0.5 * (cond + jnp.roll(cond, -1, 2))

    def faces(field):
        padded = jnp.concatenate([below(field), field, above(field)], 0)
        flow_x = face_x * (padded[:-1] - padded[1:])
        flow_y = face_y * (field - jnp.roll(field, -1, 1))
        flow_z = face_z * (field - jnp.roll(field, -1, 2))
        return (
            (flow_x[1:] - flow_x[:-1])
            + (flow_y - jnp.roll(flow_y, 1, 1))
            + (flow_z - jnp.roll(flow_z, 1, 2))
        )

    rho64, scale64 = mode_tables(length_y, length_z)
    rho = jnp.asarray(rho64, jnp.float32)
    scale = jnp.asarray(scale64, jnp.float32)
    cas_y = jnp.asarray(cas_table(length_y), jnp.float32)
    cas_z = jnp.asarray(cas_table(length_z), jnp.float32)
    step_log = jnp.asarray(rows * np.log(rho64), jnp.float32)
    closing = jnp.asarray(1.0 / (1.0 - rho64**length_x), jnp.float32)
    part = length_y // devices
    step_log = lax.dynamic_slice_in_dim(step_log, me * part, part, 0)
    closing = lax.dynamic_slice_in_dim(closing, me * part, part, 0)
    order = np.arange(devices)
    gap = jnp.asarray((order[:, None] - 1 - order[None, :]) % devices, jnp.float32)

    def both(field):
        field = jnp.einsum("xyz,zk->xyk", field, cas_z, precision=lax.Precision.HIGH)
        return jnp.einsum("xyk,yq->xqk", field, cas_y, precision=lax.Precision.HIGH)

    def apply_inverse(residual):
        spectrum = both(residual)
        head = spectrum[rows - 1]
        tail = spectrum[0]
        for i in range(1, rows):
            head = head + rho**i * spectrum[rows - 1 - i]
            tail = tail + rho**i * spectrum[i]
        ends = jnp.stack([head, tail])[None]
        ends = lax.all_to_all(ends, AXES, split_axis=2, concat_axis=0, tiled=True)
        power = jnp.exp(gap[:, :, None, None] * step_log) * closing
        left = jnp.sum(power * ends[None, :, 0], 1)
        right = jnp.sum(jnp.swapaxes(power, 0, 1) * ends[None, :, 1], 1)
        carry = jnp.stack([left, right], 1)
        carry = lax.all_to_all(carry, AXES, split_axis=0, concat_axis=2, tiled=True)
        forward, backward = [None] * rows, [None] * rows
        value = carry[0, 0]
        for i in range(rows):
            value = spectrum[i] + rho * value
            forward[i] = value
        value = carry[0, 1]
        for i in reversed(range(rows)):
            backward[i] = rho * value
            value = spectrum[i] + backward[i]
        return both(jnp.stack([scale * (f + b) for f, b in zip(forward, backward)]))

    field = v_star
    residual = -faces(v_star)
    direction = image = gamma = alpha = None
    for step in range(ITERS):
        precond = apply_inverse(residual)
        applied = mass_rate * precond + faces(precond)
        sums = jnp.stack([jnp.sum(residual * precond), jnp.sum(applied * precond)])
        sums = jnp.sum(lax.all_gather(jnp.broadcast_to(sums[:, None], (2, 128)), AXES), 0)
        gamma_next, delta = sums[0, 0], sums[1, 0]
        if step == 0:
            alpha = gamma_next / delta
            direction, image = precond, applied
        else:
            beta = gamma_next / gamma
            alpha = gamma_next / (delta - beta * gamma_next / alpha)
            direction = precond + beta * direction
            image = applied + beta * image
        gamma = gamma_next
        field = field + alpha * direction
        residual = residual - alpha * image
    return (field, recovery_next)


def split(table):
    high = table.astype(jnp.bfloat16)
    low = (table - high.astype(np.float64)).astype(jnp.bfloat16)
    return jnp.asarray(high), jnp.asarray(low)


def parts_of(block):
    high = block.astype(jnp.bfloat16)
    return high, (block - high.astype(jnp.float32)).astype(jnp.bfloat16)


def product(left, right):
    def dot(a, b):
        return jnp.dot(a, b, preferred_element_type=jnp.float32)

    return dot(left[0], right[1]) + dot(left[1], right[0]) + dot(left[0], right[0])


def kernel(
    v_ref, cond_in, yh_ref, yl_ref, zh_ref, zl_ref, rho_ref, scale_ref, sigma_ref, pair_ref,
    close_ref,
    u_ref,
    cond, face_x, face_y, face_z, zs, res, first, imag, spec, mode_h, mode_l, turn_h, turn_l,
    out, both_ends, chip, recv, sol, car, back, carry, dots, mine, gath,
    c_send, c_recv, h_send, h_recv, p_send, p_recv, e_send, e_recv, s_send, s_recv,
    g_send, g_recv,
):
    count_y = lax.axis_size("py")
    devices = lax.axis_size("px") * count_y
    chips = devices // 2
    my_y = lax.axis_index("py")
    me = lax.axis_index("px") * count_y + my_y
    core = me % 2
    my_chip = me // 2
    rows, length_y, length_z = v_ref.shape
    half = length_y // 2
    part = half // chips
    wide_y = cond_in.shape[1]
    mesh_type = pl.DeviceIdType.MESH

    def device(index):
        return (index // count_y, index % count_y)

    def strip(index):
        return pl.ds(pl.multiple_of(index * part, part), part)

    def remote(source, target, send, recv_sem, index):
        return pltpu.make_async_remote_copy(
            source, target, send, recv_sem, device_id=device(index), device_id_type=mesh_type
        )

    def halo(buffer, base):
        left = (me + devices - 1) % devices
        right = (me + 1) % devices
        return (
            remote(buffer.at[1], buffer.at[rows + 1], h_send.at[base], h_recv.at[base], left),
            remote(
                buffer.at[rows], buffer.at[0], h_send.at[base + 1], h_recv.at[base + 1], right
            ),
        )

    def start_all(make, count):
        for k in range(1, count):
            make(k).start()

    def wait_all(make, count):
        for k in range(1, count):
            make(k).wait()

    def cond_copy(k):
        other = (my_y + k) % count_y
        return pltpu.make_async_remote_copy(
            cond_in.at[pl.ds(other * rows, rows)],
            cond.at[pl.ds(1, rows), pl.ds(pl.multiple_of(my_y * wide_y, 8), wide_y), :],
            c_send.at[k], c_recv.at[k],
            device_id=(lax.axis_index("px"), other), device_id_type=mesh_type,
        )

    def ends_copy(k):
        other = (my_chip + k) % chips
        return remote(
            chip.at[:, strip(other), :], recv.at[my_chip], e_send.at[k], e_recv.at[k],
            2 * other + core,
        )

    def carry_copy(k):
        other = (my_chip + k) % chips
        return remote(
            sol.at[other], car.at[:, strip(my_chip), :], s_send.at[k], s_recv.at[k],
            2 * other + core,
        )

    def gath_copy(k):
        return remote(mine, gath.at[me], g_send.at[k], g_recv.at[k], (me + k) % devices)

    partner = me + 1 - 2 * core
    pair_ends = remote(out, both_ends.at[core], p_send.at[0], p_recv.at[0], partner)
    pair_carry = remote(back, carry.at[core], p_send.at[1], p_recv.at[1], partner)

    def flux(field, i):
        here = field[i + 1]
        total = face_x[i + 1] * (here - field[i + 2]) - face_x[i] * (field[i] - here)
        flow = face_y[i] * (here - pltpu.roll(here, length_y - 1, 0))
        total = total + (flow - pltpu.roll(flow, 1, 0))
        flow = face_z[i] * (here - pltpu.roll(here, length_z - 1, 1))
        return here, total + (flow - pltpu.roll(flow, 1, 1))

    start_all(cond_copy, count_y)
    start = zs.at[0]
    for i in range(rows):
        start[i + 1] = v_ref[i]
    field_halo = halo(start, 0)
    for copy in field_halo:
        copy.start()
    cond[pl.ds(1, rows), pl.ds(pl.multiple_of(my_y * wide_y, 8), wide_y), :] = cond_in[
        pl.ds(my_y * rows, rows)
    ]

    def clear(i, _):
        for k in range(1, ITERS):
            zs[k, i + 1] = jnp.zeros((length_y, length_z), jnp.float32)
        return 0

    lax.fori_loop(0, rows, clear, 0)
    with jax.named_scope("cond_wait"):
        wait_all(cond_copy, count_y)
    cond_halo = halo(cond, 2)
    for copy in cond_halo:
        copy.start()

    def faces(i, _):
        here = cond[i + 1]
        face_y[i] = 0.5 * (here + pltpu.roll(here, length_y - 1, 0))
        face_z[i] = 0.5 * (here + pltpu.roll(here, length_z - 1, 1))
        return 0

    with jax.named_scope("face_halo"):
        lax.fori_loop(0, rows, faces, 0)
        for copy in cond_halo + field_halo:
            copy.wait()

    def faces_along(i, _):
        face_x[i] = 0.5 * (cond[i] + cond[i + 1])
        return 0

    lax.fori_loop(0, rows + 1, faces_along, 0)

    def begin(i, _):
        _, total = flux(start, i)
        first[i] = -total
        res[i] = -total
        return 0

    with jax.named_scope("begin"):
        lax.fori_loop(0, rows, begin, 0)

    def products(step):
        block = 8
        per = length_y // block

        def body(t, sums):
            i = t // per
            at = pl.ds(pl.multiple_of((t % per) * block, block), block)
            image = imag[i, at, :]
            fresh = [zs[j, i + 1, at, :] for j in range(ITERS)]
            sums = [total + z * image for total, z in zip(sums, fresh)] + [
                sums[ITERS] + zs[step, i + 1, at, :] * first[i, at, :]
            ]
            return tuple(sums)

        zero = jnp.zeros((block, length_z), jnp.float32)
        sums = lax.fori_loop(0, rows * per, body, (zero,) * (ITERS + 1), unroll=4)
        for m, total in enumerate(sums):
            dots[step, m] = sum(total[:, c : c + 128] for c in range(0, length_z, 128))

    def block_ends(where, side, target, block=8):
        def body(b, _):
            low = pl.multiple_of(b * block, block)
            at = pl.ds(pl.multiple_of(side * half + low, block), block)
            rho = rho_ref[at, :]
            planes = [spec[i, at, :] for i in range(rows)]
            head, tail = planes[0], planes[rows - 1]
            for i in range(1, rows):
                head = planes[i] + rho * head
                tail = planes[rows - 1 - i] + rho * tail
            target[0, pl.ds(low, block), :] = head
            target[1, pl.ds(low, block), :] = tail
            return 0

        lax.fori_loop(0, half // block, body, 0, unroll=2)

    def chip_ends(block=8):
        def body(b, _):
            low = pl.multiple_of(b * block, block)
            at = pl.ds(low, block)
            sigma = sigma_ref[pl.ds(pl.multiple_of(core * half + low, block), block), :]
            chip[0, at, :] = both_ends[1, 0, at, :] + sigma * both_ends[0, 0, at, :]
            chip[1, at, :] = both_ends[0, 1, at, :] + sigma * both_ends[1, 1, at, :]
            return 0

        lax.fori_loop(0, half // block, body, 0, unroll=4)

    def core_carries(block=8):
        def body(b, _):
            low = pl.multiple_of(b * block, block)
            at = pl.ds(low, block)
            sigma = sigma_ref[pl.ds(pl.multiple_of(core * half + low, block), block), :]
            left, right = car[0, at, :], car[1, at, :]
            after = both_ends[1, 1, at, :] + sigma * right
            before = both_ends[0, 0, at, :] + sigma * left
            carry[core, 0, at, :] = jnp.where(core == 0, left, before)
            carry[core, 1, at, :] = jnp.where(core == 0, after, right)
            back[0, at, :] = jnp.where(core == 0, before, left)
            back[1, at, :] = jnp.where(core == 0, right, after)
            return 0

        lax.fori_loop(0, half // block, body, 0, unroll=4)

    def recur(side, block=16, wide=128):
        def body(b, _):
            low = pl.multiple_of(b * block, block)
            at = pl.ds(pl.multiple_of(side * half + low, block), block)
            for c in range(0, length_z, wide):
                cut = slice(c, c + wide)
                rho = rho_ref[at, cut]
                scale = scale_ref[at, cut]
                left = carry[side, 0, pl.ds(low, block), cut]
                right = carry[side, 1, pl.ds(low, block), cut]
                planes = [spec[i, at, cut] for i in range(rows)]
                ahead = [None] * rows
                value = right
                for i in reversed(range(rows)):
                    ahead[i] = rho * value
                    value = planes[i] + ahead[i]
                modes = [left + rho * value]
                value = left
                for i in range(rows):
                    value = planes[i] + rho * value
                    modes.append(value + ahead[i])
                modes.append(right + rho * value)
                for i, mode in enumerate(modes):
                    mode_h[i, at, cut], mode_l[i, at, cut] = parts_of(scale * mode)
            return 0

        lax.fori_loop(0, half // block, body, 0)

    def solve():
        own = pl.ds(pl.multiple_of(core * half + my_chip * part, part), part)
        sigma = pair_ref[own, :]
        close = close_ref[own, :]
        zero = jnp.zeros_like(sigma)

        def sums(b, pair):
            return (
                recv[b, 0] + sigma * pair[0],
                recv[chips - 1 - b, 1] + sigma * pair[1],
            )

        pair = lax.fori_loop(0, chips, sums, (zero, zero), unroll=4)

        def place(b, pair):
            sol[b, 0] = pair[0]
            sol[chips - 1 - b, 1] = pair[1]
            return sums(b, pair)

        lax.fori_loop(0, chips, place, (pair[0] * close, pair[1] * close), unroll=4)

    def ahead_z(i, _):
        turned = product(parts_of(res[i]), (zh_ref[...], zl_ref[...]))
        turn_h[i], turn_l[i] = parts_of(turned)
        return 0

    def ahead_y(side):
        at = pl.ds(pl.multiple_of(side * half, half), half)

        def body(i, _):
            spec[i, at, :] = product((yh_ref[at, :], yl_ref[at, :]), (turn_h[i], turn_l[i]))
            return 0

        lax.fori_loop(0, rows, body, 0, unroll=4)

    def inverse_z(side):
        at = pl.ds(pl.multiple_of(side * half, half), half)

        def body(i, _):
            modes = (mode_h[i, at, :], mode_l[i, at, :])
            turn_h[i, at, :], turn_l[i, at, :] = parts_of(
                product(modes, (zh_ref[...], zl_ref[...]))
            )
            return 0

        lax.fori_loop(0, rows + 2, body, 0, unroll=5)

    def iteration(step, _):
        with jax.named_scope("ahead_z"):
            lax.fori_loop(0, rows, ahead_z, 0, unroll=4)
        with jax.named_scope("ahead_y1"):
            ahead_y(1 - core)
        with jax.named_scope("ends1"):
            block_ends(spec, 1 - core, out)
        pair_ends.start()
        with jax.named_scope("ahead_y2"):
            ahead_y(core)
        with jax.named_scope("ends2"):
            block_ends(spec, core, both_ends.at[core])
        with jax.named_scope("pair_wait"):
            pair_ends.wait()
        chip_ends()
        with jax.named_scope("ends_start"):
            start_all(ends_copy, chips)
            recv[my_chip] = chip[:, strip(my_chip), :]

        @pl.when(step > 0)
        def _():
            products(step - 1)

        with jax.named_scope("ends_wait"):
            wait_all(ends_copy, chips)
        with jax.named_scope("solve"):
            solve()
            start_all(carry_copy, chips)
            car[:, strip(my_chip), :] = sol[my_chip]
        with jax.named_scope("carry_wait"):
            wait_all(carry_copy, chips)
        with jax.named_scope("recur1"):
            core_carries()
            pair_carry.start()
            recur(core)
        with jax.named_scope("inverse_z1"):
            inverse_z(core)
        with jax.named_scope("carry_pair_wait"):
            pair_carry.wait()
        with jax.named_scope("recur2"):
            recur(1 - core)
        with jax.named_scope("inverse_z2"):
            inverse_z(1 - core)

        def inverse(i, _):
            zs[step, i] = product((yh_ref[...], yl_ref[...]), (turn_h[i], turn_l[i]))
            return 0

        with jax.named_scope("inverse_y"):
            lax.fori_loop(0, rows + 2, inverse, 0, unroll=5)
        node = jnp.where(
            step == 0, 1.0 / nodes[0], jnp.where(step == 1, 1.0 / nodes[1], 1.0 / nodes[2])
        )
        latest = zs.at[step]

        def apply(i, _):
            here, total = flux(latest, i)
            image = mass_rate * here + total
            imag[i] = image
            res[i] = res[i] - node * image
            return 0

        with jax.named_scope("apply"):
            lax.fori_loop(0, rows, apply, 0)
        return 0

    lax.fori_loop(0, ITERS, iteration, 0)
    with jax.named_scope("last_products"):
        products(ITERS - 1)

    lane = lax.broadcasted_iota(jnp.int32, (1, 128), 1)
    packed = jnp.zeros((1, 128), jnp.float32)
    for k in range(ITERS):
        for m in range(ITERS + 1):
            total = jnp.sum(dots[k, m], keepdims=True)
            packed = jnp.where(lane == k * (ITERS + 1) + m, total, packed)
    mine[...] = packed
    with jax.named_scope("gather"):
        start_all(gath_copy, devices)
        gath[me] = mine[...]
        wait_all(gath_copy, devices)
    total = jnp.sum(gath[...], 0)

    def entry(k, m):
        index = k * (ITERS + 1) + m
        return total[:, index : index + 1]

    lower = [[None] * ITERS for _ in range(ITERS)]
    inverse_pivot, partial, pivots = [], [], []
    for k in range(ITERS):
        pivot = entry(k, k)
        value = entry(k, ITERS)
        for j in range(k):
            pivot = pivot - lower[k][j] * lower[k][j] * pivots[j]
            value = value - lower[k][j] * partial[j]
        pivots.append(pivot)
        usable = pivot > pivot_floor * entry(k, k)
        inverse_pivot.append(jnp.where(usable, 1.0 / jnp.where(usable, pivot, 1.0), 0.0))
        partial.append(value)
        for i in range(k + 1, ITERS):
            value = entry(i, k)
            for j in range(k):
                value = value - lower[i][j] * lower[k][j] * pivots[j]
            lower[i][k] = value * inverse_pivot[k]
    coefs = [None] * ITERS
    for k in reversed(range(ITERS)):
        value = partial[k] * inverse_pivot[k]
        for i in range(k + 1, ITERS):
            value = value - lower[i][k] * coefs[i]
        coefs[k] = value

    def finish(i, _):
        value = v_ref[i]
        for k in range(ITERS):
            value = value + coefs[k] * zs[k, i + 1]
        u_ref[i] = value
        return 0

    with jax.named_scope("finish"):
        lax.fori_loop(0, rows, finish, 0)


def fused(potential, recovery, stimulus, conductivity):
    count_y = lax.axis_size("py")
    devices = lax.axis_size("px") * count_y
    rows, length_y, length_z = potential.shape
    part = length_y // devices
    if count_y % 2 or part % 8 or length_z % 128 or conductivity.shape[1] % 8:
        return local(potential, recovery, stimulus, conductivity)
    drive = (
        excite_gain * potential * (potential - threshold) * (1.0 - potential) - potential * recovery
    )
    v_star = potential + time_step * (drive + stimulus)
    rate = base_rate + rate_slope * recovery / (potential + rate_shift)
    recovery_next = recovery + time_step * rate * (
        -recovery - excite_gain * potential * (potential - threshold - 1.0)
    )
    rho, scale = mode_tables(length_y, length_z)
    tables = split(cas_table(length_y)) + split(cas_table(length_z))
    tables += tuple(
        jnp.asarray(table, jnp.float32)
        for table in (
            rho, scale, rho**rows, rho ** (2 * rows), 1.0 / (1.0 - rho ** (rows * devices))
        )
    )
    plane = (length_y, length_z)
    whole = (rows,) + plane
    half = (2, length_y // 2, length_z)
    chips = devices // 2

    def vmem(shape, dtype=jnp.float32):
        return pltpu.VMEM(shape, dtype)

    dma = pltpu.SemaphoreType.DMA
    padded = (rows + 2,) + plane
    slots = (chips, 2, part, length_z)
    field = pl.pallas_call(
        kernel,
        out_shape=jax.ShapeDtypeStruct(whole, jnp.float32),
        in_specs=[pl.BlockSpec(memory_space=pltpu.VMEM)] * 11,
        out_specs=pl.BlockSpec(memory_space=pltpu.VMEM),
        scratch_shapes=[
            vmem(padded), vmem((rows + 1,) + plane), vmem(whole), vmem(whole),
            vmem((ITERS,) + padded), vmem(whole), vmem(whole), vmem(whole), vmem(whole),
            vmem(padded, jnp.bfloat16), vmem(padded, jnp.bfloat16),
            vmem(padded, jnp.bfloat16), vmem(padded, jnp.bfloat16),
            vmem(half), vmem((2,) + half), vmem(half), vmem(slots), vmem(slots), vmem(half),
            vmem(half), vmem((2,) + half),
            vmem((ITERS, ITERS + 1, 8, 128)), vmem((1, 128)), vmem((devices, 1, 128)),
            dma((count_y,)), dma((count_y,)), dma((4,)), dma((4,)), dma((2,)), dma((2,)),
            dma((chips,)), dma((chips,)), dma((chips,)), dma((chips,)),
            dma((devices,)), dma((devices,)),
        ],
        compiler_params=pltpu.CompilerParams(
            has_side_effects=True, vmem_limit_bytes=60 * 1024 * 1024
        ),
    )(v_star, conductivity, *tables)
    return (field, recovery_next)


def solution(mesh):
    in_specs = (
        P(AXES, None, None),
        P(AXES, None, None),
        P(AXES, None, None),
        P("px", "py", None),
    )
    out_specs = (P(AXES, None, None), P(AXES, None, None))
    return jax.shard_map(fused, mesh=mesh, in_specs=in_specs, out_specs=out_specs, check_vma=False)
```

```python
import math

import jax
import jax.numpy as jnp
import numpy as np
from jax import lax
from jax.experimental import pallas as pl
from jax.experimental.pallas import tpu as pltpu
from jax.sharding import PartitionSpec as P

ITERS = 4

mass_rate = 0.01
excite_gain = 8.0
threshold = 0.15
base_rate = 0.002
rate_slope = 0.2
rate_shift = 0.3
time_step = 0.1
nodes = (2.6, 1.0, 4.0)
pivot_floor = 1e-6
AXES = ("px", "py")


def cas_table(length):
    steps = np.arange(length)
    angle = 2.0 * math.pi / length * (steps[:, None] * steps[None, :] % length)
    return np.cos(angle) + np.sin(angle)


def wave_term(length):
    return 2.0 - 2.0 * np.cos(2.0 * math.pi / length * np.arange(length))


def mode_tables(length_y, length_z):
    shift = mass_rate + wave_term(length_y)[:, None] + wave_term(length_z)[None, :]
    root = np.sqrt(shift * (4.0 + shift))
    rho = 2.0 / (2.0 + shift + root)
    scale = 1.0 / (root * length_y * length_z)
    return rho, scale


def local(potential, recovery, stimulus, conductivity):
    devices = lax.axis_size("px") * lax.axis_size("py")
    me = lax.axis_index(AXES)
    rows, length_y, length_z = potential.shape
    length_x = rows * devices
    forth = [(i, (i + 1) % devices) for i in range(devices)]
    back = [((i + 1) % devices, i) for i in range(devices)]
    drive = (
        excite_gain * potential * (potential - threshold) * (1.0 - potential) - potential * recovery
    )
    v_star = potential + time_step * (drive + stimulus)
    rate = base_rate + rate_slope * recovery / (potential + rate_shift)
    recovery_next = recovery + time_step * rate * (
        -recovery - excite_gain * potential * (potential - threshold - 1.0)
    )
    cond = lax.all_to_all(conductivity, "py", split_axis=0, concat_axis=1, tiled=True)

    def above(field):
        return lax.ppermute(field[:1], AXES, back)

    def below(field):
        return lax.ppermute(field[-1:], AXES, forth)

    cond_x = jnp.concatenate([below(cond), cond, above(cond)], 0)
    face_x = 0.5 * (cond_x[1:] + cond_x[:-1])
    face_y = 0.5 * (cond + jnp.roll(cond, -1, 1))
    face_z = 0.5 * (cond + jnp.roll(cond, -1, 2))

    def faces(field):
        padded = jnp.concatenate([below(field), field, above(field)], 0)
        flow_x = face_x * (padded[:-1] - padded[1:])
        flow_y = face_y * (field - jnp.roll(field, -1, 1))
        flow_z = face_z * (field - jnp.roll(field, -1, 2))
        return (
            (flow_x[1:] - flow_x[:-1])
            + (flow_y - jnp.roll(flow_y, 1, 1))
            + (flow_z - jnp.roll(flow_z, 1, 2))
        )

    rho64, scale64 = mode_tables(length_y, length_z)
    rho = jnp.asarray(rho64, jnp.float32)
    scale = jnp.asarray(scale64, jnp.float32)
    cas_y = jnp.asarray(cas_table(length_y), jnp.float32)
    cas_z = jnp.asarray(cas_table(length_z), jnp.float32)
    step_log = jnp.asarray(rows * np.log(rho64), jnp.float32)
    closing = jnp.asarray(1.0 / (1.0 - rho64**length_x), jnp.float32)
    part = length_y // devices
    step_log = lax.dynamic_slice_in_dim(step_log, me * part, part, 0)
    closing = lax.dynamic_slice_in_dim(closing, me * part, part, 0)
    order = np.arange(devices)
    gap = jnp.asarray((order[:, None] - 1 - order[None, :]) % devices, jnp.float32)

    def both(field):
        field = jnp.einsum("xyz,zk->xyk", field, cas_z, precision=lax.Precision.HIGH)
        return jnp.einsum("xyk,yq->xqk", field, cas_y, precision=lax.Precision.HIGH)

    def apply_inverse(residual):
        spectrum = both(residual)
        head = spectrum[rows - 1]
        tail = spectrum[0]
        for i in range(1, rows):
            head = head + rho**i * spectrum[rows - 1 - i]
            tail = tail + rho**i * spectrum[i]
        ends = jnp.stack([head, tail])[None]
        ends = lax.all_to_all(ends, AXES, split_axis=2, concat_axis=0, tiled=True)
        power = jnp.exp(gap[:, :, None, None] * step_log) * closing
        left = jnp.sum(power * ends[None, :, 0], 1)
        right = jnp.sum(jnp.swapaxes(power, 0, 1) * ends[None, :, 1], 1)
        carry = jnp.stack([left, right], 1)
        carry = lax.all_to_all(carry, AXES, split_axis=0, concat_axis=2, tiled=True)
        forward, backward = [None] * rows, [None] * rows
        value = carry[0, 0]
        for i in range(rows):
            value = spectrum[i] + rho * value
            forward[i] = value
        value = carry[0, 1]
        for i in reversed(range(rows)):
            backward[i] = rho * value
            value = spectrum[i] + backward[i]
        return both(jnp.stack([scale * (f + b) for f, b in zip(forward, backward)]))

    field = v_star
    residual = -faces(v_star)
    direction = image = gamma = alpha = None
    for step in range(ITERS):
        precond = apply_inverse(residual)
        applied = mass_rate * precond + faces(precond)
        sums = jnp.stack([jnp.sum(residual * precond), jnp.sum(applied * precond)])
        sums = jnp.sum(lax.all_gather(jnp.broadcast_to(sums[:, None], (2, 128)), AXES), 0)
        gamma_next, delta = sums[0, 0], sums[1, 0]
        if step == 0:
            alpha = gamma_next / delta
            direction, image = precond, applied
        else:
            beta = gamma_next / gamma
            alpha = gamma_next / (delta - beta * gamma_next / alpha)
            direction = precond + beta * direction
            image = applied + beta * image
        gamma = gamma_next
        field = field + alpha * direction
        residual = residual - alpha * image
    return (field, recovery_next)


def split(table):
    high = table.astype(jnp.bfloat16)
    low = (table - high.astype(np.float64)).astype(jnp.bfloat16)
    return jnp.asarray(high), jnp.asarray(low)


def parts_of(block):
    high = block.astype(jnp.bfloat16)
    return high, (block - high.astype(jnp.float32)).astype(jnp.bfloat16)


def product(left, right):
    def dot(a, b):
        return jnp.dot(a, b, preferred_element_type=jnp.float32)

    return dot(left[0], right[1]) + dot(left[1], right[0]) + dot(left[0], right[0])


def kernel(
    v_hbm, w_hbm, i_hbm, cond_in, yh_in, yl_in, zh_in, zl_in, rho_in, scale_in, sigma_in,
    pair_in, wrap_in,
    u_ref,
    v_ref, w_ref, i_ref, yh_ref, yl_ref, zh_ref, zl_ref, rho_ref, scale_ref, sigma_ref,
    pair_ref, wrap_ref,
    cond, face_x, face_y, face_z, zs, res, first, imag, spec, mode_h, mode_l, turn_h, turn_l,
    out, both_ends, chip, recv, sol, car, back, carry, dots, mine, gath,
    c_send, c_recv, h_send, h_recv, p_send, p_recv, e_send, e_recv, s_send, s_recv,
    g_send, g_recv, l_sem,
):
    count_y = lax.axis_size("py")
    devices = lax.axis_size("px") * count_y
    chips = devices // 2
    my_y = lax.axis_index("py")
    me = lax.axis_index("px") * count_y + my_y
    core = me % 2
    my_chip = me // 2
    rows, length_y, length_z = v_ref.shape
    half = length_y // 2
    part = half // chips
    wide_y = cond_in.shape[1]
    mesh_type = pl.DeviceIdType.MESH

    def device(index):
        return (index // count_y, index % count_y)

    def strip(index):
        return pl.ds(pl.multiple_of(index * part, part), part)

    def remote(source, target, send, recv_sem, index):
        return pltpu.make_async_remote_copy(
            source, target, send, recv_sem, device_id=device(index), device_id_type=mesh_type
        )

    def halo(buffer, base):
        left = (me + devices - 1) % devices
        right = (me + 1) % devices
        return (
            remote(buffer.at[1], buffer.at[rows + 1], h_send.at[base], h_recv.at[base], left),
            remote(
                buffer.at[rows], buffer.at[0], h_send.at[base + 1], h_recv.at[base + 1], right
            ),
        )

    def start_all(make, count):
        for k in range(1, count):
            make(k).start()

    def wait_all(make, count):
        for k in range(1, count):
            make(k).wait()

    def cond_copy(row, k):
        other = (my_y + k) % count_y
        return pltpu.make_async_remote_copy(
            cond_in.at[other * rows + row],
            cond.at[row + 1, pl.ds(pl.multiple_of(my_y * wide_y, 8), wide_y), :],
            c_send.at[row, k], c_recv.at[row, k],
            device_id=(lax.axis_index("px"), other), device_id_type=mesh_type,
        )

    def ends_copy(k):
        other = (my_chip + k) % chips
        return remote(
            chip.at[:, strip(other), :], recv.at[my_chip], e_send.at[k], e_recv.at[k],
            2 * other + core,
        )

    def carry_copy(k):
        other = (my_chip + k) % chips
        return remote(
            sol.at[other], car.at[:, strip(my_chip), :], s_send.at[k], s_recv.at[k],
            2 * other + core,
        )

    def gath_copy(k):
        return remote(mine, gath.at[me], g_send.at[k], g_recv.at[k], (me + k) % devices)

    partner = me + 1 - 2 * core
    pair_ends = remote(out, both_ends.at[core], p_send.at[0], p_recv.at[0], partner)
    pair_carry = remote(back, carry.at[core], p_send.at[1], p_recv.at[1], partner)

    def flux(field, i):
        here = field[i + 1]
        total = face_x[i + 1] * (here - field[i + 2]) - face_x[i] * (field[i] - here)
        flow = face_y[i] * (here - pltpu.roll(here, length_y - 1, 0))
        total = total + (flow - pltpu.roll(flow, 1, 0))
        flow = face_z[i] * (here - pltpu.roll(here, length_z - 1, 1))
        return here, total + (flow - pltpu.roll(flow, 1, 1))

    def local_copy(source, target, index):
        return pltpu.make_async_copy(source, target, l_sem.at[index])

    for row in (0, rows - 1) + tuple(range(1, rows - 1)):
        for k in range(1, count_y):
            cond_copy(row, k).start()
    own_cond = local_copy(
        cond_in.at[pl.ds(my_y * rows, rows)],
        cond.at[pl.ds(1, rows), pl.ds(pl.multiple_of(my_y * wide_y, 8), wide_y), :],
        0,
    )
    ionic = [
        local_copy(source, target, 1 + n)
        for n, (source, target) in enumerate(((v_hbm, v_ref), (w_hbm, w_ref), (i_hbm, i_ref)))
    ]
    loads = [
        local_copy(source, target, 4 + n)
        for n, (source, target) in enumerate((
            (yh_in, yh_ref), (yl_in, yl_ref), (zh_in, zh_ref), (zl_in, zl_ref),
            (rho_in, rho_ref), (scale_in, scale_ref), (sigma_in, sigma_ref),
            (pair_in, pair_ref), (wrap_in, wrap_ref),
        ))
    ]
    for copy in ionic + [own_cond] + loads:
        copy.start()
    for copy in ionic:
        copy.wait()
    start = zs.at[0]

    def react(i, _):
        v = v_ref[i]
        drive = excite_gain * v * (v - threshold) * (1.0 - v) - v * w_ref[i]
        v = v + time_step * (drive + i_ref[i])
        v_ref[i] = v
        start[i + 1] = v
        return 0

    lax.fori_loop(0, rows, react, 0)
    field_halo = halo(start, 0)
    for copy in field_halo:
        copy.start()

    def clear(i, _):
        for k in range(1, ITERS):
            zs[k, i + 1] = jnp.zeros((length_y, length_z), jnp.float32)
        return 0

    lax.fori_loop(0, rows, clear, 0)
    own_cond.wait()
    for copy in loads:
        copy.wait()

    def arrive(row):
        for k in range(1, count_y):
            cond_copy(row, k).wait_recv()

    def faces(i):
        here = cond[i + 1]
        face_y[i] = 0.5 * (here + pltpu.roll(here, length_y - 1, 0))
        face_z[i] = 0.5 * (here + pltpu.roll(here, length_z - 1, 1))

    def faces_along(i):
        face_x[i] = 0.5 * (cond[i] + cond[i + 1])

    def begin(i):
        _, total = flux(start, i)
        first[i] = -total
        res[i] = -total
        ahead_z(i, 0)

    def ahead_z(i, _):
        turned = product(parts_of(res[i]), (zh_ref[...], zl_ref[...]))
        turn_h[i], turn_l[i] = parts_of(turned)
        return 0

    with jax.named_scope("cond_first"):
        arrive(0)
        arrive(rows - 1)
    cond_halo = halo(cond, 2)
    for copy in cond_halo:
        copy.start()
    faces(0)
    faces(rows - 1)
    with jax.named_scope("cond_1"):
        arrive(1)
    faces(1)
    faces_along(1)
    for copy in field_halo:
        copy.wait()

    def stream(t, _):
        arrive(t)
        faces(t)
        faces_along(t)
        begin(t - 1)
        return 0

    with jax.named_scope("cond_stream"):
        lax.fori_loop(2, rows - 1, stream, 0)
    with jax.named_scope("cond_halo"):
        for copy in cond_halo:
            copy.wait()
    with jax.named_scope("cond_tail"):
        faces_along(rows - 1)
        faces_along(0)
        faces_along(rows)
        begin(rows - 2)
        begin(0)
        begin(rows - 1)
        for row in range(rows):
            for k in range(1, count_y):
                cond_copy(row, k).wait_send()

    def products(step):
        block = 8
        per = length_y // block

        def body(t, sums):
            i = t // per
            at = pl.ds(pl.multiple_of((t % per) * block, block), block)
            image = imag[i, at, :]
            fresh = [zs[j, i + 1, at, :] for j in range(ITERS)]
            sums = [total + z * image for total, z in zip(sums, fresh)] + [
                sums[ITERS] + zs[step, i + 1, at, :] * first[i, at, :]
            ]
            return tuple(sums)

        zero = jnp.zeros((block, length_z), jnp.float32)
        sums = lax.fori_loop(0, rows * per, body, (zero,) * (ITERS + 1), unroll=4)
        for m, total in enumerate(sums):
            dots[step, m] = sum(total[:, c : c + 128] for c in range(0, length_z, 128))

    def block_ends(where, side, target, block=8):
        def body(b, _):
            low = pl.multiple_of(b * block, block)
            at = pl.ds(pl.multiple_of(side * half + low, block), block)
            rho = rho_ref[at, :]
            planes = [spec[i, at, :] for i in range(rows)]
            head, tail = planes[0], planes[rows - 1]
            for i in range(1, rows):
                head = planes[i] + rho * head
                tail = planes[rows - 1 - i] + rho * tail
            target[0, pl.ds(low, block), :] = head
            target[1, pl.ds(low, block), :] = tail
            return 0

        lax.fori_loop(0, half // block, body, 0, unroll=2)

    def chip_ends(block=8):
        def body(b, _):
            low = pl.multiple_of(b * block, block)
            at = pl.ds(low, block)
            sigma = sigma_ref[pl.ds(pl.multiple_of(core * half + low, block), block), :]
            chip[0, at, :] = both_ends[1, 0, at, :] + sigma * both_ends[0, 0, at, :]
            chip[1, at, :] = both_ends[0, 1, at, :] + sigma * both_ends[1, 1, at, :]
            return 0

        lax.fori_loop(0, half // block, body, 0, unroll=4)

    def core_carries(block=8):
        def body(b, _):
            low = pl.multiple_of(b * block, block)
            at = pl.ds(low, block)
            sigma = sigma_ref[pl.ds(pl.multiple_of(core * half + low, block), block), :]
            left, right = car[0, at, :], car[1, at, :]
            after = both_ends[1, 1, at, :] + sigma * right
            before = both_ends[0, 0, at, :] + sigma * left
            carry[core, 0, at, :] = jnp.where(core == 0, left, before)
            carry[core, 1, at, :] = jnp.where(core == 0, after, right)
            back[0, at, :] = jnp.where(core == 0, before, left)
            back[1, at, :] = jnp.where(core == 0, right, after)
            return 0

        lax.fori_loop(0, half // block, body, 0, unroll=4)

    def recur(side, block=16, wide=128):
        def body(b, _):
            low = pl.multiple_of(b * block, block)
            at = pl.ds(pl.multiple_of(side * half + low, block), block)
            for c in range(0, length_z, wide):
                cut = slice(c, c + wide)
                rho = rho_ref[at, cut]
                scale = scale_ref[at, cut]
                left = carry[side, 0, pl.ds(low, block), cut]
                right = carry[side, 1, pl.ds(low, block), cut]
                planes = [spec[i, at, cut] for i in range(rows)]
                ahead = [None] * rows
                value = right
                for i in reversed(range(rows)):
                    ahead[i] = rho * value
                    value = planes[i] + ahead[i]
                modes = [left + rho * value]
                value = left
                for i in range(rows):
                    value = planes[i] + rho * value
                    modes.append(value + ahead[i])
                modes.append(right + rho * value)
                for i, mode in enumerate(modes):
                    mode_h[i, at, cut], mode_l[i, at, cut] = parts_of(scale * mode)
            return 0

        lax.fori_loop(0, half // block, body, 0)

    def solve():
        own = pl.ds(pl.multiple_of(core * half + my_chip * part, part), part)
        sigma = pair_ref[own, :]
        close = 1.0 / (1.0 - wrap_ref[own, :])
        zero = jnp.zeros_like(sigma)

        def sums(b, pair):
            return (
                recv[b, 0] + sigma * pair[0],
                recv[chips - 1 - b, 1] + sigma * pair[1],
            )

        pair = lax.fori_loop(0, chips, sums, (zero, zero), unroll=4)

        def place(b, pair):
            sol[b, 0] = pair[0]
            sol[chips - 1 - b, 1] = pair[1]
            return sums(b, pair)

        lax.fori_loop(0, chips, place, (pair[0] * close, pair[1] * close), unroll=4)

    def ahead_y(side):
        at = pl.ds(pl.multiple_of(side * half, half), half)

        def body(i, _):
            spec[i, at, :] = product((yh_ref[at, :], yl_ref[at, :]), (turn_h[i], turn_l[i]))
            return 0

        lax.fori_loop(0, rows, body, 0, unroll=4)

    def inverse_z(side):
        at = pl.ds(pl.multiple_of(side * half, half), half)

        def body(i, _):
            modes = (mode_h[i, at, :], mode_l[i, at, :])
            turn_h[i, at, :], turn_l[i, at, :] = parts_of(
                product(modes, (zh_ref[...], zl_ref[...]))
            )
            return 0

        lax.fori_loop(0, rows + 2, body, 0, unroll=5)

    def iteration(step, _):
        @pl.when(step > 0)
        def _():
            with jax.named_scope("ahead_z"):
                lax.fori_loop(0, rows, ahead_z, 0, unroll=4)

        with jax.named_scope("ahead_y1"):
            ahead_y(1 - core)
        with jax.named_scope("ends1"):
            block_ends(spec, 1 - core, out)
        pair_ends.start()
        with jax.named_scope("ahead_y2"):
            ahead_y(core)
        with jax.named_scope("ends2"):
            block_ends(spec, core, both_ends.at[core])
        with jax.named_scope("pair_wait"):
            pair_ends.wait()
        chip_ends()
        with jax.named_scope("ends_start"):
            start_all(ends_copy, chips)
            recv[my_chip] = chip[:, strip(my_chip), :]

        @pl.when(step > 0)
        def _():
            products(step - 1)

        with jax.named_scope("ends_wait"):
            wait_all(ends_copy, chips)
        with jax.named_scope("solve"):
            solve()
            start_all(carry_copy, chips)
            car[:, strip(my_chip), :] = sol[my_chip]
        with jax.named_scope("carry_wait"):
            wait_all(carry_copy, chips)
        with jax.named_scope("recur1"):
            core_carries()
            pair_carry.start()
            recur(core)
        with jax.named_scope("inverse_z1"):
            inverse_z(core)
        with jax.named_scope("carry_pair_wait"):
            pair_carry.wait()
        with jax.named_scope("recur2"):
            recur(1 - core)
        with jax.named_scope("inverse_z2"):
            inverse_z(1 - core)

        def inverse(i, _):
            zs[step, i] = product((yh_ref[...], yl_ref[...]), (turn_h[i], turn_l[i]))
            return 0

        with jax.named_scope("inverse_y"):
            lax.fori_loop(0, rows + 2, inverse, 0, unroll=5)
        node = jnp.where(
            step == 0, 1.0 / nodes[0], jnp.where(step == 1, 1.0 / nodes[1], 1.0 / nodes[2])
        )
        latest = zs.at[step]

        def apply(i, _):
            here, total = flux(latest, i)
            image = mass_rate * here + total
            imag[i] = image
            res[i] = res[i] - node * image
            return 0

        with jax.named_scope("apply"):
            lax.fori_loop(0, rows, apply, 0)
        return 0

    lax.fori_loop(0, ITERS, iteration, 0)
    with jax.named_scope("last_products"):
        products(ITERS - 1)

    lane = lax.broadcasted_iota(jnp.int32, (1, 128), 1)
    packed = jnp.zeros((1, 128), jnp.float32)
    for k in range(ITERS):
        for m in range(ITERS + 1):
            total = jnp.sum(dots[k, m], keepdims=True)
            packed = jnp.where(lane == k * (ITERS + 1) + m, total, packed)
    mine[...] = packed
    with jax.named_scope("gather"):
        start_all(gath_copy, devices)
        gath[me] = mine[...]
        wait_all(gath_copy, devices)
    total = jnp.sum(gath[...], 0)

    def entry(k, m):
        index = k * (ITERS + 1) + m
        return total[:, index : index + 1]

    lower = [[None] * ITERS for _ in range(ITERS)]
    inverse_pivot, partial, pivots = [], [], []
    for k in range(ITERS):
        pivot = entry(k, k)
        value = entry(k, ITERS)
        for j in range(k):
            pivot = pivot - lower[k][j] * lower[k][j] * pivots[j]
            value = value - lower[k][j] * partial[j]
        pivots.append(pivot)
        usable = pivot > pivot_floor * entry(k, k)
        inverse_pivot.append(jnp.where(usable, 1.0 / jnp.where(usable, pivot, 1.0), 0.0))
        partial.append(value)
        for i in range(k + 1, ITERS):
            value = entry(i, k)
            for j in range(k):
                value = value - lower[i][j] * lower[k][j] * pivots[j]
            lower[i][k] = value * inverse_pivot[k]
    coefs = [None] * ITERS
    for k in reversed(range(ITERS)):
        value = partial[k] * inverse_pivot[k]
        for i in range(k + 1, ITERS):
            value = value - lower[i][k] * coefs[i]
        coefs[k] = value

    def finish(i, _):
        value = v_ref[i]
        for k in range(ITERS):
            value = value + coefs[k] * zs[k, i + 1]
        u_ref[i] = value
        return 0

    with jax.named_scope("finish"):
        lax.fori_loop(0, rows, finish, 0)


def fused(potential, recovery, stimulus, conductivity):
    count_y = lax.axis_size("py")
    devices = lax.axis_size("px") * count_y
    rows, length_y, length_z = potential.shape
    part = length_y // devices
    if count_y % 2 or part % 8 or length_z % 128 or conductivity.shape[1] % 8:
        return local(potential, recovery, stimulus, conductivity)
    rate = base_rate + rate_slope * recovery / (potential + rate_shift)
    recovery_next = recovery + time_step * rate * (
        -recovery - excite_gain * potential * (potential - threshold - 1.0)
    )
    rho, scale = mode_tables(length_y, length_z)
    tables = split(cas_table(length_y)) + split(cas_table(length_z))
    tables += tuple(
        jnp.asarray(table, jnp.float32)
        for table in (
            rho, scale, rho**rows, rho ** (2 * rows), rho ** (rows * devices)
        )
    )
    plane = (length_y, length_z)
    whole = (rows,) + plane
    half = (2, length_y // 2, length_z)
    chips = devices // 2

    def vmem(shape, dtype=jnp.float32):
        return pltpu.VMEM(shape, dtype)

    dma = pltpu.SemaphoreType.DMA
    padded = (rows + 2,) + plane
    square = [vmem((n, n), jnp.bfloat16) for n in (length_y, length_y, length_z, length_z)]
    slots = (chips, 2, part, length_z)
    field = pl.pallas_call(
        kernel,
        out_shape=jax.ShapeDtypeStruct(whole, jnp.float32),
        in_specs=[pl.BlockSpec(memory_space=pl.ANY)] * 13,
        out_specs=pl.BlockSpec(memory_space=pltpu.VMEM),
        scratch_shapes=[
            vmem(whole), vmem(whole), vmem(whole), *square,
            *(vmem(plane) for _ in range(5)),
            vmem(padded), vmem((rows + 1,) + plane), vmem(whole), vmem(whole),
            vmem((ITERS,) + padded), vmem(whole), vmem(whole), vmem(whole), vmem(whole),
            vmem(padded, jnp.bfloat16), vmem(padded, jnp.bfloat16),
            vmem(padded, jnp.bfloat16), vmem(padded, jnp.bfloat16),
            vmem(half), vmem((2,) + half), vmem(half), vmem(slots), vmem(slots), vmem(half),
            vmem(half), vmem((2,) + half),
            vmem((ITERS, ITERS + 1, 8, 128)), vmem((1, 128)), vmem((devices, 1, 128)),
            dma((rows, count_y)), dma((rows, count_y)), dma((4,)), dma((4,)), dma((2,)), dma((2,)),
            dma((chips,)), dma((chips,)), dma((chips,)), dma((chips,)),
            dma((devices,)), dma((devices,)), dma((13,)),
        ],
        compiler_params=pltpu.CompilerParams(
            has_side_effects=True, vmem_limit_bytes=60 * 1024 * 1024
        ),
    )(potential, recovery, stimulus, conductivity, *tables)
    return (field, recovery_next)


def solution(mesh):
    in_specs = (
        P(AXES, None, None),
        P(AXES, None, None),
        P(AXES, None, None),
        P("px", "py", None),
    )
    out_specs = (P(AXES, None, None), P(AXES, None, None))
    return jax.shard_map(fused, mesh=mesh, in_specs=in_specs, out_specs=out_specs, check_vma=False)
```

```python
import math

import jax
import jax.numpy as jnp
import numpy as np
from jax import lax
from jax.experimental import pallas as pl
from jax.experimental.pallas import tpu as pltpu
from jax.sharding import PartitionSpec as P

ITERS = 4

mass_rate = 0.01
excite_gain = 8.0
threshold = 0.15
base_rate = 0.002
rate_slope = 0.2
rate_shift = 0.3
time_step = 0.1
nodes = (2.6, 1.0, 4.0)
BLOCK = 64
pivot_floor = 1e-6
AXES = ("px", "py")


def cas_table(length):
    steps = np.arange(length)
    angle = 2.0 * math.pi / length * (steps[:, None] * steps[None, :] % length)
    return np.cos(angle) + np.sin(angle)


def wave_term(length):
    return 2.0 - 2.0 * np.cos(2.0 * math.pi / length * np.arange(length))


def mode_tables(length_y, length_z):
    shift = mass_rate + wave_term(length_y)[:, None] + wave_term(length_z)[None, :]
    root = np.sqrt(shift * (4.0 + shift))
    rho = 2.0 / (2.0 + shift + root)
    scale = 1.0 / (root * length_y * length_z)
    return rho, scale


def local(potential, recovery, stimulus, conductivity):
    devices = lax.axis_size("px") * lax.axis_size("py")
    me = lax.axis_index(AXES)
    rows, length_y, length_z = potential.shape
    length_x = rows * devices
    forth = [(i, (i + 1) % devices) for i in range(devices)]
    back = [((i + 1) % devices, i) for i in range(devices)]
    drive = (
        excite_gain * potential * (potential - threshold) * (1.0 - potential) - potential * recovery
    )
    v_star = potential + time_step * (drive + stimulus)
    rate = base_rate + rate_slope * recovery / (potential + rate_shift)
    recovery_next = recovery + time_step * rate * (
        -recovery - excite_gain * potential * (potential - threshold - 1.0)
    )
    cond = lax.all_to_all(conductivity, "py", split_axis=0, concat_axis=1, tiled=True)

    def above(field):
        return lax.ppermute(field[:1], AXES, back)

    def below(field):
        return lax.ppermute(field[-1:], AXES, forth)

    cond_x = jnp.concatenate([below(cond), cond, above(cond)], 0)
    face_x = 0.5 * (cond_x[1:] + cond_x[:-1])
    face_y = 0.5 * (cond + jnp.roll(cond, -1, 1))
    face_z = 0.5 * (cond + jnp.roll(cond, -1, 2))

    def faces(field):
        padded = jnp.concatenate([below(field), field, above(field)], 0)
        flow_x = face_x * (padded[:-1] - padded[1:])
        flow_y = face_y * (field - jnp.roll(field, -1, 1))
        flow_z = face_z * (field - jnp.roll(field, -1, 2))
        return (
            (flow_x[1:] - flow_x[:-1])
            + (flow_y - jnp.roll(flow_y, 1, 1))
            + (flow_z - jnp.roll(flow_z, 1, 2))
        )

    rho64, scale64 = mode_tables(length_y, length_z)
    rho = jnp.asarray(rho64, jnp.float32)
    scale = jnp.asarray(scale64, jnp.float32)
    cas_y = jnp.asarray(cas_table(length_y), jnp.float32)
    cas_z = jnp.asarray(cas_table(length_z), jnp.float32)
    step_log = jnp.asarray(rows * np.log(rho64), jnp.float32)
    closing = jnp.asarray(1.0 / (1.0 - rho64**length_x), jnp.float32)
    part = length_y // devices
    step_log = lax.dynamic_slice_in_dim(step_log, me * part, part, 0)
    closing = lax.dynamic_slice_in_dim(closing, me * part, part, 0)
    order = np.arange(devices)
    gap = jnp.asarray((order[:, None] - 1 - order[None, :]) % devices, jnp.float32)

    def both(field):
        field = jnp.einsum("xyz,zk->xyk", field, cas_z, precision=lax.Precision.HIGH)
        return jnp.einsum("xyk,yq->xqk", field, cas_y, precision=lax.Precision.HIGH)

    def apply_inverse(residual):
        spectrum = both(residual)
        head = spectrum[rows - 1]
        tail = spectrum[0]
        for i in range(1, rows):
            head = head + rho**i * spectrum[rows - 1 - i]
            tail = tail + rho**i * spectrum[i]
        ends = jnp.stack([head, tail])[None]
        ends = lax.all_to_all(ends, AXES, split_axis=2, concat_axis=0, tiled=True)
        power = jnp.exp(gap[:, :, None, None] * step_log) * closing
        left = jnp.sum(power * ends[None, :, 0], 1)
        right = jnp.sum(jnp.swapaxes(power, 0, 1) * ends[None, :, 1], 1)
        carry = jnp.stack([left, right], 1)
        carry = lax.all_to_all(carry, AXES, split_axis=0, concat_axis=2, tiled=True)
        forward, backward = [None] * rows, [None] * rows
        value = carry[0, 0]
        for i in range(rows):
            value = spectrum[i] + rho * value
            forward[i] = value
        value = carry[0, 1]
        for i in reversed(range(rows)):
            backward[i] = rho * value
            value = spectrum[i] + backward[i]
        return both(jnp.stack([scale * (f + b) for f, b in zip(forward, backward)]))

    field = v_star
    residual = -faces(v_star)
    direction = image = gamma = alpha = None
    for step in range(ITERS):
        precond = apply_inverse(residual)
        applied = mass_rate * precond + faces(precond)
        sums = jnp.stack([jnp.sum(residual * precond), jnp.sum(applied * precond)])
        sums = jnp.sum(lax.all_gather(jnp.broadcast_to(sums[:, None], (2, 128)), AXES), 0)
        gamma_next, delta = sums[0, 0], sums[1, 0]
        if step == 0:
            alpha = gamma_next / delta
            direction, image = precond, applied
        else:
            beta = gamma_next / gamma
            alpha = gamma_next / (delta - beta * gamma_next / alpha)
            direction = precond + beta * direction
            image = applied + beta * image
        gamma = gamma_next
        field = field + alpha * direction
        residual = residual - alpha * image
    return (field, recovery_next)


def bits(count):
    return [1 << n for n in range(count.bit_length() - 1)]


def split(table):
    high = table.astype(jnp.bfloat16)
    low = (table - high.astype(np.float64)).astype(jnp.bfloat16)
    return jnp.asarray(high), jnp.asarray(low)


def parts_of(block):
    high = block.astype(jnp.bfloat16)
    return high, (block - high.astype(jnp.float32)).astype(jnp.bfloat16)


def product(left, right):
    def dot(a, b):
        return jnp.dot(a, b, preferred_element_type=jnp.float32)

    return dot(left[0], right[1]) + dot(left[1], right[0]) + dot(left[0], right[0])


def kernel(
    v_hbm, w_hbm, i_hbm, cond_in, yh_in, yl_in, zh_in, zl_in, rho_in, scale_in, sigma_in,
    pair_in, wrap_in,
    u_ref,
    v_ref, w_ref, i_ref, yh_ref, yl_ref, zh_ref, zl_ref, rho_ref, scale_ref, sigma_ref,
    pair_ref, wrap_ref,
    cond, face_x, face_y, face_z, zs, res, first, imag, spec, mode_h, mode_l, turn_h, turn_l,
    out, both_ends, chip, recv, sol, car, back, carry, dots, mine, gath,
    c_send, c_recv, h_send, h_recv, p_send, p_recv, e_send, e_recv, s_send, s_recv,
    g_send, g_recv, l_sem, r_sem,
):
    count_y = lax.axis_size("py")
    devices = lax.axis_size("px") * count_y
    chips = devices // 2
    my_y = lax.axis_index("py")
    me = lax.axis_index("px") * count_y + my_y
    core = me % 2
    my_chip = me // 2
    rows, length_y, length_z = v_ref.shape
    half = length_y // 2
    part = half // chips
    wide_y = cond_in.shape[1]
    mesh_type = pl.DeviceIdType.MESH

    def device(index):
        return (index // count_y, index % count_y)

    def strip(index):
        return pl.ds(pl.multiple_of(index * part, part), part)

    def remote(source, target, send, recv_sem, index):
        return pltpu.make_async_remote_copy(
            source, target, send, recv_sem, device_id=device(index), device_id_type=mesh_type
        )

    def halo(buffer, base):
        left = (me + devices - 1) % devices
        right = (me + 1) % devices
        return (
            remote(buffer.at[1], buffer.at[rows + 1], h_send.at[base], h_recv.at[base], left),
            remote(
                buffer.at[rows], buffer.at[0], h_send.at[base + 1], h_recv.at[base + 1], right
            ),
        )

    def start_all(make, count):
        for k in range(1, count):
            make(k).start()

    def wait_all(make, count):
        for k in range(1, count):
            make(k).wait()

    def cond_copy(row, k):
        other = (my_y + k) % count_y
        return pltpu.make_async_remote_copy(
            cond_in.at[other * rows + row],
            cond.at[row + 1, pl.ds(pl.multiple_of(my_y * wide_y, 8), wide_y), :],
            c_send.at[row, k], c_recv.at[row, k],
            device_id=(lax.axis_index("px"), other), device_id_type=mesh_type,
        )

    def ends_copy(k):
        other = (my_chip + k) % chips
        return remote(
            chip.at[:, strip(other), :], recv.at[my_chip], e_send.at[k], e_recv.at[k],
            2 * other + core,
        )

    def carry_copy(k):
        other = (my_chip + k) % chips
        return remote(
            sol.at[other], car.at[:, strip(my_chip), :], s_send.at[k], s_recv.at[k],
            2 * other + core,
        )

    def gath_copy(k):
        return remote(mine, gath.at[me], g_send.at[k], g_recv.at[k], (me + k) % devices)

    partner = me + 1 - 2 * core
    pair_ends = remote(out, both_ends.at[core], p_send.at[0], p_recv.at[0], partner)
    pair_carry = remote(back, carry.at[core], p_send.at[1], p_recv.at[1], partner)

    def flux(field, i, low, block):
        at = slice(low, low + block)
        before = slice((low - 8) % length_y, (low - 8) % length_y + 8)
        after = slice((low + block) % length_y, (low + block) % length_y + 8)
        here = field[i + 1, at]
        total = face_x[i + 1, at] * (here - field[i + 2, at]) - face_x[i, at] * (
            field[i, at] - here
        )
        wide = jnp.concatenate([field[i + 1, before], here, field[i + 1, after]], 0)
        drop = wide - pltpu.roll(wide, block + 15, 0)
        flow = jnp.concatenate([face_y[i, before], face_y[i, at]], 0) * drop[: block + 8]
        total = total + (flow[8:] - pltpu.roll(flow, 1, 0)[8:])
        flow = face_z[i, at] * (here - pltpu.roll(here, length_z - 1, 1))
        return at, here, total + (flow - pltpu.roll(flow, 1, 1))

    def row_blocks(block):
        return range(0, length_y, block)

    def local_copy(source, target, index):
        return pltpu.make_async_copy(source, target, l_sem.at[index])

    my_x = lax.axis_index("px")
    size_x = lax.axis_size("px")
    rounds = [(my_x + bit - 2 * bit * (my_x // bit % 2)) * count_y + my_y for bit in bits(size_x)]
    greeted = [my_x * count_y + (my_y + k) % count_y for k in range(1, count_y)] + rounds
    barrier = pltpu.get_barrier_semaphore()
    for other in greeted:
        pl.semaphore_signal(barrier, 1, device_id=device(other), device_id_type=mesh_type)
    pl.semaphore_wait(barrier, len(greeted))

    def tell(n):
        pl.semaphore_signal(r_sem.at[n], 1, device_id=device(rounds[n]), device_id_type=mesh_type)

    with jax.named_scope("issue"):
        for row in (0, rows - 1) + tuple(range(1, rows - 1)):
            for k in range(1, count_y):
                cond_copy(row, k).start()
    own_cond = local_copy(
        cond_in.at[pl.ds(my_y * rows, rows)],
        cond.at[pl.ds(1, rows), pl.ds(pl.multiple_of(my_y * wide_y, 8), wide_y), :],
        0,
    )
    ionic = [
        local_copy(source, target, 1 + n)
        for n, (source, target) in enumerate(((v_hbm, v_ref), (w_hbm, w_ref), (i_hbm, i_ref)))
    ]
    loads = [
        local_copy(source, target, 4 + n)
        for n, (source, target) in enumerate((
            (yh_in, yh_ref), (yl_in, yl_ref), (zh_in, zh_ref), (zl_in, zl_ref),
            (rho_in, rho_ref), (scale_in, scale_ref), (sigma_in, sigma_ref),
            (pair_in, pair_ref), (wrap_in, wrap_ref),
        ))
    ]
    with jax.named_scope("issue_local"):
        for copy in ionic + [own_cond] + loads:
            copy.start()
    with jax.named_scope("ionic_wait"):
        for copy in ionic:
            copy.wait()
    for n in range(len(rounds)):
        tell(n)
        pl.semaphore_wait(r_sem.at[n], 1)
    start = zs.at[0]

    def react(i, _):
        v = v_ref[i]
        drive = excite_gain * v * (v - threshold) * (1.0 - v) - v * w_ref[i]
        v = v + time_step * (drive + i_ref[i])
        v_ref[i] = v
        start[i + 1] = v
        return 0

    lax.fori_loop(0, rows, react, 0)
    field_halo = halo(start, 0)
    for copy in field_halo:
        copy.start()

    def clear(i, _):
        for k in range(1, ITERS):
            zs[k, i + 1] = jnp.zeros((length_y, length_z), jnp.float32)
        return 0

    lax.fori_loop(0, rows, clear, 0)
    with jax.named_scope("loads_wait"):
        own_cond.wait()
        for copy in loads:
            copy.wait()

    def arrive(row):
        for k in range(1, count_y):
            cond_copy(row, k).wait_recv()

    def faces(i):
        here = cond[i + 1]
        face_y[i] = 0.5 * (here + pltpu.roll(here, length_y - 1, 0))
        face_z[i] = 0.5 * (here + pltpu.roll(here, length_z - 1, 1))

    def faces_along(i):
        face_x[i] = 0.5 * (cond[i] + cond[i + 1])

    def begin(i):
        for low in row_blocks(BLOCK):
            at, _, total = flux(start, i, low, BLOCK)
            first[i, at] = -total
            res[i, at] = -total
        ahead_z(i, 0)

    def ahead_z(i, _):
        turned = product(parts_of(res[i]), (zh_ref[...], zl_ref[...]))
        turn_h[i], turn_l[i] = parts_of(turned)
        return 0

    with jax.named_scope("cond_first"):
        arrive(0)
        arrive(rows - 1)
    cond_halo = halo(cond, 2)
    for copy in cond_halo:
        copy.start()
    faces(0)
    faces(rows - 1)
    with jax.named_scope("cond_1"):
        arrive(1)
    faces(1)
    faces_along(1)
    for copy in field_halo:
        copy.wait()

    def stream(t, _):
        arrive(t)
        faces(t)
        faces_along(t)
        begin(t - 1)
        return 0

    with jax.named_scope("cond_stream"):
        lax.fori_loop(2, rows - 1, stream, 0)
    with jax.named_scope("cond_halo"):
        for copy in cond_halo:
            copy.wait()
    with jax.named_scope("cond_tail"):
        faces_along(rows - 1)
        faces_along(0)
        faces_along(rows)
        begin(rows - 2)
        begin(0)
        begin(rows - 1)
        for row in range(rows):
            for k in range(1, count_y):
                cond_copy(row, k).wait_send()

    def products(step):
        block = 8
        per = length_y // block

        def body(t, sums):
            i = t // per
            at = pl.ds(pl.multiple_of((t % per) * block, block), block)
            image = imag[i, at, :]
            fresh = [zs[j, i + 1, at, :] for j in range(ITERS)]
            sums = [total + z * image for total, z in zip(sums, fresh)] + [
                sums[ITERS] + zs[step, i + 1, at, :] * first[i, at, :]
            ]
            return tuple(sums)

        zero = jnp.zeros((block, length_z), jnp.float32)
        sums = lax.fori_loop(0, rows * per, body, (zero,) * (ITERS + 1), unroll=16)
        keep(step, sums)

    def keep(step, sums):
        for m, total in enumerate(sums):
            dots[step, m] = sum(total[:, c : c + 128] for c in range(0, length_z, 128))

    def block_ends(where, side, target, block=8):
        def body(b, _):
            low = pl.multiple_of(b * block, block)
            at = pl.ds(pl.multiple_of(side * half + low, block), block)
            rho = rho_ref[at, :]
            planes = [spec[i, at, :] for i in range(rows)]
            head, tail = planes[0], planes[rows - 1]
            for i in range(1, rows):
                head = planes[i] + rho * head
                tail = planes[rows - 1 - i] + rho * tail
            target[0, pl.ds(low, block), :] = head
            target[1, pl.ds(low, block), :] = tail
            return 0

        lax.fori_loop(0, half // block, body, 0, unroll=2)

    def chip_ends(block=8):
        def body(b, _):
            low = pl.multiple_of(b * block, block)
            at = pl.ds(low, block)
            sigma = sigma_ref[pl.ds(pl.multiple_of(core * half + low, block), block), :]
            chip[0, at, :] = both_ends[1, 0, at, :] + sigma * both_ends[0, 0, at, :]
            chip[1, at, :] = both_ends[0, 1, at, :] + sigma * both_ends[1, 1, at, :]
            return 0

        lax.fori_loop(0, half // block, body, 0, unroll=4)

    def core_carries(block=8):
        def body(b, _):
            low = pl.multiple_of(b * block, block)
            at = pl.ds(low, block)
            sigma = sigma_ref[pl.ds(pl.multiple_of(core * half + low, block), block), :]
            left, right = car[0, at, :], car[1, at, :]
            after = both_ends[1, 1, at, :] + sigma * right
            before = both_ends[0, 0, at, :] + sigma * left
            carry[core, 0, at, :] = jnp.where(core == 0, left, before)
            carry[core, 1, at, :] = jnp.where(core == 0, after, right)
            back[0, at, :] = jnp.where(core == 0, before, left)
            back[1, at, :] = jnp.where(core == 0, right, after)
            return 0

        lax.fori_loop(0, half // block, body, 0, unroll=4)

    def recur(side, block=16, wide=128):
        def body(b, _):
            low = pl.multiple_of(b * block, block)
            at = pl.ds(pl.multiple_of(side * half + low, block), block)
            for c in range(0, length_z, wide):
                cut = slice(c, c + wide)
                rho = rho_ref[at, cut]
                scale = scale_ref[at, cut]
                left = carry[side, 0, pl.ds(low, block), cut]
                right = carry[side, 1, pl.ds(low, block), cut]
                planes = [spec[i, at, cut] for i in range(rows)]
                ahead = [None] * rows
                value = right
                for i in reversed(range(rows)):
                    ahead[i] = rho * value
                    value = planes[i] + ahead[i]
                modes = [left + rho * value]
                value = left
                for i in range(rows):
                    value = planes[i] + rho * value
                    modes.append(value + ahead[i])
                modes.append(right + rho * value)
                for i, mode in enumerate(modes):
                    mode_h[i, at, cut], mode_l[i, at, cut] = parts_of(scale * mode)
            return 0

        lax.fori_loop(0, half // block, body, 0)

    def solve():
        own = pl.ds(pl.multiple_of(core * half + my_chip * part, part), part)
        sigma = pair_ref[own, :]
        close = 1.0 / (1.0 - wrap_ref[own, :])
        zero = jnp.zeros_like(sigma)

        def sums(b, pair):
            return (
                recv[b, 0] + sigma * pair[0],
                recv[chips - 1 - b, 1] + sigma * pair[1],
            )

        pair = lax.fori_loop(0, chips, sums, (zero, zero), unroll=4)

        def place(b, pair):
            sol[b, 0] = pair[0]
            sol[chips - 1 - b, 1] = pair[1]
            return sums(b, pair)

        lax.fori_loop(0, chips, place, (pair[0] * close, pair[1] * close), unroll=4)

    def ahead_y(side):
        at = pl.ds(pl.multiple_of(side * half, half), half)

        def body(i, _):
            spec[i, at, :] = product((yh_ref[at, :], yl_ref[at, :]), (turn_h[i], turn_l[i]))
            return 0

        lax.fori_loop(0, rows, body, 0, unroll=4)

    def inverse_z(side):
        at = pl.ds(pl.multiple_of(side * half, half), half)

        def body(i, _):
            modes = (mode_h[i, at, :], mode_l[i, at, :])
            turn_h[i, at, :], turn_l[i, at, :] = parts_of(
                product(modes, (zh_ref[...], zl_ref[...]))
            )
            return 0

        lax.fori_loop(0, rows + 2, body, 0, unroll=5)

    def iteration(step, _):
        @pl.when(step > 0)
        def _():
            with jax.named_scope("ahead_z"):
                lax.fori_loop(0, rows, ahead_z, 0, unroll=4)

        with jax.named_scope("ahead_y1"):
            ahead_y(1 - core)
        with jax.named_scope("ends1"):
            block_ends(spec, 1 - core, out)
        pair_ends.start()
        with jax.named_scope("ahead_y2"):
            ahead_y(core)
        with jax.named_scope("ends2"):
            block_ends(spec, core, both_ends.at[core])
        with jax.named_scope("pair_wait"):
            pair_ends.wait()
        chip_ends()
        with jax.named_scope("ends_start"):
            start_all(ends_copy, chips)
            recv[my_chip] = chip[:, strip(my_chip), :]

        @pl.when(step > 0)
        def _():
            products(step - 1)

        with jax.named_scope("ends_wait"):
            wait_all(ends_copy, chips)
        with jax.named_scope("solve"):
            solve()
            start_all(carry_copy, chips)
            car[:, strip(my_chip), :] = sol[my_chip]
        with jax.named_scope("carry_wait"):
            wait_all(carry_copy, chips)
        with jax.named_scope("recur1"):
            core_carries()
            pair_carry.start()
            recur(core)
        with jax.named_scope("inverse_z1"):
            inverse_z(core)
        with jax.named_scope("carry_pair_wait"):
            pair_carry.wait()
        with jax.named_scope("recur2"):
            recur(1 - core)
        with jax.named_scope("inverse_z2"):
            inverse_z(1 - core)

        def inverse(i, _):
            zs[step, i] = product((yh_ref[...], yl_ref[...]), (turn_h[i], turn_l[i]))
            return 0

        with jax.named_scope("inverse_y"):
            lax.fori_loop(0, rows + 2, inverse, 0, unroll=5)
        node = jnp.where(
            step == 0, 1.0 / nodes[0], jnp.where(step == 1, 1.0 / nodes[1], 1.0 / nodes[2])
        )
        latest = zs.at[step]

        def apply(i, _):
            for low in row_blocks(BLOCK):
                at, here, total = flux(latest, i, low, BLOCK)
                image = mass_rate * here + total
                imag[i, at] = image
                res[i, at] = res[i, at] - node * image
            return 0

        def folded(value):
            return jnp.sum(value.reshape(value.shape[0] // 8, 8, length_z), 0)

        def apply_last(i, sums):
            for low in row_blocks(BLOCK):
                at, here, total = flux(latest, i, low, BLOCK)
                image = mass_rate * here + total
                fresh = [zs[j, i + 1, at] * image for j in range(ITERS)] + [here * first[i, at]]
                sums = tuple(old + folded(new) for old, new in zip(sums, fresh))
            return sums

        @pl.when(step < ITERS - 1)
        def _():
            with jax.named_scope("apply"):
                lax.fori_loop(0, rows, apply, 0)

        @pl.when(step == ITERS - 1)
        def _():
            with jax.named_scope("apply_last"):
                zero = jnp.zeros((8, length_z), jnp.float32)
                keep(step, lax.fori_loop(0, rows, apply_last, (zero,) * (ITERS + 1)))

        return 0

    lax.fori_loop(0, ITERS, iteration, 0)
    lane = lax.broadcasted_iota(jnp.int32, (1, 128), 1)
    packed = jnp.zeros((1, 128), jnp.float32)
    for k in range(ITERS):
        for m in range(ITERS + 1):
            total = jnp.sum(dots[k, m], keepdims=True)
            packed = jnp.where(lane == k * (ITERS + 1) + m, total, packed)
    mine[...] = packed
    with jax.named_scope("gather"):
        start_all(gath_copy, devices)
        gath[me] = mine[...]
        wait_all(gath_copy, devices)
    total = jnp.sum(gath[...], 0)

    def entry(k, m):
        index = k * (ITERS + 1) + m
        return total[:, index : index + 1]

    lower = [[None] * ITERS for _ in range(ITERS)]
    inverse_pivot, partial, pivots = [], [], []
    for k in range(ITERS):
        pivot = entry(k, k)
        value = entry(k, ITERS)
        for j in range(k):
            pivot = pivot - lower[k][j] * lower[k][j] * pivots[j]
            value = value - lower[k][j] * partial[j]
        pivots.append(pivot)
        usable = pivot > pivot_floor * entry(k, k)
        inverse_pivot.append(jnp.where(usable, 1.0 / jnp.where(usable, pivot, 1.0), 0.0))
        partial.append(value)
        for i in range(k + 1, ITERS):
            value = entry(i, k)
            for j in range(k):
                value = value - lower[i][j] * lower[k][j] * pivots[j]
            lower[i][k] = value * inverse_pivot[k]
    coefs = [None] * ITERS
    for k in reversed(range(ITERS)):
        value = partial[k] * inverse_pivot[k]
        for i in range(k + 1, ITERS):
            value = value - lower[i][k] * coefs[i]
        coefs[k] = value

    def finish(i, _):
        for low in row_blocks(BLOCK):
            at = slice(low, low + BLOCK)
            value = v_ref[i, at]
            for k in range(ITERS):
                value = value + coefs[k] * zs[k, i + 1, at]
            u_ref[i, at] = value
        return 0

    with jax.named_scope("finish"):
        lax.fori_loop(0, rows, finish, 0)


def fused(potential, recovery, stimulus, conductivity):
    count_y = lax.axis_size("py")
    devices = lax.axis_size("px") * count_y
    rows, length_y, length_z = potential.shape
    part = length_y // devices
    size_x = lax.axis_size("px")
    if size_x & (size_x - 1) or count_y % 2 or part % 8 or length_z % 128 or conductivity.shape[1] % 8:
        return local(potential, recovery, stimulus, conductivity)
    rate = base_rate + rate_slope * recovery / (potential + rate_shift)
    recovery_next = recovery + time_step * rate * (
        -recovery - excite_gain * potential * (potential - threshold - 1.0)
    )
    rho, scale = mode_tables(length_y, length_z)
    tables = split(cas_table(length_y)) + split(cas_table(length_z))
    tables += tuple(
        jnp.asarray(table, jnp.float32)
        for table in (
            rho, scale, rho**rows, rho ** (2 * rows), rho ** (rows * devices)
        )
    )
    plane = (length_y, length_z)
    whole = (rows,) + plane
    half = (2, length_y // 2, length_z)
    chips = devices // 2

    def vmem(shape, dtype=jnp.float32):
        return pltpu.VMEM(shape, dtype)

    dma = pltpu.SemaphoreType.DMA
    padded = (rows + 2,) + plane
    square = [vmem((n, n), jnp.bfloat16) for n in (length_y, length_y, length_z, length_z)]
    slots = (chips, 2, part, length_z)
    field = pl.pallas_call(
        kernel,
        out_shape=jax.ShapeDtypeStruct(whole, jnp.float32),
        in_specs=[pl.BlockSpec(memory_space=pl.ANY)] * 13,
        out_specs=pl.BlockSpec(memory_space=pltpu.VMEM),
        scratch_shapes=[
            vmem(whole), vmem(whole), vmem(whole), *square,
            *(vmem(plane) for _ in range(5)),
            vmem(padded), vmem((rows + 1,) + plane), vmem(whole), vmem(whole),
            vmem((ITERS,) + padded), vmem(whole), vmem(whole), vmem(whole), vmem(whole),
            vmem(padded, jnp.bfloat16), vmem(padded, jnp.bfloat16),
            vmem(padded, jnp.bfloat16), vmem(padded, jnp.bfloat16),
            vmem(half), vmem((2,) + half), vmem(half), vmem(slots), vmem(slots), vmem(half),
            vmem(half), vmem((2,) + half),
            vmem((ITERS, ITERS + 1, 8, 128)), vmem((1, 128)), vmem((devices, 1, 128)),
            dma((rows, count_y)), dma((rows, count_y)), dma((4,)), dma((4,)), dma((2,)), dma((2,)),
            dma((chips,)), dma((chips,)), dma((chips,)), dma((chips,)),
            dma((devices,)), dma((devices,)), dma((13,)),
            pltpu.SemaphoreType.REGULAR((len(bits(size_x)),)),
        ],
        compiler_params=pltpu.CompilerParams(
            collective_id=0, has_side_effects=True, vmem_limit_bytes=60 * 1024 * 1024
        ),
    )(potential, recovery, stimulus, conductivity, *tables)
    return (field, recovery_next)


def solution(mesh):
    in_specs = (
        P(AXES, None, None),
        P(AXES, None, None),
        P(AXES, None, None),
        P("px", "py", None),
    )
    out_specs = (P(AXES, None, None), P(AXES, None, None))
    return jax.shard_map(fused, mesh=mesh, in_specs=in_specs, out_specs=out_specs, check_vma=False)
```

```python
import math

import jax
import jax.numpy as jnp
import numpy as np
from jax import lax
from jax.experimental import pallas as pl
from jax.experimental.pallas import tpu as pltpu
from jax.sharding import PartitionSpec as P

ITERS = 4

mass_rate = 0.01
excite_gain = 8.0
threshold = 0.15
base_rate = 0.002
rate_slope = 0.2
rate_shift = 0.3
time_step = 0.1
nodes = (2.6, 1.0, 4.0)
BLOCK = 64
pivot_floor = 1e-6
AXES = ("px", "py")


def cas_table(length):
    steps = np.arange(length)
    angle = 2.0 * math.pi / length * (steps[:, None] * steps[None, :] % length)
    return np.cos(angle) + np.sin(angle)


def wave_term(length):
    return 2.0 - 2.0 * np.cos(2.0 * math.pi / length * np.arange(length))


def mode_tables(length_y, length_z):
    shift = mass_rate + wave_term(length_y)[:, None] + wave_term(length_z)[None, :]
    root = np.sqrt(shift * (4.0 + shift))
    rho = 2.0 / (2.0 + shift + root)
    scale = 1.0 / (root * length_y * length_z)
    return rho, scale


def local(potential, recovery, stimulus, conductivity):
    devices = lax.axis_size("px") * lax.axis_size("py")
    me = lax.axis_index(AXES)
    rows, length_y, length_z = potential.shape
    length_x = rows * devices
    forth = [(i, (i + 1) % devices) for i in range(devices)]
    back = [((i + 1) % devices, i) for i in range(devices)]
    drive = (
        excite_gain * potential * (potential - threshold) * (1.0 - potential) - potential * recovery
    )
    v_star = potential + time_step * (drive + stimulus)
    rate = base_rate + rate_slope * recovery / (potential + rate_shift)
    recovery_next = recovery + time_step * rate * (
        -recovery - excite_gain * potential * (potential - threshold - 1.0)
    )
    cond = lax.all_to_all(conductivity, "py", split_axis=0, concat_axis=1, tiled=True)

    def above(field):
        return lax.ppermute(field[:1], AXES, back)

    def below(field):
        return lax.ppermute(field[-1:], AXES, forth)

    cond_x = jnp.concatenate([below(cond), cond, above(cond)], 0)
    face_x = 0.5 * (cond_x[1:] + cond_x[:-1])
    face_y = 0.5 * (cond + jnp.roll(cond, -1, 1))
    face_z = 0.5 * (cond + jnp.roll(cond, -1, 2))

    def faces(field):
        padded = jnp.concatenate([below(field), field, above(field)], 0)
        flow_x = face_x * (padded[:-1] - padded[1:])
        flow_y = face_y * (field - jnp.roll(field, -1, 1))
        flow_z = face_z * (field - jnp.roll(field, -1, 2))
        return (
            (flow_x[1:] - flow_x[:-1])
            + (flow_y - jnp.roll(flow_y, 1, 1))
            + (flow_z - jnp.roll(flow_z, 1, 2))
        )

    rho64, scale64 = mode_tables(length_y, length_z)
    rho = jnp.asarray(rho64, jnp.float32)
    scale = jnp.asarray(scale64, jnp.float32)
    cas_y = jnp.asarray(cas_table(length_y), jnp.float32)
    cas_z = jnp.asarray(cas_table(length_z), jnp.float32)
    step_log = jnp.asarray(rows * np.log(rho64), jnp.float32)
    closing = jnp.asarray(1.0 / (1.0 - rho64**length_x), jnp.float32)
    part = length_y // devices
    step_log = lax.dynamic_slice_in_dim(step_log, me * part, part, 0)
    closing = lax.dynamic_slice_in_dim(closing, me * part, part, 0)
    order = np.arange(devices)
    gap = jnp.asarray((order[:, None] - 1 - order[None, :]) % devices, jnp.float32)

    def both(field):
        field = jnp.einsum("xyz,zk->xyk", field, cas_z, precision=lax.Precision.HIGH)
        return jnp.einsum("xyk,yq->xqk", field, cas_y, precision=lax.Precision.HIGH)

    def apply_inverse(residual):
        spectrum = both(residual)
        head = spectrum[rows - 1]
        tail = spectrum[0]
        for i in range(1, rows):
            head = head + rho**i * spectrum[rows - 1 - i]
            tail = tail + rho**i * spectrum[i]
        ends = jnp.stack([head, tail])[None]
        ends = lax.all_to_all(ends, AXES, split_axis=2, concat_axis=0, tiled=True)
        power = jnp.exp(gap[:, :, None, None] * step_log) * closing
        left = jnp.sum(power * ends[None, :, 0], 1)
        right = jnp.sum(jnp.swapaxes(power, 0, 1) * ends[None, :, 1], 1)
        carry = jnp.stack([left, right], 1)
        carry = lax.all_to_all(carry, AXES, split_axis=0, concat_axis=2, tiled=True)
        forward, backward = [None] * rows, [None] * rows
        value = carry[0, 0]
        for i in range(rows):
            value = spectrum[i] + rho * value
            forward[i] = value
        value = carry[0, 1]
        for i in reversed(range(rows)):
            backward[i] = rho * value
            value = spectrum[i] + backward[i]
        return both(jnp.stack([scale * (f + b) for f, b in zip(forward, backward)]))

    field = v_star
    residual = -faces(v_star)
    direction = image = gamma = alpha = None
    for step in range(ITERS):
        precond = apply_inverse(residual)
        applied = mass_rate * precond + faces(precond)
        sums = jnp.stack([jnp.sum(residual * precond), jnp.sum(applied * precond)])
        sums = jnp.sum(lax.all_gather(jnp.broadcast_to(sums[:, None], (2, 128)), AXES), 0)
        gamma_next, delta = sums[0, 0], sums[1, 0]
        if step == 0:
            alpha = gamma_next / delta
            direction, image = precond, applied
        else:
            beta = gamma_next / gamma
            alpha = gamma_next / (delta - beta * gamma_next / alpha)
            direction = precond + beta * direction
            image = applied + beta * image
        gamma = gamma_next
        field = field + alpha * direction
        residual = residual - alpha * image
    return (field, recovery_next)


def bits(count):
    return [1 << n for n in range(count.bit_length() - 1)]


def split(table):
    high = table.astype(jnp.bfloat16)
    low = (table - high.astype(np.float64)).astype(jnp.bfloat16)
    return jnp.asarray(high), jnp.asarray(low)


def parts_of(block):
    high = block.astype(jnp.bfloat16)
    return high, (block - high.astype(jnp.float32)).astype(jnp.bfloat16)


def product(left, right):
    def dot(a, b):
        return jnp.dot(a, b, preferred_element_type=jnp.float32)

    return dot(left[0], right[1]) + dot(left[1], right[0]) + dot(left[0], right[0])


def kernel(
    v_hbm, w_hbm, i_hbm, cond_in, yh_in, yl_in, zh_in, zl_in, rho_in, scale_in, sigma_in,
    pair_in, wrap_in,
    u_ref,
    v_ref, w_ref, i_ref, yh_ref, yl_ref, zh_ref, zl_ref, rho_ref, scale_ref, sigma_ref,
    pair_ref, wrap_ref,
    cond, face_x, face_y, face_z, zs, res, first, imag, spec, mode_h, mode_l, turn_h, turn_l,
    out, both_ends, chip, recv, sol, car, back, carry, dots, mine, gath,
    c_send, c_recv, h_send, h_recv, p_send, p_recv, e_send, e_recv, s_send, s_recv,
    g_send, g_recv, l_sem, r_sem,
):
    count_y = lax.axis_size("py")
    devices = lax.axis_size("px") * count_y
    chips = devices // 2
    my_y = lax.axis_index("py")
    me = lax.axis_index("px") * count_y + my_y
    core = me % 2
    my_chip = me // 2
    rows, length_y, length_z = v_ref.shape
    half = length_y // 2
    part = half // chips
    quarter = half // 2
    owners = chips // 2
    wide_y = cond_in.shape[1]
    mesh_type = pl.DeviceIdType.MESH

    def device(index):
        return (index // count_y, index % count_y)

    def tint(index):
        return (index // 2 + index // 4) % 2

    def owner(chunk, index):
        return 2 * index + (chunk + tint(2 * index)) % 2

    my_chunk = (my_chip + tint(my_chip)) % 2
    my_strip = my_chunk * owners + my_chip // 2

    def strip(index):
        return pl.ds(pl.multiple_of(index * part, part), part)

    def remote(source, target, send, recv_sem, index):
        return pltpu.make_async_remote_copy(
            source, target, send, recv_sem, device_id=device(index), device_id_type=mesh_type
        )

    def halo(buffer, base):
        left = (me + devices - 1) % devices
        right = (me + 1) % devices
        return (
            remote(buffer.at[1], buffer.at[rows + 1], h_send.at[base], h_recv.at[base], left),
            remote(
                buffer.at[rows], buffer.at[0], h_send.at[base + 1], h_recv.at[base + 1], right
            ),
        )

    def start_all(make, count):
        for k in range(1, count):
            make(k).start()

    def wait_all(make, count):
        for k in range(1, count):
            make(k).wait()

    def cond_copy(row, k):
        other = (my_y + k) % count_y
        return pltpu.make_async_remote_copy(
            cond_in.at[other * rows + row],
            cond.at[row + 1, pl.ds(pl.multiple_of(my_y * wide_y, 8), wide_y), :],
            c_send.at[row, k], c_recv.at[row, k],
            device_id=(lax.axis_index("px"), other), device_id_type=mesh_type,
        )

    def ends_copy(chunk, index, source):
        at = chunk * owners + index
        return remote(
            chip.at[:, strip(at), :], recv.at[source], e_send.at[at], e_recv.at[source],
            2 * owner(chunk, index) + core,
        )

    def carry_copy(other, source, strip_at):
        return remote(
            sol.at[other], car.at[:, strip(strip_at), :], s_send.at[other], s_recv.at[source],
            2 * other + core,
        )

    def unless_mine(other, action):
        pl.when(other != my_chip)(action)

    def ends_start(chunk):
        for index in range(owners):
            index = (my_chip // 2 + index) % owners
            unless_mine(owner(chunk, index), ends_copy(chunk, index, my_chip).start)

    def ends_wait():
        for chunk in range(2):
            for index in range(owners):
                unless_mine(owner(chunk, index), ends_copy(chunk, index, my_chip).wait_send)
        for source in range(chips):
            unless_mine(source, ends_copy(0, 0, source).wait_recv)

    def carry_start():
        for k in range(1, chips):
            carry_copy((my_chip + k) % chips, my_chip, my_strip).start()

    def carry_wait(chunk):
        for index in range(owners):
            other = owner(chunk, index)
            unless_mine(other, carry_copy(0, other, chunk * owners + index).wait_recv)

    def carry_sent():
        for k in range(1, chips):
            carry_copy((my_chip + k) % chips, my_chip, my_strip).wait_send()

    def gath_copy(k):
        return remote(mine, gath.at[me], g_send.at[k], g_recv.at[k], (me + k) % devices)

    partner = me + 1 - 2 * core
    pair_ends = remote(out, both_ends.at[core], p_send.at[0], p_recv.at[0], partner)
    pair_carry = []
    for n in range(2):
        cut = pl.ds(n * quarter, quarter)
        pair_carry.append(remote(
            back.at[:, cut, :], carry.at[core, :, cut, :], p_send.at[1 + n], p_recv.at[1 + n],
            partner,
        ))

    def flux(field, i, low, block):
        at = slice(low, low + block)
        before = slice((low - 8) % length_y, (low - 8) % length_y + 8)
        after = slice((low + block) % length_y, (low + block) % length_y + 8)
        here = field[i + 1, at]
        total = face_x[i + 1, at] * (here - field[i + 2, at]) - face_x[i, at] * (
            field[i, at] - here
        )
        wide = jnp.concatenate([field[i + 1, before], here, field[i + 1, after]], 0)
        drop = wide - pltpu.roll(wide, block + 15, 0)
        flow = jnp.concatenate([face_y[i, before], face_y[i, at]], 0) * drop[: block + 8]
        total = total + (flow[8:] - pltpu.roll(flow, 1, 0)[8:])
        flow = face_z[i, at] * (here - pltpu.roll(here, length_z - 1, 1))
        return at, here, total + (flow - pltpu.roll(flow, 1, 1))

    def row_blocks(block):
        return range(0, length_y, block)

    def local_copy(source, target, index):
        return pltpu.make_async_copy(source, target, l_sem.at[index])

    my_x = lax.axis_index("px")
    size_x = lax.axis_size("px")
    rounds = [(my_x + bit - 2 * bit * (my_x // bit % 2)) * count_y + my_y for bit in bits(size_x)]
    greeted = [my_x * count_y + (my_y + k) % count_y for k in range(1, count_y)] + rounds
    barrier = pltpu.get_barrier_semaphore()
    for other in greeted:
        pl.semaphore_signal(barrier, 1, device_id=device(other), device_id_type=mesh_type)
    pl.semaphore_wait(barrier, len(greeted))

    def tell(n):
        pl.semaphore_signal(r_sem.at[n], 1, device_id=device(rounds[n]), device_id_type=mesh_type)

    with jax.named_scope("issue"):
        for row in (0, rows - 1) + tuple(range(1, rows - 1)):
            for k in range(1, count_y):
                cond_copy(row, k).start()
    own_cond = local_copy(
        cond_in.at[pl.ds(my_y * rows, rows)],
        cond.at[pl.ds(1, rows), pl.ds(pl.multiple_of(my_y * wide_y, 8), wide_y), :],
        0,
    )
    ionic = [
        local_copy(source, target, 1 + n)
        for n, (source, target) in enumerate(((v_hbm, v_ref), (w_hbm, w_ref), (i_hbm, i_ref)))
    ]
    loads = [
        local_copy(source, target, 4 + n)
        for n, (source, target) in enumerate((
            (yh_in, yh_ref), (yl_in, yl_ref), (zh_in, zh_ref), (zl_in, zl_ref),
            (rho_in, rho_ref), (scale_in, scale_ref), (sigma_in, sigma_ref),
            (pair_in, pair_ref), (wrap_in, wrap_ref),
        ))
    ]
    with jax.named_scope("issue_local"):
        for copy in ionic + [own_cond] + loads:
            copy.start()
    with jax.named_scope("ionic_wait"):
        for copy in ionic:
            copy.wait()
    for n in range(len(rounds)):
        tell(n)
        pl.semaphore_wait(r_sem.at[n], 1)
    start = zs.at[0]

    def react(i, _):
        v = v_ref[i]
        drive = excite_gain * v * (v - threshold) * (1.0 - v) - v * w_ref[i]
        v = v + time_step * (drive + i_ref[i])
        v_ref[i] = v
        start[i + 1] = v
        return 0

    lax.fori_loop(0, rows, react, 0)
    field_halo = halo(start, 0)
    for copy in field_halo:
        copy.start()

    def clear(i, _):
        for k in range(1, ITERS):
            zs[k, i + 1] = jnp.zeros((length_y, length_z), jnp.float32)
        return 0

    lax.fori_loop(0, rows, clear, 0)
    with jax.named_scope("loads_wait"):
        own_cond.wait()
        for copy in loads:
            copy.wait()

    def arrive(row):
        for k in range(1, count_y):
            cond_copy(row, k).wait_recv()

    def faces(i):
        here = cond[i + 1]
        face_y[i] = 0.5 * (here + pltpu.roll(here, length_y - 1, 0))
        face_z[i] = 0.5 * (here + pltpu.roll(here, length_z - 1, 1))

    def faces_along(i):
        face_x[i] = 0.5 * (cond[i] + cond[i + 1])

    def begin(i):
        for low in row_blocks(BLOCK):
            at, _, total = flux(start, i, low, BLOCK)
            first[i, at] = -total
            res[i, at] = -total
        ahead_z(i, 0)

    def ahead_z(i, _):
        turned = product(parts_of(res[i]), (zh_ref[...], zl_ref[...]))
        turn_h[i], turn_l[i] = parts_of(turned)
        return 0

    with jax.named_scope("cond_first"):
        arrive(0)
        arrive(rows - 1)
    cond_halo = halo(cond, 2)
    for copy in cond_halo:
        copy.start()
    faces(0)
    faces(rows - 1)
    with jax.named_scope("cond_1"):
        arrive(1)
    faces(1)
    faces_along(1)
    for copy in field_halo:
        copy.wait()

    def stream(t, _):
        arrive(t)
        faces(t)
        faces_along(t)
        begin(t - 1)
        return 0

    with jax.named_scope("cond_stream"):
        lax.fori_loop(2, rows - 1, stream, 0)
    with jax.named_scope("cond_halo"):
        for copy in cond_halo:
            copy.wait()
    with jax.named_scope("cond_tail"):
        faces_along(rows - 1)
        faces_along(0)
        faces_along(rows)
        begin(rows - 2)
        begin(0)
        begin(rows - 1)
        for row in range(rows):
            for k in range(1, count_y):
                cond_copy(row, k).wait_send()

    def products(step):
        block = 8
        per = length_y // block

        def body(t, sums):
            i = t // per
            at = pl.ds(pl.multiple_of((t % per) * block, block), block)
            image = imag[i, at, :]
            fresh = [zs[j, i + 1, at, :] for j in range(ITERS)]
            sums = [total + z * image for total, z in zip(sums, fresh)] + [
                sums[ITERS] + zs[step, i + 1, at, :] * first[i, at, :]
            ]
            return tuple(sums)

        zero = jnp.zeros((block, length_z), jnp.float32)
        sums = lax.fori_loop(0, rows * per, body, (zero,) * (ITERS + 1), unroll=16)
        keep(step, sums)

    def keep(step, sums):
        for m, total in enumerate(sums):
            dots[step, m] = sum(total[:, c : c + 128] for c in range(0, length_z, 128))

    def block_ends(where, side, target, block=8):
        def body(b, _):
            low = pl.multiple_of(b * block, block)
            at = pl.ds(pl.multiple_of(side * half + low, block), block)
            rho = rho_ref[at, :]
            planes = [spec[i, at, :] for i in range(rows)]
            head, tail = planes[0], planes[rows - 1]
            for i in range(1, rows):
                head = planes[i] + rho * head
                tail = planes[rows - 1 - i] + rho * tail
            target[0, pl.ds(low, block), :] = head
            target[1, pl.ds(low, block), :] = tail
            return 0

        lax.fori_loop(0, half // block, body, 0, unroll=2)

    def chip_ends(chunk, block=8):
        def body(b, _):
            low = pl.multiple_of(chunk * quarter + b * block, block)
            at = pl.ds(low, block)
            sigma = sigma_ref[pl.ds(pl.multiple_of(core * half + low, block), block), :]
            chip[0, at, :] = both_ends[1, 0, at, :] + sigma * both_ends[0, 0, at, :]
            chip[1, at, :] = both_ends[0, 1, at, :] + sigma * both_ends[1, 1, at, :]
            return 0

        lax.fori_loop(0, quarter // block, body, 0, unroll=4)

    def core_carries(chunk, block=8):
        def body(b, _):
            low = pl.multiple_of(chunk * quarter + b * block, block)
            at = pl.ds(low, block)
            sigma = sigma_ref[pl.ds(pl.multiple_of(core * half + low, block), block), :]
            left, right = car[0, at, :], car[1, at, :]
            after = both_ends[1, 1, at, :] + sigma * right
            before = both_ends[0, 0, at, :] + sigma * left
            carry[core, 0, at, :] = jnp.where(core == 0, left, before)
            carry[core, 1, at, :] = jnp.where(core == 0, after, right)
            back[0, at, :] = jnp.where(core == 0, before, left)
            back[1, at, :] = jnp.where(core == 0, right, after)
            return 0

        lax.fori_loop(0, quarter // block, body, 0, unroll=4)

    def recur(side, chunk, block=16, wide=128):
        def body(b, _):
            low = pl.multiple_of(chunk * quarter + b * block, block)
            at = pl.ds(pl.multiple_of(side * half + low, block), block)
            for c in range(0, length_z, wide):
                cut = slice(c, c + wide)
                rho = rho_ref[at, cut]
                scale = scale_ref[at, cut]
                left = carry[side, 0, pl.ds(low, block), cut]
                right = carry[side, 1, pl.ds(low, block), cut]
                planes = [spec[i, at, cut] for i in range(rows)]
                ahead = [None] * rows
                value = right
                for i in reversed(range(rows)):
                    ahead[i] = rho * value
                    value = planes[i] + ahead[i]
                modes = [left + rho * value]
                value = left
                for i in range(rows):
                    value = planes[i] + rho * value
                    modes.append(value + ahead[i])
                modes.append(right + rho * value)
                for i, mode in enumerate(modes):
                    mode_h[i, at, cut], mode_l[i, at, cut] = parts_of(scale * mode)
            return 0

        lax.fori_loop(0, quarter // block, body, 0)

    def solve():
        own = pl.ds(pl.multiple_of(core * half + my_strip * part, part), part)
        sigma = pair_ref[own, :]
        close = 1.0 / (1.0 - wrap_ref[own, :])
        zero = jnp.zeros_like(sigma)

        def sums(b, pair):
            return (
                recv[b, 0] + sigma * pair[0],
                recv[chips - 1 - b, 1] + sigma * pair[1],
            )

        pair = lax.fori_loop(0, chips, sums, (zero, zero), unroll=4)

        def place(b, pair):
            sol[b, 0] = pair[0]
            sol[chips - 1 - b, 1] = pair[1]
            return sums(b, pair)

        lax.fori_loop(0, chips, place, (pair[0] * close, pair[1] * close), unroll=4)

    def ahead_y(side):
        at = pl.ds(pl.multiple_of(side * half, half), half)

        def body(i, _):
            spec[i, at, :] = product((yh_ref[at, :], yl_ref[at, :]), (turn_h[i], turn_l[i]))
            return 0

        lax.fori_loop(0, rows, body, 0, unroll=4)

    def inverse_z(side, chunk):
        at = pl.ds(pl.multiple_of(side * half + chunk * quarter, quarter), quarter)

        group = (rows + 2) // 2

        def body(g, _):
            planes = pl.ds(g * group, group)
            shape = (group, quarter, length_z)
            modes = tuple(
                mode[planes, at, :].reshape(group * quarter, length_z) for mode in (mode_h, mode_l)
            )
            high, low = parts_of(product(modes, (zh_ref[...], zl_ref[...])))
            turn_h[planes, at, :] = high.reshape(shape)
            turn_l[planes, at, :] = low.reshape(shape)
            return 0

        lax.fori_loop(0, 2, body, 0, unroll=True)

    def iteration(step, _):
        @pl.when(step > 0)
        def _():
            with jax.named_scope("ahead_z"):
                lax.fori_loop(0, rows, ahead_z, 0, unroll=4)

        with jax.named_scope("ahead_y1"):
            ahead_y(1 - core)
        with jax.named_scope("ends1"):
            block_ends(spec, 1 - core, out)
        pair_ends.start()
        with jax.named_scope("ahead_y2"):
            ahead_y(core)
        with jax.named_scope("ends2"):
            block_ends(spec, core, both_ends.at[core])
        with jax.named_scope("pair_wait"):
            pair_ends.wait()
        with jax.named_scope("ends_start"):
            chip_ends(0)
            ends_start(0)
            chip_ends(1)

        @pl.when(step > 0)
        def _():
            products(step - 1)

        with jax.named_scope("ends_start1"):
            ends_start(1)
            recv[my_chip] = chip[:, strip(my_strip), :]

        with jax.named_scope("ends_wait"):
            ends_wait()
        with jax.named_scope("solve"):
            solve()
            carry_start()
            car[:, strip(my_strip), :] = sol[my_chip]
        for chunk in range(2):
            with jax.named_scope("carry_wait"):
                carry_wait(chunk)
            with jax.named_scope("recur1"):
                core_carries(chunk)
                pair_carry[chunk].start()
                recur(core, chunk)
            with jax.named_scope("inverse_z1"):
                inverse_z(core, chunk)
            with jax.named_scope("carry_pair_wait"):
                pair_carry[chunk].wait()
            with jax.named_scope("recur2"):
                recur(1 - core, chunk)
            with jax.named_scope("inverse_z2"):
                inverse_z(1 - core, chunk)
        carry_sent()

        def inverse(i, _):
            zs[step, i] = product((yh_ref[...], yl_ref[...]), (turn_h[i], turn_l[i]))
            return 0

        with jax.named_scope("inverse_y"):
            lax.fori_loop(0, rows + 2, inverse, 0, unroll=5)
        node = jnp.where(
            step == 0, 1.0 / nodes[0], jnp.where(step == 1, 1.0 / nodes[1], 1.0 / nodes[2])
        )
        latest = zs.at[step]

        def apply(i, _):
            for low in row_blocks(BLOCK):
                at, here, total = flux(latest, i, low, BLOCK)
                image = mass_rate * here + total
                imag[i, at] = image
                res[i, at] = res[i, at] - node * image
            return 0

        def folded(value):
            return jnp.sum(value.reshape(value.shape[0] // 8, 8, length_z), 0)

        def apply_last(i, sums):
            for low in row_blocks(BLOCK):
                at, here, total = flux(latest, i, low, BLOCK)
                image = mass_rate * here + total
                fresh = [zs[j, i + 1, at] * image for j in range(ITERS)] + [here * first[i, at]]
                sums = tuple(old + folded(new) for old, new in zip(sums, fresh))
            return sums

        @pl.when(step < ITERS - 1)
        def _():
            with jax.named_scope("apply"):
                lax.fori_loop(0, rows, apply, 0)

        @pl.when(step == ITERS - 1)
        def _():
            with jax.named_scope("apply_last"):
                zero = jnp.zeros((8, length_z), jnp.float32)
                keep(step, lax.fori_loop(0, rows, apply_last, (zero,) * (ITERS + 1)))

        return 0

    lax.fori_loop(0, ITERS, iteration, 0)
    lane = lax.broadcasted_iota(jnp.int32, (1, 128), 1)
    packed = jnp.zeros((1, 128), jnp.float32)
    for k in range(ITERS):
        for m in range(ITERS + 1):
            total = jnp.sum(dots[k, m], keepdims=True)
            packed = jnp.where(lane == k * (ITERS + 1) + m, total, packed)
    mine[...] = packed
    with jax.named_scope("gather"):
        start_all(gath_copy, devices)
        gath[me] = mine[...]
        wait_all(gath_copy, devices)
    total = jnp.sum(gath[...], 0)

    def entry(k, m):
        index = k * (ITERS + 1) + m
        return total[:, index : index + 1]

    lower = [[None] * ITERS for _ in range(ITERS)]
    inverse_pivot, partial, pivots = [], [], []
    for k in range(ITERS):
        pivot = entry(k, k)
        value = entry(k, ITERS)
        for j in range(k):
            pivot = pivot - lower[k][j] * lower[k][j] * pivots[j]
            value = value - lower[k][j] * partial[j]
        pivots.append(pivot)
        usable = pivot > pivot_floor * entry(k, k)
        inverse_pivot.append(jnp.where(usable, 1.0 / jnp.where(usable, pivot, 1.0), 0.0))
        partial.append(value)
        for i in range(k + 1, ITERS):
            value = entry(i, k)
            for j in range(k):
                value = value - lower[i][j] * lower[k][j] * pivots[j]
            lower[i][k] = value * inverse_pivot[k]
    coefs = [None] * ITERS
    for k in reversed(range(ITERS)):
        value = partial[k] * inverse_pivot[k]
        for i in range(k + 1, ITERS):
            value = value - lower[i][k] * coefs[i]
        coefs[k] = value

    def finish(i, _):
        for low in row_blocks(BLOCK):
            at = slice(low, low + BLOCK)
            value = v_ref[i, at]
            for k in range(ITERS):
                value = value + coefs[k] * zs[k, i + 1, at]
            u_ref[i, at] = value
        return 0

    with jax.named_scope("finish"):
        lax.fori_loop(0, rows, finish, 0)


def fused(potential, recovery, stimulus, conductivity):
    count_y = lax.axis_size("py")
    devices = lax.axis_size("px") * count_y
    rows, length_y, length_z = potential.shape
    part = length_y // devices
    size_x = lax.axis_size("px")
    if size_x & (size_x - 1) or size_x < 2 or count_y % 2 or part % 8 or length_z % 128 or conductivity.shape[1] % 8:
        return local(potential, recovery, stimulus, conductivity)
    rate = base_rate + rate_slope * recovery / (potential + rate_shift)
    recovery_next = recovery + time_step * rate * (
        -recovery - excite_gain * potential * (potential - threshold - 1.0)
    )
    rho, scale = mode_tables(length_y, length_z)
    tables = split(cas_table(length_y)) + split(cas_table(length_z))
    tables += tuple(
        jnp.asarray(table, jnp.float32)
        for table in (
            rho, scale, rho**rows, rho ** (2 * rows), rho ** (rows * devices)
        )
    )
    plane = (length_y, length_z)
    whole = (rows,) + plane
    half = (2, length_y // 2, length_z)
    chips = devices // 2

    def vmem(shape, dtype=jnp.float32):
        return pltpu.VMEM(shape, dtype)

    dma = pltpu.SemaphoreType.DMA
    padded = (rows + 2,) + plane
    square = [vmem((n, n), jnp.bfloat16) for n in (length_y, length_y, length_z, length_z)]
    slots = (chips, 2, part, length_z)
    field = pl.pallas_call(
        kernel,
        out_shape=jax.ShapeDtypeStruct(whole, jnp.float32),
        in_specs=[pl.BlockSpec(memory_space=pl.ANY)] * 13,
        out_specs=pl.BlockSpec(memory_space=pltpu.VMEM),
        scratch_shapes=[
            vmem(whole), vmem(whole), vmem(whole), *square,
            *(vmem(plane) for _ in range(5)),
            vmem(padded), vmem((rows + 1,) + plane), vmem(whole), vmem(whole),
            vmem((ITERS,) + padded), vmem(whole), vmem(whole), vmem(whole), vmem(whole),
            vmem(padded, jnp.bfloat16), vmem(padded, jnp.bfloat16),
            vmem(padded, jnp.bfloat16), vmem(padded, jnp.bfloat16),
            vmem(half), vmem((2,) + half), vmem(half), vmem(slots), vmem(slots), vmem(half),
            vmem(half), vmem((2,) + half),
            vmem((ITERS, ITERS + 1, 8, 128)), vmem((1, 128)), vmem((devices, 1, 128)),
            dma((rows, count_y)), dma((rows, count_y)), dma((4,)), dma((4,)), dma((3,)), dma((3,)),
            dma((chips,)), dma((chips,)), dma((chips,)), dma((chips,)),
            dma((devices,)), dma((devices,)), dma((13,)),
            pltpu.SemaphoreType.REGULAR((len(bits(size_x)),)),
        ],
        compiler_params=pltpu.CompilerParams(
            collective_id=0, has_side_effects=True, vmem_limit_bytes=60 * 1024 * 1024
        ),
    )(potential, recovery, stimulus, conductivity, *tables)
    return (field, recovery_next)


def solution(mesh):
    in_specs = (
        P(AXES, None, None),
        P(AXES, None, None),
        P(AXES, None, None),
        P("px", "py", None),
    )
    out_specs = (P(AXES, None, None), P(AXES, None, None))
    return jax.shard_map(fused, mesh=mesh, in_specs=in_specs, out_specs=out_specs, check_vma=False)
```

```python
import math

import jax
import jax.numpy as jnp
import numpy as np
from jax import lax
from jax.experimental import pallas as pl
from jax.experimental.pallas import tpu as pltpu
from jax.sharding import PartitionSpec as P

ITERS = 4

mass_rate = 0.01
excite_gain = 8.0
threshold = 0.15
base_rate = 0.002
rate_slope = 0.2
rate_shift = 0.3
time_step = 0.1
nodes = (2.6, 1.0, 4.0)
BLOCK = 64
pivot_floor = 1e-6
AXES = ("px", "py")


def cas_table(length):
    steps = np.arange(length)
    angle = 2.0 * math.pi / length * (steps[:, None] * steps[None, :] % length)
    return np.cos(angle) + np.sin(angle)


def wave_term(length):
    return 2.0 - 2.0 * np.cos(2.0 * math.pi / length * np.arange(length))


def mode_tables(length_y, length_z):
    shift = mass_rate + wave_term(length_y)[:, None] + wave_term(length_z)[None, :]
    root = np.sqrt(shift * (4.0 + shift))
    rho = 2.0 / (2.0 + shift + root)
    scale = 1.0 / (root * length_y * length_z)
    return rho, scale


def local(potential, recovery, stimulus, conductivity):
    devices = lax.axis_size("px") * lax.axis_size("py")
    me = lax.axis_index(AXES)
    rows, length_y, length_z = potential.shape
    length_x = rows * devices
    forth = [(i, (i + 1) % devices) for i in range(devices)]
    back = [((i + 1) % devices, i) for i in range(devices)]
    drive = (
        excite_gain * potential * (potential - threshold) * (1.0 - potential) - potential * recovery
    )
    v_star = potential + time_step * (drive + stimulus)
    rate = base_rate + rate_slope * recovery / (potential + rate_shift)
    recovery_next = recovery + time_step * rate * (
        -recovery - excite_gain * potential * (potential - threshold - 1.0)
    )
    cond = lax.all_to_all(conductivity, "py", split_axis=0, concat_axis=1, tiled=True)

    def above(field):
        return lax.ppermute(field[:1], AXES, back)

    def below(field):
        return lax.ppermute(field[-1:], AXES, forth)

    cond_x = jnp.concatenate([below(cond), cond, above(cond)], 0)
    face_x = 0.5 * (cond_x[1:] + cond_x[:-1])
    face_y = 0.5 * (cond + jnp.roll(cond, -1, 1))
    face_z = 0.5 * (cond + jnp.roll(cond, -1, 2))

    def faces(field):
        padded = jnp.concatenate([below(field), field, above(field)], 0)
        flow_x = face_x * (padded[:-1] - padded[1:])
        flow_y = face_y * (field - jnp.roll(field, -1, 1))
        flow_z = face_z * (field - jnp.roll(field, -1, 2))
        return (
            (flow_x[1:] - flow_x[:-1])
            + (flow_y - jnp.roll(flow_y, 1, 1))
            + (flow_z - jnp.roll(flow_z, 1, 2))
        )

    rho64, scale64 = mode_tables(length_y, length_z)
    rho = jnp.asarray(rho64, jnp.float32)
    scale = jnp.asarray(scale64, jnp.float32)
    cas_y = jnp.asarray(cas_table(length_y), jnp.float32)
    cas_z = jnp.asarray(cas_table(length_z), jnp.float32)
    step_log = jnp.asarray(rows * np.log(rho64), jnp.float32)
    closing = jnp.asarray(1.0 / (1.0 - rho64**length_x), jnp.float32)
    part = length_y // devices
    step_log = lax.dynamic_slice_in_dim(step_log, me * part, part, 0)
    closing = lax.dynamic_slice_in_dim(closing, me * part, part, 0)
    order = np.arange(devices)
    gap = jnp.asarray((order[:, None] - 1 - order[None, :]) % devices, jnp.float32)

    def both(field):
        field = jnp.einsum("xyz,zk->xyk", field, cas_z, precision=lax.Precision.HIGH)
        return jnp.einsum("xyk,yq->xqk", field, cas_y, precision=lax.Precision.HIGH)

    def apply_inverse(residual):
        spectrum = both(residual)
        head = spectrum[rows - 1]
        tail = spectrum[0]
        for i in range(1, rows):
            head = head + rho**i * spectrum[rows - 1 - i]
            tail = tail + rho**i * spectrum[i]
        ends = jnp.stack([head, tail])[None]
        ends = lax.all_to_all(ends, AXES, split_axis=2, concat_axis=0, tiled=True)
        power = jnp.exp(gap[:, :, None, None] * step_log) * closing
        left = jnp.sum(power * ends[None, :, 0], 1)
        right = jnp.sum(jnp.swapaxes(power, 0, 1) * ends[None, :, 1], 1)
        carry = jnp.stack([left, right], 1)
        carry = lax.all_to_all(carry, AXES, split_axis=0, concat_axis=2, tiled=True)
        forward, backward = [None] * rows, [None] * rows
        value = carry[0, 0]
        for i in range(rows):
            value = spectrum[i] + rho * value
            forward[i] = value
        value = carry[0, 1]
        for i in reversed(range(rows)):
            backward[i] = rho * value
            value = spectrum[i] + backward[i]
        return both(jnp.stack([scale * (f + b) for f, b in zip(forward, backward)]))

    field = v_star
    residual = -faces(v_star)
    direction = image = gamma = alpha = None
    for step in range(ITERS):
        precond = apply_inverse(residual)
        applied = mass_rate * precond + faces(precond)
        sums = jnp.stack([jnp.sum(residual * precond), jnp.sum(applied * precond)])
        sums = jnp.sum(lax.all_gather(jnp.broadcast_to(sums[:, None], (2, 128)), AXES), 0)
        gamma_next, delta = sums[0, 0], sums[1, 0]
        if step == 0:
            alpha = gamma_next / delta
            direction, image = precond, applied
        else:
            beta = gamma_next / gamma
            alpha = gamma_next / (delta - beta * gamma_next / alpha)
            direction = precond + beta * direction
            image = applied + beta * image
        gamma = gamma_next
        field = field + alpha * direction
        residual = residual - alpha * image
    return (field, recovery_next)


def bits(count):
    return [1 << n for n in range(count.bit_length() - 1)]


def split(table):
    high = table.astype(jnp.bfloat16)
    low = (table - high.astype(np.float64)).astype(jnp.bfloat16)
    return jnp.asarray(high), jnp.asarray(low)


def parts_of(block):
    high = block.astype(jnp.bfloat16)
    return high, (block - high.astype(jnp.float32)).astype(jnp.bfloat16)


def product(left, right):
    def dot(a, b):
        return jnp.dot(a, b, preferred_element_type=jnp.float32)

    return dot(left[0], right[1]) + dot(left[1], right[0]) + dot(left[0], right[0])


def kernel(
    v_hbm, w_hbm, i_hbm, cond_in, yh_in, yl_in, zh_in, zl_in, rho_in, scale_in, sigma_in,
    pair_in, wrap_in,
    u_hbm,
    v_ref, w_ref, i_ref, yh_ref, yl_ref, zh_ref, zl_ref, rho_ref, scale_ref, sigma_ref,
    pair_ref, wrap_ref,
    cond, face_x, face_y, face_z, back_y, back_z, centre, zs, res, first, imag, spec, mode_h, mode_l, turn_h, turn_l,
    out, both_ends, chip, recv, sol, car, back, carry, dots, mine, gath,
    c_send, c_recv, h_send, h_recv, p_send, p_recv, e_send, e_recv, s_send, s_recv,
    g_send, g_recv, l_sem, r_sem, u_sem, k_send, k_recv,
):
    count_y = lax.axis_size("py")
    devices = lax.axis_size("px") * count_y
    chips = devices // 2
    my_y = lax.axis_index("py")
    me = lax.axis_index("px") * count_y + my_y
    core = me % 2
    my_chip = me // 2
    rows, length_y, length_z = v_ref.shape
    half = length_y // 2
    part = half // chips
    quarter = half // 2
    owners = chips // 2
    wide_y = cond_in.shape[1]
    mesh_type = pl.DeviceIdType.MESH

    def device(index):
        return (index // count_y, index % count_y)

    def tint(index):
        return (index // 2 + index // 4) % 2

    def owner(chunk, index):
        return 2 * index + (chunk + tint(2 * index)) % 2

    my_chunk = (my_chip + tint(my_chip)) % 2
    my_strip = my_chunk * owners + my_chip // 2

    def strip(index):
        return pl.ds(pl.multiple_of(index * part, part), part)

    def remote(source, target, send, recv_sem, index):
        return pltpu.make_async_remote_copy(
            source, target, send, recv_sem, device_id=device(index), device_id_type=mesh_type
        )

    def halo(buffer, base):
        left = (me + devices - 1) % devices
        right = (me + 1) % devices
        return (
            remote(buffer.at[1], buffer.at[rows + 1], h_send.at[base], h_recv.at[base], left),
            remote(
                buffer.at[rows], buffer.at[0], h_send.at[base + 1], h_recv.at[base + 1], right
            ),
        )

    def start_all(make, count):
        for k in range(1, count):
            make(k).start()

    def wait_all(make, count):
        for k in range(1, count):
            make(k).wait()

    def cond_copy(row, k):
        other = (my_y + k) % count_y
        return pltpu.make_async_remote_copy(
            cond_in.at[other * rows + row],
            cond.at[row + 1, pl.ds(pl.multiple_of(my_y * wide_y, 8), wide_y), :],
            c_send.at[row, k], c_recv.at[row, k],
            device_id=(lax.axis_index("px"), other), device_id_type=mesh_type,
        )

    def ends_copy(chunk, index, source):
        at = chunk * owners + index
        return remote(
            chip.at[:, strip(at), :], recv.at[source], e_send.at[at], e_recv.at[source],
            2 * owner(chunk, index) + core,
        )

    def carry_copy(other, source, strip_at):
        return remote(
            sol.at[other], car.at[:, strip(strip_at), :], s_send.at[other], s_recv.at[source],
            2 * other + core,
        )

    def unless_mine(other, action):
        pl.when(other != my_chip)(action)

    def ends_start(chunk):
        for index in range(owners):
            index = (my_chip // 2 + index) % owners
            unless_mine(owner(chunk, index), ends_copy(chunk, index, my_chip).start)

    def ends_wait():
        for chunk in range(2):
            for index in range(owners):
                unless_mine(owner(chunk, index), ends_copy(chunk, index, my_chip).wait_send)
        for source in range(chips):
            unless_mine(source, ends_copy(0, 0, source).wait_recv)

    def carry_start():
        for k in range(1, chips):
            carry_copy((my_chip + k) % chips, my_chip, my_strip).start()

    def carry_wait(chunk):
        for index in range(owners):
            other = owner(chunk, index)
            unless_mine(other, carry_copy(0, other, chunk * owners + index).wait_recv)

    def carry_sent():
        for k in range(1, chips):
            carry_copy((my_chip + k) % chips, my_chip, my_strip).wait_send()

    def gath_copy(k):
        return remote(mine, gath.at[me], g_send.at[k], g_recv.at[k], (me + k) % devices)

    partner = me + 1 - 2 * core
    pair_ends = remote(out, both_ends.at[core], p_send.at[0], p_recv.at[0], partner)
    pair_carry = []
    for n in range(2):
        cut = pl.ds(n * quarter, quarter)
        pair_carry.append(remote(
            back.at[:, cut, :], carry.at[core, :, cut, :], p_send.at[1 + n], p_recv.at[1 + n],
            partner,
        ))

    def flux(field, i, low, block):
        at = slice(low, low + block)
        before = slice((low - 8) % length_y, (low - 8) % length_y + 8)
        after = slice((low + block) % length_y, (low + block) % length_y + 8)
        here = field[i + 1, at]
        wide = jnp.concatenate([field[i + 1, before], here, field[i + 1, after]], 0)
        count = block + 16
        image = centre[i, at] * here
        image = image - face_x[i + 1, at] * field[i + 2, at]
        image = image - face_x[i, at] * field[i, at]
        image = image - face_y[i, at] * pltpu.roll(wide, count - 1, 0)[8 : block + 8]
        image = image - back_y[i, at] * pltpu.roll(wide, 1, 0)[8 : block + 8]
        image = image - face_z[i, at] * pltpu.roll(here, length_z - 1, 1)
        image = image - back_z[i, at] * pltpu.roll(here, 1, 1)
        return at, here, image

    def row_blocks(block):
        return range(0, length_y, block)

    def local_copy(source, target, index):
        return pltpu.make_async_copy(source, target, l_sem.at[index])

    my_x = lax.axis_index("px")
    size_x = lax.axis_size("px")
    rounds = [(my_x + bit - 2 * bit * (my_x // bit % 2)) * count_y + my_y for bit in bits(size_x)]
    greeted = [my_x * count_y + (my_y + k) % count_y for k in range(1, count_y)] + rounds
    barrier = pltpu.get_barrier_semaphore()
    with jax.named_scope("greet"):
        for other in greeted:
            pl.semaphore_signal(barrier, 1, device_id=device(other), device_id_type=mesh_type)
        pl.semaphore_wait(barrier, len(greeted))

    def tell(n):
        pl.semaphore_signal(r_sem.at[n], 1, device_id=device(rounds[n]), device_id_type=mesh_type)

    with jax.named_scope("issue"):
        for row in (0, rows - 1) + tuple(range(1, rows - 1)):
            for k in range(1, count_y):
                cond_copy(row, k).start()
    own_cond = local_copy(
        cond_in.at[pl.ds(my_y * rows, rows)],
        cond.at[pl.ds(1, rows), pl.ds(pl.multiple_of(my_y * wide_y, 8), wide_y), :],
        0,
    )
    ionic = [
        local_copy(source, target, 1 + n)
        for n, (source, target) in enumerate(((v_hbm, v_ref), (w_hbm, w_ref), (i_hbm, i_ref)))
    ]
    loads = [
        local_copy(source, target, 4 + n)
        for n, (source, target) in enumerate((
            (yh_in, yh_ref), (yl_in, yl_ref), (zh_in, zh_ref), (zl_in, zl_ref),
            (rho_in, rho_ref), (scale_in, scale_ref), (sigma_in, sigma_ref),
            (pair_in, pair_ref), (wrap_in, wrap_ref),
        ))
    ]
    with jax.named_scope("issue_local"):
        for copy in ionic + [own_cond] + loads:
            copy.start()
    with jax.named_scope("ionic_wait"):
        for copy in ionic:
            copy.wait()
    for n in range(len(rounds)):
        tell(n)
        pl.semaphore_wait(r_sem.at[n], 1)
    start = zs.at[0]

    def react(i, _):
        v = v_ref[i]
        drive = excite_gain * v * (v - threshold) * (1.0 - v) - v * w_ref[i]
        v = v + time_step * (drive + i_ref[i])
        v_ref[i] = v
        start[i + 1] = v
        return 0

    lax.fori_loop(0, rows, react, 0)
    field_halo = halo(start, 0)
    for copy in field_halo:
        copy.start()

    def clear(i, _):
        for k in range(1, ITERS):
            zs[k, i + 1] = jnp.zeros((length_y, length_z), jnp.float32)
        return 0

    lax.fori_loop(0, rows, clear, 0)
    with jax.named_scope("loads_wait"):
        own_cond.wait()
        for copy in loads:
            copy.wait()

    def arrive(row):
        for k in range(1, count_y):
            cond_copy(row, k).wait_recv()

    def faces(i):
        here = cond[i + 1]
        face_y[i] = 0.5 * (here + pltpu.roll(here, length_y - 1, 0))
        back_y[i] = 0.5 * (here + pltpu.roll(here, 1, 0))
        face_z[i] = 0.5 * (here + pltpu.roll(here, length_z - 1, 1))
        back_z[i] = 0.5 * (here + pltpu.roll(here, 1, 1))

    def faces_along(i):
        face_x[i] = 0.5 * (cond[i] + cond[i + 1])

    def begin(i):
        for low in row_blocks(BLOCK):
            at = slice(low, low + BLOCK)
            centre[i, at] = (
                mass_rate
                + (face_x[i, at] + face_x[i + 1, at])
                + (face_y[i, at] + back_y[i, at])
                + (face_z[i, at] + back_z[i, at])
            )
            _, here, image = flux(start, i, low, BLOCK)
            value = mass_rate * here - image
            first[i, at] = value
            res[i, at] = value
        ahead_z(i, 0)
        spec[i] = product((yh_ref[...], yl_ref[...]), (turn_h[i], turn_l[i]))

    def ahead_z(i, _):
        turned = product(parts_of(res[i]), (zh_ref[...], zl_ref[...]))
        turn_h[i], turn_l[i] = parts_of(turned)
        return 0

    def edge_copy(m, slot_row):
        row = 2 * rows * m + (2 * rows - 1) * (1 - slot_row)
        target = (my_x * count_y + 2 * m + 2 - 3 * slot_row + devices) % devices
        at = pl.ds(pl.multiple_of(my_y * wide_y, 8), wide_y)
        place = cond.at[slot_row * (rows + 1), at, :]
        here = local_copy(cond_in.at[row], place, 13)
        there = remote(
            cond_in.at[row], place, k_send.at[2 * m + slot_row], k_recv.at[my_y], target
        )
        return target, here, there

    def edge_arrival(k):
        place = cond.at[core * (rows + 1), pl.ds(k * wide_y, wide_y), :]
        return remote(cond_in.at[0], place, k_send.at[0], k_recv.at[k], partner)

    edges = [(m, side) for m in range(count_y // 2) for side in range(2)]
    for m, side in edges:
        target, here, there = edge_copy(m, side)
        pl.when(target == me)(here.start)
        pl.when(target != me)(there.start)
    owner_x = ((me + 2 * core - 1 + devices) % devices) // count_y

    with jax.named_scope("cond_first"):
        arrive(0)
        arrive(rows - 1)
    inner = remote(
        cond.at[rows - core * (rows - 1)], cond.at[core * (rows + 1)],
        h_send.at[2], h_recv.at[2], partner,
    )
    inner.start()
    faces(0)
    faces(rows - 1)
    with jax.named_scope("cond_1"):
        arrive(1)
    faces(1)
    faces_along(1)

    def stream(t, _):
        arrive(t)
        faces(t)
        faces_along(t)
        begin(t - 1)
        return 0

    with jax.named_scope("cond_stream"):
        lax.fori_loop(2, rows - 1, stream, 0)
    faces_along(rows - 1)
    begin(rows - 2)
    with jax.named_scope("cond_halo"):
        for copy in field_halo:
            copy.wait()
        inner.wait()
        for m, side in edges:
            target, here, there = edge_copy(m, side)
            pl.when(target == me)(here.wait)
            pl.when(target != me)(there.wait_send)
        for k in range(count_y):
            pl.when(owner_x * count_y + k != me)(edge_arrival(k).wait_recv)
    with jax.named_scope("cond_tail"):
        faces_along(0)
        faces_along(rows)
        begin(0)
        begin(rows - 1)
        for row in range(rows):
            for k in range(1, count_y):
                cond_copy(row, k).wait_send()

    def products(step):
        block = 8
        per = length_y // block

        def body(t, sums):
            i = t // per
            at = pl.ds(pl.multiple_of((t % per) * block, block), block)
            image = imag[i, at, :]
            fresh = [zs[j, i + 1, at, :] for j in range(ITERS)]
            sums = [total + z * image for total, z in zip(sums, fresh)] + [
                sums[ITERS] + zs[step, i + 1, at, :] * first[i, at, :]
            ]
            return tuple(sums)

        zero = jnp.zeros((block, length_z), jnp.float32)
        sums = lax.fori_loop(0, rows * per, body, (zero,) * (ITERS + 1), unroll=16)
        keep(step, sums)

    def keep(step, sums):
        for m, total in enumerate(sums):
            dots[step, m] = sum(total[:, c : c + 128] for c in range(0, length_z, 128))

    def block_ends(where, side, target, block=8):
        def body(b, _):
            low = pl.multiple_of(b * block, block)
            at = pl.ds(pl.multiple_of(side * half + low, block), block)
            rho = rho_ref[at, :]
            planes = [spec[i, at, :] for i in range(rows)]
            head, tail = planes[0], planes[rows - 1]
            for i in range(1, rows):
                head = planes[i] + rho * head
                tail = planes[rows - 1 - i] + rho * tail
            target[0, pl.ds(low, block), :] = head
            target[1, pl.ds(low, block), :] = tail
            return 0

        lax.fori_loop(0, half // block, body, 0, unroll=2)

    def chip_ends(chunk, block=8):
        def body(b, _):
            low = pl.multiple_of(chunk * quarter + b * block, block)
            at = pl.ds(low, block)
            sigma = sigma_ref[pl.ds(pl.multiple_of(core * half + low, block), block), :]
            chip[0, at, :] = both_ends[1, 0, at, :] + sigma * both_ends[0, 0, at, :]
            chip[1, at, :] = both_ends[0, 1, at, :] + sigma * both_ends[1, 1, at, :]
            return 0

        lax.fori_loop(0, quarter // block, body, 0, unroll=4)

    def core_carries(chunk, block=8):
        def body(b, _):
            low = pl.multiple_of(chunk * quarter + b * block, block)
            at = pl.ds(low, block)
            sigma = sigma_ref[pl.ds(pl.multiple_of(core * half + low, block), block), :]
            left, right = car[0, at, :], car[1, at, :]
            after = both_ends[1, 1, at, :] + sigma * right
            before = both_ends[0, 0, at, :] + sigma * left
            carry[core, 0, at, :] = jnp.where(core == 0, left, before)
            carry[core, 1, at, :] = jnp.where(core == 0, after, right)
            back[0, at, :] = jnp.where(core == 0, before, left)
            back[1, at, :] = jnp.where(core == 0, right, after)
            return 0

        lax.fori_loop(0, quarter // block, body, 0, unroll=4)

    def recur(side, chunk, block=16, wide=128):
        def body(b, _):
            low = pl.multiple_of(chunk * quarter + b * block, block)
            at = pl.ds(pl.multiple_of(side * half + low, block), block)
            for c in range(0, length_z, wide):
                cut = slice(c, c + wide)
                rho = rho_ref[at, cut]
                scale = scale_ref[at, cut]
                left = carry[side, 0, pl.ds(low, block), cut]
                right = carry[side, 1, pl.ds(low, block), cut]
                planes = [spec[i, at, cut] for i in range(rows)]
                ahead = [None] * rows
                value = right
                for i in reversed(range(rows)):
                    ahead[i] = rho * value
                    value = planes[i] + ahead[i]
                modes = [left + rho * value]
                value = left
                for i in range(rows):
                    value = planes[i] + rho * value
                    modes.append(value + ahead[i])
                modes.append(right + rho * value)
                for i, mode in enumerate(modes):
                    mode_h[i, at, cut], mode_l[i, at, cut] = parts_of(scale * mode)
            return 0

        lax.fori_loop(0, quarter // block, body, 0)

    def solve():
        own = pl.ds(pl.multiple_of(core * half + my_strip * part, part), part)
        sigma = pair_ref[own, :]
        close = 1.0 / (1.0 - wrap_ref[own, :])
        zero = jnp.zeros_like(sigma)

        def sums(b, pair):
            return (
                recv[b, 0] + sigma * pair[0],
                recv[chips - 1 - b, 1] + sigma * pair[1],
            )

        pair = lax.fori_loop(0, chips, sums, (zero, zero), unroll=4)

        def place(b, pair):
            sol[b, 0] = pair[0]
            sol[chips - 1 - b, 1] = pair[1]
            return sums(b, pair)

        lax.fori_loop(0, chips, place, (pair[0] * close, pair[1] * close), unroll=4)

    def ahead_y(side):
        at = pl.ds(pl.multiple_of(side * half, half), half)

        def body(i, _):
            spec[i, at, :] = product((yh_ref[at, :], yl_ref[at, :]), (turn_h[i], turn_l[i]))
            return 0

        lax.fori_loop(0, rows, body, 0, unroll=4)

    def inverse_z(side, chunk):
        at = pl.ds(pl.multiple_of(side * half + chunk * quarter, quarter), quarter)

        group = (rows + 2) // 2

        def body(g, _):
            planes = pl.ds(g * group, group)
            shape = (group, quarter, length_z)
            modes = tuple(
                mode[planes, at, :].reshape(group * quarter, length_z) for mode in (mode_h, mode_l)
            )
            high, low = parts_of(product(modes, (zh_ref[...], zl_ref[...])))
            turn_h[planes, at, :] = high.reshape(shape)
            turn_l[planes, at, :] = low.reshape(shape)
            return 0

        lax.fori_loop(0, 2, body, 0, unroll=True)

    def iteration(step, _):
        @pl.when(step > 0)
        def _():
            with jax.named_scope("ahead_z"):
                lax.fori_loop(0, rows, ahead_z, 0, unroll=4)

        @pl.when(step > 0)
        def _():
            with jax.named_scope("ahead_y1"):
                ahead_y(1 - core)

        with jax.named_scope("ends1"):
            block_ends(spec, 1 - core, out)
        pair_ends.start()

        @pl.when(step > 0)
        def _():
            with jax.named_scope("ahead_y2"):
                ahead_y(core)

        with jax.named_scope("ends2"):
            block_ends(spec, core, both_ends.at[core])
        with jax.named_scope("pair_wait"):
            pair_ends.wait()
        with jax.named_scope("ends_start"):
            chip_ends(0)
            ends_start(0)
            chip_ends(1)

        @pl.when(step > 0)
        def _():
            products(step - 1)

        with jax.named_scope("ends_start1"):
            ends_start(1)
            recv[my_chip] = chip[:, strip(my_strip), :]

        with jax.named_scope("ends_wait"):
            ends_wait()
        with jax.named_scope("solve"):
            solve()
            carry_start()
            car[:, strip(my_strip), :] = sol[my_chip]
        for chunk in range(2):
            with jax.named_scope("carry_wait"):
                carry_wait(chunk)
            with jax.named_scope("recur1"):
                core_carries(chunk)
                pair_carry[chunk].start()
                recur(core, chunk)
            with jax.named_scope("inverse_z1"):
                inverse_z(core, chunk)
            with jax.named_scope("carry_pair_wait"):
                pair_carry[chunk].wait()
            with jax.named_scope("recur2"):
                recur(1 - core, chunk)
            with jax.named_scope("inverse_z2"):
                inverse_z(1 - core, chunk)
        carry_sent()

        def inverse(i, _):
            zs[step, i] = product((yh_ref[...], yl_ref[...]), (turn_h[i], turn_l[i]))
            return 0

        with jax.named_scope("inverse_y"):
            lax.fori_loop(0, rows + 2, inverse, 0, unroll=5)
        node = jnp.where(
            step == 0, 1.0 / nodes[0], jnp.where(step == 1, 1.0 / nodes[1], 1.0 / nodes[2])
        )
        latest = zs.at[step]

        def apply(i, _):
            for low in row_blocks(BLOCK):
                at, here, image = flux(latest, i, low, BLOCK)
                imag[i, at] = image
                res[i, at] = res[i, at] - node * image
            return 0

        def folded(value):
            return jnp.sum(value.reshape(value.shape[0] // 8, 8, length_z), 0)

        def apply_last(i, sums):
            for low in row_blocks(BLOCK):
                at, here, image = flux(latest, i, low, BLOCK)
                fresh = [zs[j, i + 1, at] * image for j in range(ITERS)] + [here * first[i, at]]
                sums = tuple(old + folded(new) for old, new in zip(sums, fresh))
            return sums

        @pl.when(step < ITERS - 1)
        def _():
            with jax.named_scope("apply"):
                lax.fori_loop(0, rows, apply, 0)

        @pl.when(step == ITERS - 1)
        def _():
            with jax.named_scope("apply_last"):
                zero = jnp.zeros((8, length_z), jnp.float32)
                keep(step, lax.fori_loop(0, rows, apply_last, (zero,) * (ITERS + 1)))

        return 0

    lax.fori_loop(0, ITERS, iteration, 0)
    lane = lax.broadcasted_iota(jnp.int32, (1, 128), 1)
    packed = jnp.zeros((1, 128), jnp.float32)
    for k in range(ITERS):
        for m in range(ITERS + 1):
            total = jnp.sum(dots[k, m], keepdims=True)
            packed = jnp.where(lane == k * (ITERS + 1) + m, total, packed)
    mine[...] = packed
    with jax.named_scope("gather"):
        start_all(gath_copy, devices)
        gath[me] = mine[...]
        wait_all(gath_copy, devices)
    total = jnp.sum(gath[...], 0)

    def entry(k, m):
        index = k * (ITERS + 1) + m
        return total[:, index : index + 1]

    lower = [[None] * ITERS for _ in range(ITERS)]
    inverse_pivot, partial, pivots = [], [], []
    for k in range(ITERS):
        pivot = entry(k, k)
        value = entry(k, ITERS)
        for j in range(k):
            pivot = pivot - lower[k][j] * lower[k][j] * pivots[j]
            value = value - lower[k][j] * partial[j]
        pivots.append(pivot)
        usable = pivot > pivot_floor * entry(k, k)
        inverse_pivot.append(jnp.where(usable, 1.0 / jnp.where(usable, pivot, 1.0), 0.0))
        partial.append(value)
        for i in range(k + 1, ITERS):
            value = entry(i, k)
            for j in range(k):
                value = value - lower[i][j] * lower[k][j] * pivots[j]
            lower[i][k] = value * inverse_pivot[k]
    coefs = [None] * ITERS
    for k in reversed(range(ITERS)):
        value = partial[k] * inverse_pivot[k]
        for i in range(k + 1, ITERS):
            value = value - lower[i][k] * coefs[i]
        coefs[k] = value

    def result(i):
        return pltpu.make_async_copy(v_ref.at[i], u_hbm.at[i], u_sem.at[i])

    def finish(i, _):
        for low in row_blocks(BLOCK):
            at = slice(low, low + BLOCK)
            value = v_ref[i, at]
            for k in range(ITERS):
                value = value + coefs[k] * zs[k, i + 1, at]
            v_ref[i, at] = value
        result(i).start()
        return 0

    with jax.named_scope("finish"):
        lax.fori_loop(0, rows, finish, 0)
        for i in range(rows):
            result(i).wait()


def fused(potential, recovery, stimulus, conductivity):
    count_y = lax.axis_size("py")
    devices = lax.axis_size("px") * count_y
    rows, length_y, length_z = potential.shape
    part = length_y // devices
    size_x = lax.axis_size("px")
    if size_x & (size_x - 1) or size_x < 2 or count_y % 2 or part % 8 or length_z % 128 or conductivity.shape[1] % 8:
        return local(potential, recovery, stimulus, conductivity)
    rate = base_rate + rate_slope * recovery / (potential + rate_shift)
    recovery_next = recovery + time_step * rate * (
        -recovery - excite_gain * potential * (potential - threshold - 1.0)
    )
    rho, scale = mode_tables(length_y, length_z)
    tables = split(cas_table(length_y)) + split(cas_table(length_z))
    tables += tuple(
        jnp.asarray(table, jnp.float32)
        for table in (
            rho, scale, rho**rows, rho ** (2 * rows), rho ** (rows * devices)
        )
    )
    plane = (length_y, length_z)
    whole = (rows,) + plane
    half = (2, length_y // 2, length_z)
    chips = devices // 2

    def vmem(shape, dtype=jnp.float32):
        return pltpu.VMEM(shape, dtype)

    dma = pltpu.SemaphoreType.DMA
    padded = (rows + 2,) + plane
    square = [vmem((n, n), jnp.bfloat16) for n in (length_y, length_y, length_z, length_z)]
    slots = (chips, 2, part, length_z)
    field = pl.pallas_call(
        kernel,
        out_shape=jax.ShapeDtypeStruct(whole, jnp.float32),
        in_specs=[pl.BlockSpec(memory_space=pl.ANY)] * 13,
        out_specs=pl.BlockSpec(memory_space=pl.ANY),
        scratch_shapes=[
            vmem(whole), vmem(whole), vmem(whole), *square,
            *(vmem(plane) for _ in range(5)),
            vmem(padded), vmem((rows + 1,) + plane), *(vmem(whole) for _ in range(5)),
            vmem((ITERS,) + padded), vmem(whole), vmem(whole), vmem(whole), vmem(whole),
            vmem(padded, jnp.bfloat16), vmem(padded, jnp.bfloat16),
            vmem(padded, jnp.bfloat16), vmem(padded, jnp.bfloat16),
            vmem(half), vmem((2,) + half), vmem(half), vmem(slots), vmem(slots), vmem(half),
            vmem(half), vmem((2,) + half),
            vmem((ITERS, ITERS + 1, 8, 128)), vmem((1, 128)), vmem((devices, 1, 128)),
            dma((rows, count_y)), dma((rows, count_y)), dma((4,)), dma((4,)), dma((3,)), dma((3,)),
            dma((chips,)), dma((chips,)), dma((chips,)), dma((chips,)),
            dma((devices,)), dma((devices,)), dma((14,)),
            pltpu.SemaphoreType.REGULAR((len(bits(size_x)),)),
            dma((rows,)), dma((count_y,)), dma((count_y,)),
        ],
        compiler_params=pltpu.CompilerParams(
            collective_id=0, has_side_effects=True, vmem_limit_bytes=60 * 1024 * 1024
        ),
    )(potential, recovery, stimulus, conductivity, *tables)
    return (field, recovery_next)


def solution(mesh):
    in_specs = (
        P(AXES, None, None),
        P(AXES, None, None),
        P(AXES, None, None),
        P("px", "py", None),
    )
    out_specs = (P(AXES, None, None), P(AXES, None, None))
    return jax.shard_map(fused, mesh=mesh, in_specs=in_specs, out_specs=out_specs, check_vma=False)
```

```python
import math

import jax
import jax.numpy as jnp
import numpy as np
from jax import lax
from jax.experimental import pallas as pl
from jax.experimental.pallas import tpu as pltpu
from jax.sharding import PartitionSpec as P

ITERS = 4

mass_rate = 0.01
excite_gain = 8.0
threshold = 0.15
base_rate = 0.002
rate_slope = 0.2
rate_shift = 0.3
time_step = 0.1
nodes = (2.6, 1.0, 4.0)
BLOCK = 64
pivot_floor = 1e-6
AXES = ("px", "py")


def cas_table(length):
    steps = np.arange(length)
    angle = 2.0 * math.pi / length * (steps[:, None] * steps[None, :] % length)
    return np.cos(angle) + np.sin(angle)


def wave_term(length):
    return 2.0 - 2.0 * np.cos(2.0 * math.pi / length * np.arange(length))


def mode_tables(length_y, length_z):
    shift = mass_rate + wave_term(length_y)[:, None] + wave_term(length_z)[None, :]
    root = np.sqrt(shift * (4.0 + shift))
    rho = 2.0 / (2.0 + shift + root)
    scale = 1.0 / (root * length_y * length_z)
    return rho, scale


def local(potential, recovery, stimulus, conductivity):
    devices = lax.axis_size("px") * lax.axis_size("py")
    me = lax.axis_index(AXES)
    rows, length_y, length_z = potential.shape
    length_x = rows * devices
    forth = [(i, (i + 1) % devices) for i in range(devices)]
    back = [((i + 1) % devices, i) for i in range(devices)]
    drive = (
        excite_gain * potential * (potential - threshold) * (1.0 - potential) - potential * recovery
    )
    v_star = potential + time_step * (drive + stimulus)
    rate = base_rate + rate_slope * recovery / (potential + rate_shift)
    recovery_next = recovery + time_step * rate * (
        -recovery - excite_gain * potential * (potential - threshold - 1.0)
    )
    cond = lax.all_to_all(conductivity, "py", split_axis=0, concat_axis=1, tiled=True)

    def above(field):
        return lax.ppermute(field[:1], AXES, back)

    def below(field):
        return lax.ppermute(field[-1:], AXES, forth)

    cond_x = jnp.concatenate([below(cond), cond, above(cond)], 0)
    face_x = 0.5 * (cond_x[1:] + cond_x[:-1])
    face_y = 0.5 * (cond + jnp.roll(cond, -1, 1))
    face_z = 0.5 * (cond + jnp.roll(cond, -1, 2))

    def faces(field):
        padded = jnp.concatenate([below(field), field, above(field)], 0)
        flow_x = face_x * (padded[:-1] - padded[1:])
        flow_y = face_y * (field - jnp.roll(field, -1, 1))
        flow_z = face_z * (field - jnp.roll(field, -1, 2))
        return (
            (flow_x[1:] - flow_x[:-1])
            + (flow_y - jnp.roll(flow_y, 1, 1))
            + (flow_z - jnp.roll(flow_z, 1, 2))
        )

    rho64, scale64 = mode_tables(length_y, length_z)
    rho = jnp.asarray(rho64, jnp.float32)
    scale = jnp.asarray(scale64, jnp.float32)
    cas_y = jnp.asarray(cas_table(length_y), jnp.float32)
    cas_z = jnp.asarray(cas_table(length_z), jnp.float32)
    step_log = jnp.asarray(rows * np.log(rho64), jnp.float32)
    closing = jnp.asarray(1.0 / (1.0 - rho64**length_x), jnp.float32)
    part = length_y // devices
    step_log = lax.dynamic_slice_in_dim(step_log, me * part, part, 0)
    closing = lax.dynamic_slice_in_dim(closing, me * part, part, 0)
    order = np.arange(devices)
    gap = jnp.asarray((order[:, None] - 1 - order[None, :]) % devices, jnp.float32)

    def both(field):
        field = jnp.einsum("xyz,zk->xyk", field, cas_z, precision=lax.Precision.HIGH)
        return jnp.einsum("xyk,yq->xqk", field, cas_y, precision=lax.Precision.HIGH)

    def apply_inverse(residual):
        spectrum = both(residual)
        head = spectrum[rows - 1]
        tail = spectrum[0]
        for i in range(1, rows):
            head = head + rho**i * spectrum[rows - 1 - i]
            tail = tail + rho**i * spectrum[i]
        ends = jnp.stack([head, tail])[None]
        ends = lax.all_to_all(ends, AXES, split_axis=2, concat_axis=0, tiled=True)
        power = jnp.exp(gap[:, :, None, None] * step_log) * closing
        left = jnp.sum(power * ends[None, :, 0], 1)
        right = jnp.sum(jnp.swapaxes(power, 0, 1) * ends[None, :, 1], 1)
        carry = jnp.stack([left, right], 1)
        carry = lax.all_to_all(carry, AXES, split_axis=0, concat_axis=2, tiled=True)
        forward, backward = [None] * rows, [None] * rows
        value = carry[0, 0]
        for i in range(rows):
            value = spectrum[i] + rho * value
            forward[i] = value
        value = carry[0, 1]
        for i in reversed(range(rows)):
            backward[i] = rho * value
            value = spectrum[i] + backward[i]
        return both(jnp.stack([scale * (f + b) for f, b in zip(forward, backward)]))

    field = v_star
    residual = -faces(v_star)
    direction = image = gamma = alpha = None
    for step in range(ITERS):
        precond = apply_inverse(residual)
        applied = mass_rate * precond + faces(precond)
        sums = jnp.stack([jnp.sum(residual * precond), jnp.sum(applied * precond)])
        sums = jnp.sum(lax.all_gather(jnp.broadcast_to(sums[:, None], (2, 128)), AXES), 0)
        gamma_next, delta = sums[0, 0], sums[1, 0]
        if step == 0:
            alpha = gamma_next / delta
            direction, image = precond, applied
        else:
            beta = gamma_next / gamma
            alpha = gamma_next / (delta - beta * gamma_next / alpha)
            direction = precond + beta * direction
            image = applied + beta * image
        gamma = gamma_next
        field = field + alpha * direction
        residual = residual - alpha * image
    return (field, recovery_next)


def bits(count):
    return [1 << n for n in range(count.bit_length() - 1)]


def split(table):
    high = table.astype(jnp.bfloat16)
    low = (table - high.astype(np.float64)).astype(jnp.bfloat16)
    return jnp.asarray(high), jnp.asarray(low)


def parts_of(block):
    high = block.astype(jnp.bfloat16)
    return high, (block - high.astype(jnp.float32)).astype(jnp.bfloat16)


def product(left, right):
    def dot(a, b):
        return jnp.dot(a, b, preferred_element_type=jnp.float32)

    return dot(left[0], right[1]) + dot(left[1], right[0]) + dot(left[0], right[0])


def kernel(
    v_hbm, w_hbm, i_hbm, cond_in, yh_in, yl_in, zh_in, zl_in, rho_in, scale_in, sigma_in,
    pair_in, wrap_in,
    u_hbm, n_hbm,
    v_ref, w_ref, i_ref, yh_ref, yl_ref, zh_ref, zl_ref, rho_ref, scale_ref, sigma_ref,
    pair_ref, wrap_ref,
    cond, face_x, face_y, face_z, back_y, back_z, centre, zs, res, first, imag, spec, mode_h, mode_l, turn_h, turn_l,
    out, both_ends, chip, recv, sol, car, back, carry, dots, mine, gath,
    c_send, c_recv, h_send, h_recv, p_send, p_recv, e_send, e_recv, s_send, s_recv,
    g_send, g_recv, l_sem, r_sem, u_sem, k_send, k_recv,
):
    count_y = lax.axis_size("py")
    devices = lax.axis_size("px") * count_y
    chips = devices // 2
    my_y = lax.axis_index("py")
    me = lax.axis_index("px") * count_y + my_y
    core = me % 2
    my_chip = me // 2
    rows, length_y, length_z = v_ref.shape
    half = length_y // 2
    part = half // chips
    quarter = half // 2
    owners = chips // 2
    wide_y = cond_in.shape[1]
    mesh_type = pl.DeviceIdType.MESH

    def device(index):
        return (index // count_y, index % count_y)

    def tint(index):
        return (index // 2 + index // 4) % 2

    def owner(chunk, index):
        return 2 * index + (chunk + tint(2 * index)) % 2

    my_chunk = (my_chip + tint(my_chip)) % 2
    my_strip = my_chunk * owners + my_chip // 2

    def strip(index):
        return pl.ds(pl.multiple_of(index * part, part), part)

    def remote(source, target, send, recv_sem, index):
        return pltpu.make_async_remote_copy(
            source, target, send, recv_sem, device_id=device(index), device_id_type=mesh_type
        )

    def halo(buffer, base):
        left = (me + devices - 1) % devices
        right = (me + 1) % devices
        return (
            remote(buffer.at[1], buffer.at[rows + 1], h_send.at[base], h_recv.at[base], left),
            remote(
                buffer.at[rows], buffer.at[0], h_send.at[base + 1], h_recv.at[base + 1], right
            ),
        )

    def start_all(make, count):
        for k in range(1, count):
            make(k).start()

    def wait_all(make, count):
        for k in range(1, count):
            make(k).wait()

    def cond_copy(row, k):
        other = (my_y + k) % count_y
        return pltpu.make_async_remote_copy(
            cond_in.at[other * rows + row],
            cond.at[row + 1, pl.ds(pl.multiple_of(my_y * wide_y, 8), wide_y), :],
            c_send.at[row, k], c_recv.at[row, k],
            device_id=(lax.axis_index("px"), other), device_id_type=mesh_type,
        )

    def ends_copy(chunk, index, source):
        at = chunk * owners + index
        return remote(
            chip.at[:, strip(at), :], recv.at[source], e_send.at[at], e_recv.at[source],
            2 * owner(chunk, index) + core,
        )

    def carry_copy(other, source, strip_at):
        return remote(
            sol.at[other], car.at[:, strip(strip_at), :], s_send.at[other], s_recv.at[source],
            2 * other + core,
        )

    def unless_mine(other, action):
        pl.when(other != my_chip)(action)

    def ends_start(chunk):
        for index in range(owners):
            index = (my_chip // 2 + index) % owners
            unless_mine(owner(chunk, index), ends_copy(chunk, index, my_chip).start)

    def ends_wait():
        for source in range(chips):
            unless_mine(source, ends_copy(0, 0, source).wait_recv)

    def ends_sent():
        for chunk in range(2):
            for index in range(owners):
                unless_mine(owner(chunk, index), ends_copy(chunk, index, my_chip).wait_send)

    def carry_start():
        for k in range(1, chips):
            carry_copy((my_chip + k) % chips, my_chip, my_strip).start()

    def carry_wait(chunk):
        for index in range(owners):
            other = owner(chunk, index)
            unless_mine(other, carry_copy(0, other, chunk * owners + index).wait_recv)

    def carry_sent():
        for k in range(1, chips):
            carry_copy((my_chip + k) % chips, my_chip, my_strip).wait_send()

    def gath_copy(k):
        return remote(mine, gath.at[me], g_send.at[k], g_recv.at[k], (me + k) % devices)

    partner = me + 1 - 2 * core
    pair_ends = remote(out, both_ends.at[core], p_send.at[0], p_recv.at[0], partner)
    pair_carry = []
    for n in range(2):
        cut = pl.ds(n * quarter, quarter)
        pair_carry.append(remote(
            back.at[:, cut, :], carry.at[core, :, cut, :], p_send.at[1 + n], p_recv.at[1 + n],
            partner,
        ))

    def flux(field, i, low, block):
        at = slice(low, low + block)
        before = slice((low - 8) % length_y, (low - 8) % length_y + 8)
        after = slice((low + block) % length_y, (low + block) % length_y + 8)
        here = field[i + 1, at]
        wide = jnp.concatenate([field[i + 1, before], here, field[i + 1, after]], 0)
        count = block + 16
        image = centre[i, at] * here
        image = image - face_x[i + 1, at] * field[i + 2, at]
        image = image - face_x[i, at] * field[i, at]
        image = image - face_y[i, at] * pltpu.roll(wide, count - 1, 0)[8 : block + 8]
        image = image - back_y[i, at] * pltpu.roll(wide, 1, 0)[8 : block + 8]
        image = image - face_z[i, at] * pltpu.roll(here, length_z - 1, 1)
        image = image - back_z[i, at] * pltpu.roll(here, 1, 1)
        return at, here, image

    def row_blocks(block):
        return range(0, length_y, block)

    def local_copy(source, target, index):
        return pltpu.make_async_copy(source, target, l_sem.at[index])

    my_x = lax.axis_index("px")
    size_x = lax.axis_size("px")
    rounds = [(my_x + bit - 2 * bit * (my_x // bit % 2)) * count_y + my_y for bit in bits(size_x)]
    greeted = [my_x * count_y + (my_y + k) % count_y for k in range(1, count_y)] + rounds
    barrier = pltpu.get_barrier_semaphore()
    with jax.named_scope("greet"):
        for other in greeted:
            pl.semaphore_signal(barrier, 1, device_id=device(other), device_id_type=mesh_type)
        pl.semaphore_wait(barrier, len(greeted))

    def tell(n):
        pl.semaphore_signal(r_sem.at[n], 1, device_id=device(rounds[n]), device_id_type=mesh_type)

    with jax.named_scope("issue"):
        for row in (0, rows - 1) + tuple(range(1, rows - 1)):
            for k in range(1, count_y):
                cond_copy(row, k).start()
    own_cond = local_copy(
        cond_in.at[pl.ds(my_y * rows, rows)],
        cond.at[pl.ds(1, rows), pl.ds(pl.multiple_of(my_y * wide_y, 8), wide_y), :],
        0,
    )
    ionic = [
        local_copy(source, target, 1 + n)
        for n, (source, target) in enumerate(((v_hbm, v_ref), (w_hbm, w_ref), (i_hbm, i_ref)))
    ]
    loads = [
        local_copy(source, target, 4 + n)
        for n, (source, target) in enumerate((
            (yh_in, yh_ref), (yl_in, yl_ref), (zh_in, zh_ref), (zl_in, zl_ref),
            (rho_in, rho_ref), (scale_in, scale_ref), (sigma_in, sigma_ref),
            (pair_in, pair_ref), (wrap_in, wrap_ref),
        ))
    ]
    with jax.named_scope("issue_local"):
        for copy in ionic + [own_cond] + loads:
            copy.start()
    with jax.named_scope("ionic_wait"):
        for copy in ionic:
            copy.wait()
    for n in range(len(rounds)):
        tell(n)
        pl.semaphore_wait(r_sem.at[n], 1)
    start = zs.at[0]

    def react(i, _):
        v, w = v_ref[i], w_ref[i]
        rate = base_rate + rate_slope * w / (v + rate_shift)
        w_ref[i] = w + time_step * rate * (-w - excite_gain * v * (v - threshold - 1.0))
        drive = excite_gain * v * (v - threshold) * (1.0 - v) - v * w
        v = v + time_step * (drive + i_ref[i])
        v_ref[i] = v
        start[i + 1] = v
        return 0

    lax.fori_loop(0, rows, react, 0)
    recovered = pltpu.make_async_copy(w_ref, n_hbm, u_sem.at[rows])
    recovered.start()
    field_halo = halo(start, 0)
    for copy in field_halo:
        copy.start()

    def clear(i, _):
        for k in range(1, ITERS):
            zs[k, i + 1] = jnp.zeros((length_y, length_z), jnp.float32)
        return 0

    lax.fori_loop(0, rows, clear, 0)
    with jax.named_scope("loads_wait"):
        own_cond.wait()
        for copy in loads:
            copy.wait()

    def arrive(row):
        for k in range(1, count_y):
            cond_copy(row, k).wait_recv()

    def faces(i):
        here = cond[i + 1]
        face_y[i] = 0.5 * (here + pltpu.roll(here, length_y - 1, 0))
        back_y[i] = 0.5 * (here + pltpu.roll(here, 1, 0))
        face_z[i] = 0.5 * (here + pltpu.roll(here, length_z - 1, 1))
        back_z[i] = 0.5 * (here + pltpu.roll(here, 1, 1))

    def faces_along(i):
        face_x[i] = 0.5 * (cond[i] + cond[i + 1])

    def begin(i):
        for low in row_blocks(BLOCK):
            at = slice(low, low + BLOCK)
            centre[i, at] = (
                mass_rate
                + (face_x[i, at] + face_x[i + 1, at])
                + (face_y[i, at] + back_y[i, at])
                + (face_z[i, at] + back_z[i, at])
            )
            _, here, image = flux(start, i, low, BLOCK)
            value = mass_rate * here - image
            first[i, at] = value
            res[i, at] = value
        ahead_z(i, 0)
        spec[i] = product((yh_ref[...], yl_ref[...]), (turn_h[i], turn_l[i]))

    def ahead_z(i, _):
        turned = product(parts_of(res[i]), (zh_ref[...], zl_ref[...]))
        turn_h[i], turn_l[i] = parts_of(turned)
        return 0

    def edge_copy(m, slot_row):
        row = 2 * rows * m + (2 * rows - 1) * (1 - slot_row)
        target = (my_x * count_y + 2 * m + 2 - 3 * slot_row + devices) % devices
        at = pl.ds(pl.multiple_of(my_y * wide_y, 8), wide_y)
        place = cond.at[slot_row * (rows + 1), at, :]
        here = local_copy(cond_in.at[row], place, 13)
        there = remote(
            cond_in.at[row], place, k_send.at[2 * m + slot_row], k_recv.at[my_y], target
        )
        return target, here, there

    def edge_arrival(k):
        place = cond.at[core * (rows + 1), pl.ds(k * wide_y, wide_y), :]
        return remote(cond_in.at[0], place, k_send.at[0], k_recv.at[k], partner)

    edges = [(m, side) for m in range(count_y // 2) for side in range(2)]
    for m, side in edges:
        target, here, there = edge_copy(m, side)
        pl.when(target == me)(here.start)
        pl.when(target != me)(there.start)
    owner_x = ((me + 2 * core - 1 + devices) % devices) // count_y

    with jax.named_scope("cond_first"):
        arrive(0)
        arrive(rows - 1)
    inner = remote(
        cond.at[rows - core * (rows - 1)], cond.at[core * (rows + 1)],
        h_send.at[2], h_recv.at[2], partner,
    )
    inner.start()
    faces(0)
    faces(rows - 1)
    with jax.named_scope("cond_1"):
        arrive(1)
    faces(1)
    faces_along(1)

    def stream(t, _):
        arrive(t)
        faces(t)
        faces_along(t)
        begin(t - 1)
        return 0

    with jax.named_scope("cond_stream"):
        lax.fori_loop(2, rows - 1, stream, 0)
    faces_along(rows - 1)
    begin(rows - 2)
    with jax.named_scope("cond_halo"):
        for copy in field_halo:
            copy.wait()
        inner.wait()
        for m, side in edges:
            target, here, there = edge_copy(m, side)
            pl.when(target == me)(here.wait)
            pl.when(target != me)(there.wait_send)
        for k in range(count_y):
            pl.when(owner_x * count_y + k != me)(edge_arrival(k).wait_recv)
    with jax.named_scope("cond_tail"):
        faces_along(0)
        faces_along(rows)
        begin(0)
        begin(rows - 1)
        for row in range(rows):
            for k in range(1, count_y):
                cond_copy(row, k).wait_send()

    def products(step):
        block = 8
        per = length_y // block

        def body(t, sums):
            i = t // per
            at = pl.ds(pl.multiple_of((t % per) * block, block), block)
            image = imag[i, at, :]
            fresh = [zs[j, i + 1, at, :] for j in range(ITERS)]
            sums = [total + z * image for total, z in zip(sums, fresh)] + [
                sums[ITERS] + zs[step, i + 1, at, :] * first[i, at, :]
            ]
            return tuple(sums)

        zero = jnp.zeros((block, length_z), jnp.float32)
        sums = lax.fori_loop(0, rows * per, body, (zero,) * (ITERS + 1), unroll=16)
        keep(step, sums)

    def keep(step, sums):
        for m, total in enumerate(sums):
            dots[step, m] = sum(total[:, c : c + 128] for c in range(0, length_z, 128))

    def block_ends(where, side, target, block=8):
        def body(b, _):
            low = pl.multiple_of(b * block, block)
            at = pl.ds(pl.multiple_of(side * half + low, block), block)
            rho = rho_ref[at, :]
            planes = [spec[i, at, :] for i in range(rows)]
            head, tail = planes[0], planes[rows - 1]
            for i in range(1, rows):
                head = planes[i] + rho * head
                tail = planes[rows - 1 - i] + rho * tail
            target[0, pl.ds(low, block), :] = head
            target[1, pl.ds(low, block), :] = tail
            return 0

        lax.fori_loop(0, half // block, body, 0, unroll=4)

    def chip_ends(chunk, block=8):
        def body(b, _):
            low = pl.multiple_of(chunk * quarter + b * block, block)
            at = pl.ds(low, block)
            sigma = sigma_ref[pl.ds(pl.multiple_of(core * half + low, block), block), :]
            chip[0, at, :] = both_ends[1, 0, at, :] + sigma * both_ends[0, 0, at, :]
            chip[1, at, :] = both_ends[0, 1, at, :] + sigma * both_ends[1, 1, at, :]
            return 0

        lax.fori_loop(0, quarter // block, body, 0, unroll=4)

    def core_carries(chunk, block=8):
        def body(b, _):
            low = pl.multiple_of(chunk * quarter + b * block, block)
            at = pl.ds(low, block)
            sigma = sigma_ref[pl.ds(pl.multiple_of(core * half + low, block), block), :]
            left, right = car[0, at, :], car[1, at, :]
            after = both_ends[1, 1, at, :] + sigma * right
            before = both_ends[0, 0, at, :] + sigma * left
            carry[core, 0, at, :] = jnp.where(core == 0, left, before)
            carry[core, 1, at, :] = jnp.where(core == 0, after, right)
            back[0, at, :] = jnp.where(core == 0, before, left)
            back[1, at, :] = jnp.where(core == 0, right, after)
            return 0

        lax.fori_loop(0, quarter // block, body, 0, unroll=4)

    def recur(side, chunk, block=16, wide=128):
        def body(b, _):
            low = pl.multiple_of(chunk * quarter + b * block, block)
            at = pl.ds(pl.multiple_of(side * half + low, block), block)
            for c in range(0, length_z, wide):
                cut = slice(c, c + wide)
                rho = rho_ref[at, cut]
                scale = scale_ref[at, cut]
                left = carry[side, 0, pl.ds(low, block), cut]
                right = carry[side, 1, pl.ds(low, block), cut]
                planes = [spec[i, at, cut] for i in range(rows)]
                ahead = [None] * rows
                value = right
                for i in reversed(range(rows)):
                    ahead[i] = rho * value
                    value = planes[i] + ahead[i]
                modes = [left + rho * value]
                value = left
                for i in range(rows):
                    value = planes[i] + rho * value
                    modes.append(value + ahead[i])
                modes.append(right + rho * value)
                for i, mode in enumerate(modes):
                    mode_h[i, at, cut], mode_l[i, at, cut] = parts_of(scale * mode)
            return 0

        lax.fori_loop(0, quarter // block, body, 0)

    def solve():
        own = pl.ds(pl.multiple_of(core * half + my_strip * part, part), part)
        sigma = pair_ref[own, :]
        close = 1.0 / (1.0 - wrap_ref[own, :])
        zero = jnp.zeros_like(sigma)

        def sums(b, pair):
            return (
                recv[b, 0] + sigma * pair[0],
                recv[chips - 1 - b, 1] + sigma * pair[1],
            )

        pair = lax.fori_loop(0, chips, sums, (zero, zero), unroll=4)

        def place(b, pair):
            sol[b, 0] = pair[0]
            sol[chips - 1 - b, 1] = pair[1]
            return sums(b, pair)

        lax.fori_loop(0, chips, place, (pair[0] * close, pair[1] * close), unroll=4)

    def ahead_y(side):
        at = pl.ds(pl.multiple_of(side * half, half), half)

        def body(i, _):
            spec[i, at, :] = product((yh_ref[at, :], yl_ref[at, :]), (turn_h[i], turn_l[i]))
            return 0

        lax.fori_loop(0, rows, body, 0, unroll=8)

    def inverse_z(side, chunk):
        at = pl.ds(pl.multiple_of(side * half + chunk * quarter, quarter), quarter)

        group = (rows + 2) // 2

        def body(g, _):
            planes = pl.ds(g * group, group)
            shape = (group, quarter, length_z)
            modes = tuple(
                mode[planes, at, :].reshape(group * quarter, length_z) for mode in (mode_h, mode_l)
            )
            high, low = parts_of(product(modes, (zh_ref[...], zl_ref[...])))
            turn_h[planes, at, :] = high.reshape(shape)
            turn_l[planes, at, :] = low.reshape(shape)
            return 0

        lax.fori_loop(0, 2, body, 0, unroll=True)

    def iteration(step, _):
        @pl.when(step > 0)
        def _():
            with jax.named_scope("ahead_z"):
                lax.fori_loop(0, rows, ahead_z, 0, unroll=8)

        @pl.when(step > 0)
        def _():
            with jax.named_scope("ahead_y1"):
                ahead_y(1 - core)

        with jax.named_scope("ends1"):
            block_ends(spec, 1 - core, out)
        pair_ends.start()

        @pl.when(step > 0)
        def _():
            with jax.named_scope("ahead_y2"):
                ahead_y(core)

        with jax.named_scope("ends2"):
            block_ends(spec, core, both_ends.at[core])
        with jax.named_scope("pair_wait"):
            pair_ends.wait()
        with jax.named_scope("ends_start"):
            chip_ends(0)
            ends_start(0)
            chip_ends(1)

        @pl.when(step > 0)
        def _():
            products(step - 1)

        with jax.named_scope("ends_start1"):
            ends_start(1)
            recv[my_chip] = chip[:, strip(my_strip), :]

        with jax.named_scope("ends_wait"):
            ends_wait()
        with jax.named_scope("solve"):
            solve()
            carry_start()
            car[:, strip(my_strip), :] = sol[my_chip]
        for chunk in range(2):
            with jax.named_scope("carry_wait"):
                carry_wait(chunk)
            with jax.named_scope("recur1"):
                core_carries(chunk)
                pair_carry[chunk].start()
                recur(core, chunk)
            with jax.named_scope("inverse_z1"):
                inverse_z(core, chunk)
            with jax.named_scope("carry_pair_wait"):
                pair_carry[chunk].wait()
            with jax.named_scope("recur2"):
                recur(1 - core, chunk)
            with jax.named_scope("inverse_z2"):
                inverse_z(1 - core, chunk)
        ends_sent()
        carry_sent()

        def inverse(i, _):
            zs[step, i] = product((yh_ref[...], yl_ref[...]), (turn_h[i], turn_l[i]))
            return 0

        with jax.named_scope("inverse_y"):
            lax.fori_loop(0, rows + 2, inverse, 0, unroll=10)
        node = jnp.where(
            step == 0, 1.0 / nodes[0], jnp.where(step == 1, 1.0 / nodes[1], 1.0 / nodes[2])
        )
        latest = zs.at[step]

        def apply(i, _):
            for low in row_blocks(BLOCK):
                at, here, image = flux(latest, i, low, BLOCK)
                imag[i, at] = image
                res[i, at] = res[i, at] - node * image
            return 0

        def folded(value):
            return jnp.sum(value.reshape(value.shape[0] // 8, 8, length_z), 0)

        def apply_last(i, sums):
            for low in row_blocks(BLOCK):
                at, here, image = flux(latest, i, low, BLOCK)
                fresh = [zs[j, i + 1, at] * image for j in range(ITERS)] + [here * first[i, at]]
                sums = tuple(old + folded(new) for old, new in zip(sums, fresh))
            return sums

        @pl.when(step < ITERS - 1)
        def _():
            with jax.named_scope("apply"):
                lax.fori_loop(0, rows, apply, 0)

        @pl.when(step == ITERS - 1)
        def _():
            with jax.named_scope("apply_last"):
                zero = jnp.zeros((8, length_z), jnp.float32)
                keep(step, lax.fori_loop(0, rows, apply_last, (zero,) * (ITERS + 1)))

        return 0

    lax.fori_loop(0, ITERS, iteration, 0)
    lane = lax.broadcasted_iota(jnp.int32, (1, 128), 1)
    packed = jnp.zeros((1, 128), jnp.float32)
    for k in range(ITERS):
        for m in range(ITERS + 1):
            total = jnp.sum(dots[k, m], keepdims=True)
            packed = jnp.where(lane == k * (ITERS + 1) + m, total, packed)
    mine[...] = packed
    with jax.named_scope("gather"):
        start_all(gath_copy, devices)
        gath[me] = mine[...]
        wait_all(gath_copy, devices)
    total = jnp.sum(gath[...], 0)

    def entry(k, m):
        index = k * (ITERS + 1) + m
        return total[:, index : index + 1]

    lower = [[None] * ITERS for _ in range(ITERS)]
    inverse_pivot, partial, pivots = [], [], []
    for k in range(ITERS):
        pivot = entry(k, k)
        value = entry(k, ITERS)
        for j in range(k):
            pivot = pivot - lower[k][j] * lower[k][j] * pivots[j]
            value = value - lower[k][j] * partial[j]
        pivots.append(pivot)
        usable = pivot > pivot_floor * entry(k, k)
        inverse_pivot.append(jnp.where(usable, 1.0 / jnp.where(usable, pivot, 1.0), 0.0))
        partial.append(value)
        for i in range(k + 1, ITERS):
            value = entry(i, k)
            for j in range(k):
                value = value - lower[i][j] * lower[k][j] * pivots[j]
            lower[i][k] = value * inverse_pivot[k]
    coefs = [None] * ITERS
    for k in reversed(range(ITERS)):
        value = partial[k] * inverse_pivot[k]
        for i in range(k + 1, ITERS):
            value = value - lower[i][k] * coefs[i]
        coefs[k] = value

    def result(i):
        return pltpu.make_async_copy(v_ref.at[i], u_hbm.at[i], u_sem.at[i])

    def finish(i, _):
        for low in row_blocks(BLOCK):
            at = slice(low, low + BLOCK)
            value = v_ref[i, at]
            for k in range(ITERS):
                value = value + coefs[k] * zs[k, i + 1, at]
            v_ref[i, at] = value
        result(i).start()
        return 0

    with jax.named_scope("finish"):
        lax.fori_loop(0, rows, finish, 0)
        for i in range(rows):
            result(i).wait()
        recovered.wait()


def fused(potential, recovery, stimulus, conductivity):
    count_y = lax.axis_size("py")
    devices = lax.axis_size("px") * count_y
    rows, length_y, length_z = potential.shape
    part = length_y // devices
    size_x = lax.axis_size("px")
    if size_x & (size_x - 1) or size_x < 2 or count_y % 2 or part % 8 or length_z % 128 or conductivity.shape[1] % 8:
        return local(potential, recovery, stimulus, conductivity)
    rho, scale = mode_tables(length_y, length_z)
    tables = split(cas_table(length_y)) + split(cas_table(length_z))
    tables += tuple(
        jnp.asarray(table, jnp.float32)
        for table in (
            rho, scale, rho**rows, rho ** (2 * rows), rho ** (rows * devices)
        )
    )
    plane = (length_y, length_z)
    whole = (rows,) + plane
    half = (2, length_y // 2, length_z)
    chips = devices // 2

    def vmem(shape, dtype=jnp.float32):
        return pltpu.VMEM(shape, dtype)

    dma = pltpu.SemaphoreType.DMA
    padded = (rows + 2,) + plane
    square = [vmem((n, n), jnp.bfloat16) for n in (length_y, length_y, length_z, length_z)]
    slots = (chips, 2, part, length_z)
    return pl.pallas_call(
        kernel,
        out_shape=(jax.ShapeDtypeStruct(whole, jnp.float32),) * 2,
        in_specs=[pl.BlockSpec(memory_space=pl.ANY)] * 13,
        out_specs=(pl.BlockSpec(memory_space=pl.ANY),) * 2,
        scratch_shapes=[
            vmem(whole), vmem(whole), vmem(whole), *square,
            *(vmem(plane) for _ in range(5)),
            vmem(padded), vmem((rows + 1,) + plane), *(vmem(whole) for _ in range(5)),
            vmem((ITERS,) + padded), vmem(whole), vmem(whole), vmem(whole), vmem(whole),
            vmem(padded, jnp.bfloat16), vmem(padded, jnp.bfloat16),
            vmem(padded, jnp.bfloat16), vmem(padded, jnp.bfloat16),
            vmem(half), vmem((2,) + half), vmem(half), vmem(slots), vmem(slots), vmem(half),
            vmem(half), vmem((2,) + half),
            vmem((ITERS, ITERS + 1, 8, 128)), vmem((1, 128)), vmem((devices, 1, 128)),
            dma((rows, count_y)), dma((rows, count_y)), dma((4,)), dma((4,)), dma((3,)), dma((3,)),
            dma((chips,)), dma((chips,)), dma((chips,)), dma((chips,)),
            dma((devices,)), dma((devices,)), dma((14,)),
            pltpu.SemaphoreType.REGULAR((len(bits(size_x)),)),
            dma((rows + 1,)), dma((count_y,)), dma((count_y,)),
        ],
        compiler_params=pltpu.CompilerParams(
            collective_id=0, has_side_effects=True, vmem_limit_bytes=60 * 1024 * 1024
        ),
    )(potential, recovery, stimulus, conductivity, *tables)


def solution(mesh):
    in_specs = (
        P(AXES, None, None),
        P(AXES, None, None),
        P(AXES, None, None),
        P("px", "py", None),
    )
    out_specs = (P(AXES, None, None), P(AXES, None, None))
    return jax.shard_map(fused, mesh=mesh, in_specs=in_specs, out_specs=out_specs, check_vma=False)
```
